32 devices in a mesh: seq: 16 (over z, x, core), tp: 2 (over y).
Axes of the slice: x: 2, y: 2, z: 4, core: 2. Of those that a mesh axis runs over, the one named last changes fastest.
Arguments:
- tokens: bfloat16 [4096, 4096], P('seq', 'tp'), may hold values from -6 to 6
- decay_rate: float32 [4096, 16], P('tp'), as said below
- angle: float32 [4096, 16], P('tp'), may hold values from -3.140625 to 3.140625
- in_coef: float32 [4096, 16], P('tp'), may hold values from -4 to 4
- out_coef: float32 [2, 4096, 16], P(None, 'tp'), may hold values from -1.5 to 1.5
- skip_coef: float32 [4096], P('tp'), may hold values from 0.3 to 1.5
- gate_weight: bfloat16 [4096, 4096], P('seq', 'tp'), may hold values from -0.09375 to 0.09375
- out_weight: bfloat16 [4096, 4096], P('seq', 'tp'), may hold values from -0.09375 to 0.09375
Outputs:
- mixed_out: bfloat16 [4096, 4096], P('seq', 'tp')
The draws below stay inside these ranges and needn't reach their ends.
Inputs may be any that keep to these rules, and one draw needn't show every extreme that they name: `decay_rate`: every entry is positive and below 0.034.
All inputs are finite; a program needn't handle non-finite values.
Results may differ from the reference program's by a relative error of at most 0.01.
Values may be sent and summed in bfloat16 or wider, within the bound.
A program may use at most 192 MiB of HBM per device.

```python
import jax
import jax.numpy as jnp
from jax import lax

D = 4096
H = 16
TOKENS = 4096


def draw_decay_rate(key, part):
    key_rate = jax.random.fold_in(key, 11)
    spread = jax.random.uniform(key_rate, (D, H), jnp.float32)
    lowest = jnp.log(0.5 / TOKENS)
    highest = jnp.log(1.0 / 30.0)
    rate_draw = jnp.exp(lowest + spread * (highest - lowest))
    return rate_draw


def level_of(stream_key, extent, split, least, top_value):
    level, own = 1.0, jax.random.fold_in(stream_key, 6)
    for position, shards_of in split:
        steps = jnp.exp(jax.random.uniform(jax.random.fold_in(own, position), (shards_of,), jnp.float32, least / len(split), top_value / len(split)))
        level = level * jnp.repeat(steps, extent[position] // shards_of).reshape([-1 if axis == position else 1 for axis in range(len(extent))])
    return level


def noise(own_key, dims, scale, bound, cuts=(), kind=jnp.bfloat16):
    loudness = level_of(own_key, dims, cuts, -0.22, 0.18) if cuts else 1.0
    drawn = jax.random.normal(own_key, dims, jnp.float32) * scale * loudness
    return jnp.minimum(jnp.maximum(drawn, -bound), bound).astype(kind)


def setup_inputs(seed: int = 0) -> dict:
    keys = jax.random.split(jax.random.key(seed), 9)
    return {
        "tokens": noise(keys[0], (TOKENS, D), 1.0, 6.0, ((0, 16), (1, 2))),
        "decay_rate": draw_decay_rate(jax.random.fold_in(keys[8], 71), 0),
        "angle": jnp.clip(jax.random.uniform(keys[2], (D, H), jnp.float32, -3.140625, 3.140625), -3.140625, 3.140625),
        "in_coef": noise(keys[3], (D, H), 1.0, 4.0, ((0, 2),), jnp.float32),
        "out_coef": noise(keys[4], (2, D, H), H ** -0.5, 1.5, ((1, 2),), jnp.float32),
        "skip_coef": jnp.clip(0.3 + 1.2 * jax.random.uniform(keys[5], (D,), jnp.float32) ** level_of(keys[5], (D,), ((0, 2),), -0.2, 0.2), 0.3, 1.5),
        "gate_weight": noise(keys[6], (D, D), D ** -0.5, 0.09375, ((0, 16), (1, 2))),
        "out_weight": noise(keys[7], (D, D), D ** -0.5, 0.09375, ((0, 16), (1, 2))),
    }


def kernel_block(rate, rotation_rate, in_part, out_real, out_imag, length):
    positions = jnp.arange(length).astype(jnp.float32)[:, None, None]
    magnitude = 1.0 - rate
    scaled = in_part * jnp.sqrt(1.0 - magnitude * magnitude)
    damping = jnp.exp(positions * jnp.log1p(-rate))
    rotation = positions * rotation_rate
    summands = scaled * damping * (out_real * jnp.cos(rotation) - out_imag * jnp.sin(rotation))
    return lax.optimization_barrier(jnp.sum(summands, axis=2))

def reference(tokens, decay_rate, angle, in_coef, out_coef, skip_coef, gate_weight, out_weight):
    length = tokens.shape[0]
    channels = tokens.shape[1]
    group_size = min(128, channels)
    group_count = channels // group_size
    values = tokens.astype(jnp.float32)

    def per_group(group_index):
        offset = group_index * group_size
        columns = lax.dynamic_slice_in_dim(values, offset, group_size, 1)

        def select(table):
            return lax.dynamic_slice_in_dim(table, offset, group_size, 0)
        kernel = kernel_block(select(decay_rate), select(angle), select(in_coef), select(out_coef[0]), select(out_coef[1]), length)
        spectrum = jnp.fft.rfft(columns, n=2 * length, axis=0) * jnp.fft.rfft(kernel, n=2 * length, axis=0)
        return jnp.fft.irfft(spectrum, n=2 * length, axis=0)[:length]
    blocks = lax.map(per_group, jnp.arange(group_count, dtype=jnp.int32))
    smoothed = jnp.transpose(blocks, (1, 0, 2)).reshape(length, channels) + skip_coef * values
    gate_pre = jnp.dot(tokens, gate_weight, preferred_element_type=jnp.float32)
    hidden = (jax.nn.silu(smoothed) * jax.nn.sigmoid(gate_pre)).astype(jnp.bfloat16)
    return jnp.dot(hidden, out_weight, preferred_element_type=jnp.float32).astype(jnp.bfloat16)
```

```python
import functools

import jax
import jax.numpy as jnp
from jax import lax
from jax.experimental import pallas as pl
from jax.experimental.pallas import tpu as pltpu
from jax.sharding import PartitionSpec as P

LANES = 128
UNROLL = 8
MESH = pl.DeviceIdType.MESH
F32, BF16 = jnp.float32, jnp.bfloat16


def mixer_kernel(
    lines, parts, dims,
    tok, gate_w, out_w, q_re_ref, q_im_ref, c_re_ref, c_im_ref, s_re_ref, s_im_ref, skip_ref,
    out_ref,
    te, x2d, y2d, st, cin, cout, A, W, own, cs, cr, hid, ost,
    l_w, l_te, l_a, sw_s, sw_r, te_s, te_r, z_s, z_r, x_s, x_r, p_s, p_r, po_s, ch_s, ch_r, c_s, c_r, o_s, o_r,
):
    rows, width = tok.shape
    bw = gate_w.shape[0]
    blk = 2 * bw
    chunks = width // blk
    halves = chunks // 2
    sub = chunks * bw // LANES
    tiles = bw // LANES
    two = 2 * rows

    s = lax.axis_index("seq")
    y = lax.axis_index("tp")
    z, x, c = s // 4, (s // 2) % 2, s % 2
    pos = z * 2 + x

    def dev(zz, xx, cc, yy):
        return ((zz * 2 + xx) * 2 + cc, yy)

    partner = dev(z, x, 1 - c, y)
    is_mid = (z > 0) & (z < lines - 1)

    def hint(v, m):
        return v if isinstance(v, int) else pl.multiple_of(v, m)

    def ds(start, size, m):
        return pl.ds(hint(start, m), size)

    def remote(src, dst, ssem, rsem, where):
        return pltpu.make_async_remote_copy(src, dst, ssem, rsem, device_id=where, device_id_type=MESH)

    weights = (gate_w, out_w)
    others = [(xx, yy) for yy in range(parts) for xx in range(2)]
    peers = others[1:]

    def w_local(w, j):
        return pltpu.make_async_copy(
            weights[w].at[:, ds(j * blk + c * bw, bw, bw)],
            W.at[w, j, ds(z * blk + c * bw, bw, bw)], l_w.at[w, j])

    def w_swap(w, j):
        return remote(
            weights[w].at[:, ds(j * blk + (1 - c) * bw, bw, bw)],
            W.at[w, j, ds(z * blk + c * bw, bw, bw)], sw_s.at[w, j], sw_r.at[w, j], partner)

    def te_local(j):
        return pltpu.make_async_copy(
            tok.at[:, ds(j * blk + c * bw, bw, bw)], te.at[ds(c * rows, rows, rows), ds(j * bw, bw, bw)], l_te.at[j])

    def te_swap(j):
        return remote(
            tok.at[:, ds(j * blk + (1 - c) * bw, bw, bw)],
            te.at[ds(c * rows, rows, rows), ds(j * bw, bw, bw)], te_s.at[j], te_r.at[j], partner)

    def piece(w, j, o):
        return W.at[w, j, ds(o * blk, blk, blk)]

    def z_send(w, j, o, side):
        where = dev(z + (1 if side else -1), x, c, y)
        return remote(piece(w, j, o), piece(w, j, o), z_s.at[side, w, j, o], z_r.at[w, j, o], where)

    def at_peer(dx, dy):
        return (x + dx) % 2, (y + dy) % parts

    def a_cols(yy, jj):
        return ds((yy * halves + jj) * blk, blk, blk)

    def slot(dx, yy):
        return dx * parts + yy

    def t_send(dx, dy, jj):
        xx, yy = at_peer(dx, dy)
        return remote(
            tok.at[:, ds((2 * jj + xx) * blk, blk, blk)],
            A.at[0, ds((x * 2 + c) * rows, rows, rows), a_cols(y, jj)],
            x_s.at[0, dx * parts + dy, jj], x_r.at[0, slot(dx, y), jj], dev(z, xx, c, yy))

    def t_got(dx, dy, jj):
        xx, yy = at_peer(dx, dy)
        dst = A.at[0, ds((xx * 2 + c) * rows, rows, rows), a_cols(yy, jj)]
        return remote(dst, dst, x_s.at[0, dx * parts + dy, jj], x_r.at[0, slot(dx, yy), jj], dev(z, xx, c, yy))

    def t_local(jj):
        return pltpu.make_async_copy(
            tok.at[:, ds((2 * jj + x) * blk, blk, blk)],
            A.at[0, ds((x * 2 + c) * rows, rows, rows), a_cols(y, jj)], l_a.at[jj])

    def t_own(jj):
        return remote(
            tok.at[:, ds((2 * jj + x) * blk, blk, blk)],
            A.at[0, ds((x * 2 + c) * rows, rows, rows), a_cols(y, jj)],
            p_s.at[0, 0, jj], p_r.at[0, slot(0, y), jj], partner)

    def t_pass(dx, dy, jj):
        xx, yy = at_peer(dx, dy)
        ref = A.at[0, ds((xx * 2 + c) * rows, rows, rows), a_cols(yy, jj)]
        return remote(ref, ref, p_s.at[0, dx * parts + dy, jj], p_r.at[0, slot(dx, yy), jj], partner)

    def t_passed(dx, dy, jj):
        xx, yy = at_peer(dx, dy)
        ref = A.at[0, ds((xx * 2 + 1 - c) * rows, rows, rows), a_cols(yy, jj)]
        return remote(ref, ref, p_s.at[0, dx * parts + dy, jj], p_r.at[0, slot(dx, yy), jj], partner)

    def h_ref(xx, yy, jj, cc):
        cols = ds((yy * halves + jj) * blk + cc * bw, bw, bw)
        return A.at[1, ds(xx * two, two, two), cols]

    def h_send(dx, dy, jj, j):
        xx, yy = at_peer(dx, dy)
        return remote(
            hid.at[j], h_ref(x, y, jj, c), x_s.at[1, dx * parts + dy, jj], x_r.at[1, slot(dx, y), jj],
            dev(z, xx, c, yy))

    def h_got(dx, dy, jj):
        xx, yy = at_peer(dx, dy)
        ref = h_ref(xx, yy, jj, c)
        return remote(ref, ref, x_s.at[1, dx * parts + dy, jj], x_r.at[1, slot(dx, yy), jj], dev(z, xx, c, yy))

    def h_own(jj, j):
        return remote(hid.at[j], h_ref(x, y, jj, c), p_s.at[1, 0, jj], p_r.at[1, slot(0, y), jj], partner)

    def h_pass(dx, dy, jj):
        xx, yy = at_peer(dx, dy)
        ref = h_ref(xx, yy, jj, c)
        return remote(ref, ref, p_s.at[1, dx * parts + dy, jj], p_r.at[1, slot(dx, yy), jj], partner)

    def h_passed(dx, dy, jj):
        xx, yy = at_peer(dx, dy)
        ref = h_ref(xx, yy, jj, 1 - c)
        return remote(ref, ref, p_s.at[1, dx * parts + dy, jj], p_r.at[1, slot(dx, yy), jj], partner)

    def c_send(w, j):
        return remote(cs.at[w, j], cr.at[w, j], c_s.at[w, j], c_r.at[w, j], dev(z, 1 - x, c, y))

    def chain_send():
        nxt = pos + 1
        return remote(cout, cin, ch_s, ch_r, dev(nxt // 2, nxt % 2, c, y))

    def o_send(j):
        return remote(ost.at[j], out_ref.at[:, ds(j * blk + c * bw, bw, bw)], o_s.at[j], o_r.at[j], partner)

    def o_got(j):
        ref = out_ref.at[:, ds(j * blk + (1 - c) * bw, bw, bw)]
        return remote(ost.at[j], ref, o_s.at[j], o_r.at[j], partner)

    def each(n, f):
        def body(i, carry):
            f(i)
            return carry
        lax.fori_loop(0, n, body, 0)

    each(chunks, lambda j: w_local(0, j).start())
    each(chunks, lambda j: te_local(j).start())
    each(halves, lambda jj: t_local(jj).start())
    each(chunks, lambda j: w_local(1, j).start())

    barrier = pltpu.get_barrier_semaphore()

    def greet(where):
        pl.semaphore_signal(barrier, inc=1, device_id=where, device_id_type=MESH)

    greet(partner)
    for dx, dy in peers:
        xx, yy = at_peer(dx, dy)
        greet(dev(z, xx, c, yy))
    line_peers = [
        (z > 0, dev(z - 1, x, c, y)),
        (z < lines - 1, dev(z + 1, x, c, y)),
        ((x == 1) & (z < lines - 1), dev(z + 1, 0, c, y)),
        ((x == 0) & (z > 0), dev(z - 1, 1, c, y)),
    ]
    for there, where in line_peers:
        @pl.when(there)
        def _():
            greet(where)
    pl.semaphore_wait(barrier, 1 + len(peers) + sum(there.astype(jnp.int32) for there, _ in line_peers))

    each(chunks, lambda j: w_swap(0, j).start())
    for dx, dy in peers:
        each(halves, lambda jj: t_send(dx, dy, jj).start())
    each(chunks, lambda j: te_swap(j).start())
    each(halves, lambda jj: t_own(jj).start())
    each(chunks, lambda j: w_swap(1, j).start())

    def own_ready(w, j):
        w_local(w, j).wait()
        w_swap(w, j).wait_recv()

    def own_send(w, j):
        @pl.when(z > 0)
        def _():
            z_send(w, j, z, 0).start()

        @pl.when(z < lines - 1)
        def _():
            z_send(w, j, z, 1).start()

    def forward(w, j, d):
        @pl.when(is_mid & (z + d < lines))
        def _():
            z_send(w, j, z + d, 0).wait_recv()
            z_send(w, j, z + d, 0).start()

        @pl.when(is_mid & (z - d >= 0))
        def _():
            z_send(w, j, z - d, 1).wait_recv()
            z_send(w, j, z - d, 1).start()

    def at_end(w, j):
        for d in range(1, lines):
            @pl.when(z == 0)
            def _():
                z_send(w, j, d, 0).wait_recv()

            @pl.when(z == lines - 1)
            def _():
                z_send(w, j, lines - 1 - d, 0).wait_recv()

    def first_sends(j):
        own_ready(0, j)
        own_send(0, j)

    each(chunks, first_sends)

    def te_ready(j):
        te_local(j).wait()
        te_swap(j).wait_recv()

    each(chunks, te_ready)

    def lay(i, carry):
        for e in range(sub):
            v = te[pl.ds(i * 16, 16), e * LANES:(e + 1) * LANES].astype(F32)
            x2d[pl.ds(i * 16 * sub + e, 16, stride=sub), :] = v
        return carry

    lax.fori_loop(0, two // 16, lay, 0)

    def second_own(j):
        own_ready(1, j)

        @pl.when(jnp.logical_not(is_mid))
        def _():
            own_send(1, j)

    each(chunks, second_own)

    half = dims // 2

    def tile(ref, h):
        return ref[h * sub:(h + 1) * sub, :]

    def step(state, v, q_re, q_im):
        return [(a * re - b * im + v, a * im + b * re) for (re, im), a, b in zip(state, q_re, q_im)]

    def end_half(k):
        hs = range(k * half, (k + 1) * half)
        q_re = [tile(q_re_ref, h) for h in hs]
        q_im = [tile(q_im_ref, h) for h in hs]
        zero = jnp.zeros((sub, LANES), F32)

        def body(i, state):
            for u in range(UNROLL):
                state = step(state, x2d[ds((i * UNROLL + u) * sub, sub, sub), :], q_re, q_im)
            return state

        state = lax.fori_loop(0, two // UNROLL, body, [(zero, zero)] * half)
        for h, (re, im) in zip(hs, state):
            st[0, h * sub:(h + 1) * sub, :] = re
            st[1, h * sub:(h + 1) * sub, :] = im

    end_half(0)
    each(chunks, lambda j: forward(0, j, 1))
    end_half(1)

    def tokens_on(dx, dy):
        def go(jj):
            t_got(dx, dy, jj).wait_recv()
            t_pass(dx, dy, jj).start()
        each(halves, go)

    @pl.when(pos == 0)
    def _():
        cin[...] = jnp.zeros_like(cin)

    @pl.when(pos > 0)
    def _():
        chain_send().wait_recv()

    i_re, i_im = cin[0].astype(F32), cin[1].astype(F32)
    a, b = s_re_ref[...], s_im_ref[...]
    cout[0] = (a * i_re - b * i_im + st[0]).astype(BF16)
    cout[1] = (a * i_im + b * i_re + st[1]).astype(BF16)
    st[0] = i_re
    st[1] = i_im

    @pl.when(pos < 2 * lines - 1)
    def _():
        chain_send().start()

    for dx, dy in peers:
        tokens_on(dx, dy)

    def smooth_half(k):
        hs = range(k * half, (k + 1) * half)
        q_re = [tile(q_re_ref, h) for h in hs]
        q_im = [tile(q_im_ref, h) for h in hs]
        c_re = [tile(c_re_ref, h) for h in hs]
        c_im = [tile(c_im_ref, h) for h in hs]
        skip = skip_ref[...]
        state = [(tile(st.at[0], h), tile(st.at[1], h)) for h in hs]

        def body(i, state):
            for u in range(UNROLL):
                at = ds((i * UNROLL + u) * sub, sub, sub)
                v = x2d[at, :]
                state = step(state, v, q_re, q_im)
                sums = [c_re[h] * state[h][0] - c_im[h] * state[h][1] for h in range(half)]
                while len(sums) > 1:
                    sums = [sum(sums[m:m + 2]) for m in range(0, len(sums), 2)]
                before = v * skip if k == 0 else y2d[at, :]
                y2d[at, :] = before + sums[0]
            return state

        lax.fori_loop(0, two // UNROLL, body, state)

    smooth_half(0)
    for d in range(2, lines - 1):
        each(halves, lambda j: forward(0, j, d))
    smooth_half(1)
    for d in range(2, lines - 1):
        each(halves, lambda j: forward(0, halves + j, d))

    def mid_own(j):
        @pl.when(is_mid)
        def _():
            own_send(1, j)

    def stage(j):
        for d in range(1, lines - 1):
            forward(1, j, d)

    each(halves, mid_own)

    def local_tokens(jj):
        t_local(jj).wait()
        for dx, dy in others:
            t_passed(dx, dy, jj).wait_recv()

    each(halves, local_tokens)

    def project(w, j):
        @pl.when(jnp.logical_not(is_mid))
        def _():
            at_end(w, j)
        right = W[w, j]
        away = jnp.dot(A[w, ds((1 - x) * two, two, two), :], right, preferred_element_type=F32)
        cs[w, j] = away.astype(BF16)
        c_send(w, j).start()
        own[j] = jnp.dot(A[w, ds(x * two, two, two), :], right, preferred_element_type=F32)

    each(chunks, lambda j: project(0, j))
    stage(0)

    def hidden(j):
        c_send(0, j).wait_recv()
        jj = j // 2
        target = j % 2

        def band(i, carry):
            at = pl.ds(pl.multiple_of(i * 16, 16), 16)
            for e in range(tiles):
                lane = slice(e * LANES, (e + 1) * LANES)
                smooth = y2d[pl.ds(i * 16 * sub + j * tiles + e, 16, stride=sub), :]
                gate = own[j, at, lane] + cr[0, j, at, lane].astype(F32)
                value = smooth * jax.nn.sigmoid(smooth) * jax.nn.sigmoid(gate)
                hid[j, at, lane] = value.astype(BF16)
            return carry

        lax.fori_loop(0, two // 16, band, 0)

        @pl.when(target == x)
        def _():
            h_own(jj, j).start()
            for dx, dy in peers:
                if dx == 0:
                    h_send(dx, dy, jj, j).start()
            h_ref(x, y, jj, c)[...] = hid[j]

        @pl.when(target != x)
        def _():
            for dx, dy in peers:
                if dx == 1:
                    h_send(dx, dy, jj, j).start()

    each(halves, hidden)
    stage(1)
    each(halves, lambda j: mid_own(halves + j))
    each(halves, lambda j: hidden(halves + j))

    for dx, dy in peers:
        def hidden_on(jj):
            h_got(dx, dy, jj).wait_recv()
            h_pass(dx, dy, jj).start()
        each(halves, hidden_on)
    each(chunks - 2, lambda j: stage(2 + j))

    def all_hidden(jj):
        for dx, dy in others:
            h_passed(dx, dy, jj).wait_recv()

    each(halves, all_hidden)

    def finish(j):
        c_send(1, j).wait_recv()
        mine = ds(c * rows, rows, rows)
        theirs = ds((1 - c) * rows, rows, rows)
        ost[j] = (own[j, theirs, :] + cr[1, j, theirs, :].astype(F32)).astype(BF16)
        o_send(j).start()
        out_ref[:, ds(j * blk + c * bw, bw, bw)] = (own[j, mine, :] + cr[1, j, mine, :].astype(F32)).astype(BF16)

    project(1, 0)

    def last(j):
        project(1, j + 1)
        finish(j)

    each(chunks - 1, last)
    finish(chunks - 1)
    each(chunks, lambda j: o_got(j).wait_recv())

    def settle(j):
        for w in range(2):
            w_swap(w, j).wait_send()
            c_send(w, j).wait_send()

            @pl.when(z > 0)
            def _():
                z_send(w, j, z, 0).wait_send()

            @pl.when(z < lines - 1)
            def _():
                z_send(w, j, z, 1).wait_send()
            for d in range(1, lines - 1):
                @pl.when(is_mid & (z + d < lines))
                def _():
                    z_send(w, j, z + d, 0).wait_send()

                @pl.when(is_mid & (z - d >= 0))
                def _():
                    z_send(w, j, z - d, 1).wait_send()
        te_swap(j).wait_send()
        o_send(j).wait_send()

    each(chunks, settle)

    def settle_exchange(jj):
        t_own(jj).wait_send()
        h_own(jj, 0).wait_send()
        for dx, dy in peers:
            t_send(dx, dy, jj).wait_send()
            h_send(dx, dy, jj, 0).wait_send()
            t_pass(dx, dy, jj).wait_send()
            h_pass(dx, dy, jj).wait_send()

    each(halves, settle_exchange)

    @pl.when(pos < 2 * lines - 1)
    def _():
        chain_send().wait_send()


def per_device(shards, parts, tokens, decay_rate, angle, in_coef, out_coef, skip_coef, gate_weight, out_weight):
    rows, width = tokens.shape
    dims = decay_rate.shape[1]
    lines = shards // 4
    bw = gate_weight.shape[0]
    blk = 2 * bw
    chunks = width // blk
    assert shards % 4 == 0 and lines > 1 and dims % 2 == 0
    assert chunks % 2 == 0 and bw % LANES == 0 and chunks * 2 * parts == shards
    sub = chunks * bw // LANES
    two = 2 * rows
    depth = lines * blk
    core = lax.axis_index("seq") % 2

    def spread(table):
        table = table.reshape(chunks, 2, bw, dims)
        table = lax.dynamic_index_in_dim(table, core, 1, keepdims=False)
        return table.reshape(chunks * bw, dims).T.reshape(dims * sub, LANES)

    rate = spread(decay_rate)
    theta = spread(angle)
    magnitude = 1.0 - rate
    scaled = spread(in_coef) * jnp.sqrt(1.0 - magnitude * magnitude)
    c_re = scaled * spread(out_coef[0])
    c_im = scaled * spread(out_coef[1])
    q_re = magnitude * jnp.cos(theta)
    q_im = magnitude * jnp.sin(theta)
    span_mag = jnp.exp(two * jnp.log1p(-rate))
    span_re = span_mag * jnp.cos(two * theta)
    span_im = span_mag * jnp.sin(two * theta)
    skip = lax.dynamic_index_in_dim(skip_coef.reshape(chunks, 2, bw), core, 1, keepdims=False).reshape(sub, LANES)

    hbm = pl.BlockSpec(memory_space=pltpu.HBM)
    vmem = pl.BlockSpec(memory_space=pltpu.VMEM)
    dma = pltpu.SemaphoreType.DMA
    halves = chunks // 2
    n = 2 * parts
    flops = 2 * 2 * 4 * rows * depth * chunks * bw
    return pl.pallas_call(
        functools.partial(mixer_kernel, lines, parts, dims),
        in_specs=[hbm] * 3 + [vmem] * 7,
        out_specs=vmem,
        out_shape=jax.ShapeDtypeStruct((rows, width), BF16),
        scratch_shapes=[
            pltpu.VMEM((two, chunks * bw), BF16),
            pltpu.VMEM((two * sub, LANES), F32),
            pltpu.VMEM((two * sub, LANES), F32),
            pltpu.VMEM((2, dims * sub, LANES), F32),
            pltpu.VMEM((2, dims * sub, LANES), BF16),
            pltpu.VMEM((2, dims * sub, LANES), BF16),
            pltpu.VMEM((2, 4 * rows, depth), BF16),
            pltpu.VMEM((2, chunks, depth, bw), BF16),
            pltpu.VMEM((chunks, two, bw), F32),
            pltpu.VMEM((2, chunks, two, bw), BF16),
            pltpu.VMEM((2, chunks, two, bw), BF16),
            pltpu.VMEM((chunks, two, bw), BF16),
            pltpu.VMEM((chunks, rows, bw), BF16),
            dma((2, chunks)),
            dma((chunks,)),
            dma((halves,)),
            dma((2, chunks)),
            dma((2, chunks)),
            dma((chunks,)),
            dma((chunks,)),
            dma((2, 2, chunks, lines)),
            dma((2, chunks, lines)),
            dma((2, n, halves)),
            dma((2, n, halves)),
            dma((2, n, halves)),
            dma((2, n, halves)),
            dma((halves,)),
            dma,
            dma,
            dma((2, chunks)),
            dma((2, chunks)),
            dma((chunks,)),
            dma((chunks,)),
        ],
        compiler_params=pltpu.CompilerParams(
            collective_id=0, has_side_effects=True, vmem_limit_bytes=56 * 1024 * 1024
        ),
        cost_estimate=pl.CostEstimate(flops=flops, bytes_accessed=4 * tokens.size, transcendentals=0),
        name="mixer",
    )(
        tokens, gate_weight, out_weight, q_re, q_im, c_re, c_im, span_re, span_im, skip,
    )


def solution(mesh):
    in_specs = (
        P("seq", "tp"),
        P("tp", None),
        P("tp", None),
        P("tp", None),
        P(None, "tp", None),
        P("tp"),
        P("seq", "tp"),
        P("seq", "tp"),
    )
    body = functools.partial(per_device, mesh.shape["seq"], mesh.shape["tp"])
    return jax.shard_map(body, mesh=mesh, in_specs=in_specs, out_specs=P("seq", "tp"), check_vma=False)
```

```python
import functools

import jax
import jax.numpy as jnp
from jax import lax
from jax.experimental import pallas as pl
from jax.experimental.pallas import tpu as pltpu
from jax.sharding import PartitionSpec as P

LANES = 128
UNROLL = 8
MESH = pl.DeviceIdType.MESH
F32, BF16 = jnp.float32, jnp.bfloat16


def mixer_kernel(
    lines, parts, dims,
    tok, gate_w, out_w, decay, angle, in_coef, out_coef, skip_in,
    out_ref,
    raw, q_re_ref, q_im_ref, c_re_ref, c_im_ref, s_re_ref, s_im_ref, skip_ref, te, x2d, y2d, st, cin, cout, A, W, own, cs, cr, hid, ost,
    l_w, l_te, l_a, l_raw, sw_s, sw_r, te_s, te_r, z_s, z_r, x_s, x_r, p_s, p_r, po_s, ch_s, ch_r, c_s, c_r, o_s, o_r,
):
    rows, width = tok.shape
    bw = gate_w.shape[0]
    blk = 2 * bw
    chunks = width // blk
    halves = chunks // 2
    sub = chunks * bw // LANES
    tiles = bw // LANES
    two = 2 * rows

    s = lax.axis_index("seq")
    y = lax.axis_index("tp")
    z, x, c = s // 4, (s // 2) % 2, s % 2
    pos = z * 2 + x

    def dev(zz, xx, cc, yy):
        return ((zz * 2 + xx) * 2 + cc, yy)

    partner = dev(z, x, 1 - c, y)
    is_mid = (z > 0) & (z < lines - 1)

    def hint(v, m):
        return v if isinstance(v, int) else pl.multiple_of(v, m)

    def ds(start, size, m):
        return pl.ds(hint(start, m), size)

    def remote(src, dst, ssem, rsem, where):
        return pltpu.make_async_remote_copy(src, dst, ssem, rsem, device_id=where, device_id_type=MESH)

    weights = (gate_w, out_w)
    others = [(xx, yy) for yy in range(parts) for xx in range(2)]
    peers = others[1:]

    def w_local(w, j):
        return pltpu.make_async_copy(
            weights[w].at[:, ds(j * blk + c * bw, bw, bw)],
            W.at[w, j, ds(z * blk + c * bw, bw, bw)], l_w.at[w, j])

    def w_swap(w, j):
        return remote(
            weights[w].at[:, ds(j * blk + (1 - c) * bw, bw, bw)],
            W.at[w, j, ds(z * blk + c * bw, bw, bw)], sw_s.at[w, j], sw_r.at[w, j], partner)

    def te_local(j):
        return pltpu.make_async_copy(
            tok.at[:, ds(j * blk + c * bw, bw, bw)], te.at[ds(c * rows, rows, rows), ds(j * bw, bw, bw)], l_te.at[j])

    def raw_local(t, j):
        source = (decay, angle, in_coef, out_coef.at[0], out_coef.at[1])[t]
        return pltpu.make_async_copy(
            source.at[:, ds(j * blk + c * bw, bw, bw)], raw.at[t, :, ds(j * bw, bw, bw)], l_raw.at[t, j])

    def te_swap(j):
        return remote(
            tok.at[:, ds(j * blk + (1 - c) * bw, bw, bw)],
            te.at[ds(c * rows, rows, rows), ds(j * bw, bw, bw)], te_s.at[j], te_r.at[j], partner)

    def piece(w, j, o):
        return W.at[w, j, ds(o * blk, blk, blk)]

    def z_send(w, j, o, side):
        where = dev(z + (1 if side else -1), x, c, y)
        return remote(piece(w, j, o), piece(w, j, o), z_s.at[side, w, j, o], z_r.at[w, j, o], where)

    def at_peer(dx, dy):
        return (x + dx) % 2, (y + dy) % parts

    def a_cols(yy, jj):
        return ds((yy * halves + jj) * blk, blk, blk)

    def slot(dx, yy):
        return dx * parts + yy

    def t_send(dx, dy, jj):
        xx, yy = at_peer(dx, dy)
        return remote(
            tok.at[:, ds((2 * jj + xx) * blk, blk, blk)],
            A.at[0, ds((x * 2 + c) * rows, rows, rows), a_cols(y, jj)],
            x_s.at[0, dx * parts + dy, jj], x_r.at[0, slot(dx, y), jj], dev(z, xx, c, yy))

    def t_got(dx, dy, jj):
        xx, yy = at_peer(dx, dy)
        dst = A.at[0, ds((xx * 2 + c) * rows, rows, rows), a_cols(yy, jj)]
        return remote(dst, dst, x_s.at[0, dx * parts + dy, jj], x_r.at[0, slot(dx, yy), jj], dev(z, xx, c, yy))

    def t_local(jj):
        return pltpu.make_async_copy(
            tok.at[:, ds((2 * jj + x) * blk, blk, blk)],
            A.at[0, ds((x * 2 + c) * rows, rows, rows), a_cols(y, jj)], l_a.at[jj])

    def t_own(jj):
        return remote(
            tok.at[:, ds((2 * jj + x) * blk, blk, blk)],
            A.at[0, ds((x * 2 + c) * rows, rows, rows), a_cols(y, jj)],
            p_s.at[0, 0, jj], p_r.at[0, slot(0, y), jj], partner)

    def t_pass(dx, dy, jj):
        xx, yy = at_peer(dx, dy)
        ref = A.at[0, ds((xx * 2 + c) * rows, rows, rows), a_cols(yy, jj)]
        return remote(ref, ref, p_s.at[0, dx * parts + dy, jj], p_r.at[0, slot(dx, yy), jj], partner)

    def t_passed(dx, dy, jj):
        xx, yy = at_peer(dx, dy)
        ref = A.at[0, ds((xx * 2 + 1 - c) * rows, rows, rows), a_cols(yy, jj)]
        return remote(ref, ref, p_s.at[0, dx * parts + dy, jj], p_r.at[0, slot(dx, yy), jj], partner)

    def h_ref(xx, yy, jj, cc):
        cols = ds((yy * halves + jj) * blk + cc * bw, bw, bw)
        return A.at[1, ds(xx * two, two, two), cols]

    def h_send(dx, dy, jj, j):
        xx, yy = at_peer(dx, dy)
        return remote(
            hid.at[j], h_ref(x, y, jj, c), x_s.at[1, dx * parts + dy, jj], x_r.at[1, slot(dx, y), jj],
            dev(z, xx, c, yy))

    def h_got(dx, dy, jj):
        xx, yy = at_peer(dx, dy)
        ref = h_ref(xx, yy, jj, c)
        return remote(ref, ref, x_s.at[1, dx * parts + dy, jj], x_r.at[1, slot(dx, yy), jj], dev(z, xx, c, yy))

    def h_own(jj, j):
        return remote(hid.at[j], h_ref(x, y, jj, c), p_s.at[1, 0, jj], p_r.at[1, slot(0, y), jj], partner)

    def h_pass(dx, dy, jj):
        xx, yy = at_peer(dx, dy)
        ref = h_ref(xx, yy, jj, c)
        return remote(ref, ref, p_s.at[1, dx * parts + dy, jj], p_r.at[1, slot(dx, yy), jj], partner)

    def h_passed(dx, dy, jj):
        xx, yy = at_peer(dx, dy)
        ref = h_ref(xx, yy, jj, 1 - c)
        return remote(ref, ref, p_s.at[1, dx * parts + dy, jj], p_r.at[1, slot(dx, yy), jj], partner)

    def c_send(w, j):
        return remote(cs.at[w, j], cr.at[w, j], c_s.at[w, j], c_r.at[w, j], dev(z, 1 - x, c, y))

    def chain_send():
        nxt = pos + 1
        return remote(cout, cin, ch_s, ch_r, dev(nxt // 2, nxt % 2, c, y))

    def o_send(j):
        return remote(ost.at[j], out_ref.at[:, ds(j * blk + c * bw, bw, bw)], o_s.at[j], o_r.at[j], partner)

    def o_got(j):
        ref = out_ref.at[:, ds(j * blk + (1 - c) * bw, bw, bw)]
        return remote(ost.at[j], ref, o_s.at[j], o_r.at[j], partner)

    def each(n, f):
        def body(i, carry):
            f(i)
            return carry
        lax.fori_loop(0, n, body, 0)

    each(chunks, lambda j: w_local(0, j).start())
    each(chunks, lambda j: te_local(j).start())
    for t in range(5):
        each(chunks, lambda j: raw_local(t, j).start())
    each(halves, lambda jj: t_local(jj).start())
    each(chunks, lambda j: w_local(1, j).start())

    barrier = pltpu.get_barrier_semaphore()

    def greet(where):
        pl.semaphore_signal(barrier, inc=1, device_id=where, device_id_type=MESH)

    greet(partner)
    for dx, dy in peers:
        xx, yy = at_peer(dx, dy)
        greet(dev(z, xx, c, yy))
    line_peers = [
        (z > 0, dev(z - 1, x, c, y)),
        (z < lines - 1, dev(z + 1, x, c, y)),
        ((x == 1) & (z < lines - 1), dev(z + 1, 0, c, y)),
        ((x == 0) & (z > 0), dev(z - 1, 1, c, y)),
    ]
    for there, where in line_peers:
        @pl.when(there)
        def _():
            greet(where)
    pl.semaphore_wait(barrier, 1 + len(peers) + sum(there.astype(jnp.int32) for there, _ in line_peers))

    each(chunks, lambda j: w_swap(0, j).start())
    for dx, dy in peers:
        each(halves, lambda jj: t_send(dx, dy, jj).start())
    each(chunks, lambda j: te_swap(j).start())
    each(halves, lambda jj: t_own(jj).start())
    each(chunks, lambda j: w_swap(1, j).start())

    def own_ready(w, j):
        w_local(w, j).wait()
        w_swap(w, j).wait_recv()

    def own_send(w, j):
        @pl.when(z > 0)
        def _():
            z_send(w, j, z, 0).start()

        @pl.when(z < lines - 1)
        def _():
            z_send(w, j, z, 1).start()

    def forward(w, j, d):
        @pl.when(is_mid & (z + d < lines))
        def _():
            z_send(w, j, z + d, 0).wait_recv()
            z_send(w, j, z + d, 0).start()

        @pl.when(is_mid & (z - d >= 0))
        def _():
            z_send(w, j, z - d, 1).wait_recv()
            z_send(w, j, z - d, 1).start()

    def at_end(w, j):
        for d in range(1, lines):
            @pl.when(z == 0)
            def _():
                z_send(w, j, d, 0).wait_recv()

            @pl.when(z == lines - 1)
            def _():
                z_send(w, j, lines - 1 - d, 0).wait_recv()

    def first_sends(j):
        own_ready(0, j)
        own_send(0, j)

    each(chunks, first_sends)

    for t in range(5):
        each(chunks, lambda j: raw_local(t, j).wait())
    for e in range(sub):
        band = slice(e * LANES, (e + 1) * LANES)
        rate, theta, scale, o_re, o_im = (raw[t, :, band] for t in range(5))
        magnitude = 1.0 - rate
        scale = scale * jnp.sqrt(1.0 - magnitude * magnitude)
        at = pl.ds(e, dims, stride=sub)
        c_re_ref[at, :] = scale * o_re
        c_im_ref[at, :] = scale * o_im
        q_re_ref[at, :] = magnitude * jnp.cos(theta)
        q_im_ref[at, :] = magnitude * jnp.sin(theta)
        k, lane = e // tiles, e % tiles
        row = 2 * k * tiles + lane
        skip_ref[e:e + 1, :] = jnp.where(c == 0, skip_in[row:row + 1, :], skip_in[row + tiles:row + tiles + 1, :])

    def span_of():
        base = q_re_ref[...], q_im_ref[...]
        total = None
        count = two
        while count:
            if count % 2:
                total = base if total is None else (
                    total[0] * base[0] - total[1] * base[1], total[0] * base[1] + total[1] * base[0])
            base = base[0] * base[0] - base[1] * base[1], 2.0 * base[0] * base[1]
            count //= 2
        s_re_ref[...] = total[0]
        s_im_ref[...] = total[1]

    span_of()

    def te_ready(j):
        te_local(j).wait()
        te_swap(j).wait_recv()

    each(chunks, te_ready)

    def lay(i, carry):
        for e in range(sub):
            v = te[pl.ds(i * 16, 16), e * LANES:(e + 1) * LANES].astype(F32)
            x2d[pl.ds(i * 16 * sub + e, 16, stride=sub), :] = v
        return carry

    lax.fori_loop(0, two // 16, lay, 0)

    def second_own(j):
        own_ready(1, j)

        @pl.when(jnp.logical_not(is_mid))
        def _():
            own_send(1, j)

    each(chunks, second_own)

    half = dims // 2

    def tile(ref, h):
        return ref[h * sub:(h + 1) * sub, :]

    def step(state, v, q_re, q_im):
        return [(a * re - b * im + v, a * im + b * re) for (re, im), a, b in zip(state, q_re, q_im)]

    def end_half(k):
        hs = range(k * half, (k + 1) * half)
        q_re = [tile(q_re_ref, h) for h in hs]
        q_im = [tile(q_im_ref, h) for h in hs]
        zero = jnp.zeros((sub, LANES), F32)

        def body(i, state):
            for u in range(UNROLL):
                state = step(state, x2d[ds((i * UNROLL + u) * sub, sub, sub), :], q_re, q_im)
            return state

        state = lax.fori_loop(0, two // UNROLL, body, [(zero, zero)] * half)
        for h, (re, im) in zip(hs, state):
            st[0, h * sub:(h + 1) * sub, :] = re
            st[1, h * sub:(h + 1) * sub, :] = im

    end_half(0)
    each(chunks, lambda j: forward(0, j, 1))
    end_half(1)

    def tokens_on(dx, dy):
        def go(jj):
            t_got(dx, dy, jj).wait_recv()
            t_pass(dx, dy, jj).start()
        each(halves, go)

    @pl.when(pos == 0)
    def _():
        cin[...] = jnp.zeros_like(cin)

    @pl.when(pos > 0)
    def _():
        chain_send().wait_recv()

    i_re, i_im = cin[0].astype(F32), cin[1].astype(F32)
    a, b = s_re_ref[...], s_im_ref[...]
    cout[0] = (a * i_re - b * i_im + st[0]).astype(BF16)
    cout[1] = (a * i_im + b * i_re + st[1]).astype(BF16)
    st[0] = i_re
    st[1] = i_im

    @pl.when(pos < 2 * lines - 1)
    def _():
        chain_send().start()

    for dx, dy in peers:
        tokens_on(dx, dy)

    def smooth_half(k):
        hs = range(k * half, (k + 1) * half)
        q_re = [tile(q_re_ref, h) for h in hs]
        q_im = [tile(q_im_ref, h) for h in hs]
        c_re = [tile(c_re_ref, h) for h in hs]
        c_im = [tile(c_im_ref, h) for h in hs]
        skip = skip_ref[...]
        state = [(tile(st.at[0], h), tile(st.at[1], h)) for h in hs]

        def body(i, state):
            for u in range(UNROLL):
                at = ds((i * UNROLL + u) * sub, sub, sub)
                v = x2d[at, :]
                state = step(state, v, q_re, q_im)
                sums = [c_re[h] * state[h][0] - c_im[h] * state[h][1] for h in range(half)]
                while len(sums) > 1:
                    sums = [sum(sums[m:m + 2]) for m in range(0, len(sums), 2)]
                before = v * skip if k == 0 else y2d[at, :]
                y2d[at, :] = before + sums[0]
            return state

        lax.fori_loop(0, two // UNROLL, body, state)

    smooth_half(0)
    for d in range(2, lines - 1):
        each(halves, lambda j: forward(0, j, d))
    smooth_half(1)
    for d in range(2, lines - 1):
        each(halves, lambda j: forward(0, halves + j, d))

    def mid_own(j):
        @pl.when(is_mid)
        def _():
            own_send(1, j)

    def stage(j):
        for d in range(1, lines - 1):
            forward(1, j, d)

    each(halves, mid_own)

    def local_tokens(jj):
        t_local(jj).wait()
        for dx, dy in others:
            t_passed(dx, dy, jj).wait_recv()

    each(halves, local_tokens)

    def project(w, j):
        @pl.when(jnp.logical_not(is_mid))
        def _():
            at_end(w, j)
        right = W[w, j]
        away = jnp.dot(A[w, ds((1 - x) * two, two, two), :], right, preferred_element_type=F32)
        cs[w, j] = away.astype(BF16)
        c_send(w, j).start()
        own[j] = jnp.dot(A[w, ds(x * two, two, two), :], right, preferred_element_type=F32)

    each(chunks, lambda j: project(0, j))
    stage(0)

    def hidden(j):
        c_send(0, j).wait_recv()
        jj = j // 2
        target = j % 2

        def band(i, carry):
            at = pl.ds(pl.multiple_of(i * 16, 16), 16)
            for e in range(tiles):
                lane = slice(e * LANES, (e + 1) * LANES)
                smooth = y2d[pl.ds(i * 16 * sub + j * tiles + e, 16, stride=sub), :]
                gate = own[j, at, lane] + cr[0, j, at, lane].astype(F32)
                value = smooth * jax.nn.sigmoid(smooth) * jax.nn.sigmoid(gate)
                hid[j, at, lane] = value.astype(BF16)
            return carry

        lax.fori_loop(0, two // 16, band, 0)

        @pl.when(target == x)
        def _():
            h_own(jj, j).start()
            for dx, dy in peers:
                if dx == 0:
                    h_send(dx, dy, jj, j).start()
            h_ref(x, y, jj, c)[...] = hid[j]

        @pl.when(target != x)
        def _():
            for dx, dy in peers:
                if dx == 1:
                    h_send(dx, dy, jj, j).start()

    each(halves, hidden)
    stage(1)
    each(halves, lambda j: mid_own(halves + j))
    each(halves, lambda j: hidden(halves + j))

    for dx, dy in peers:
        def hidden_on(jj):
            h_got(dx, dy, jj).wait_recv()
            h_pass(dx, dy, jj).start()
        each(halves, hidden_on)
    each(chunks - 2, lambda j: stage(2 + j))

    def all_hidden(jj):
        for dx, dy in others:
            h_passed(dx, dy, jj).wait_recv()

    each(halves, all_hidden)

    def finish(j):
        c_send(1, j).wait_recv()
        mine = ds(c * rows, rows, rows)
        theirs = ds((1 - c) * rows, rows, rows)
        ost[j] = (own[j, theirs, :] + cr[1, j, theirs, :].astype(F32)).astype(BF16)
        o_send(j).start()
        out_ref[:, ds(j * blk + c * bw, bw, bw)] = (own[j, mine, :] + cr[1, j, mine, :].astype(F32)).astype(BF16)

    project(1, 0)

    def last(j):
        project(1, j + 1)
        finish(j)

    each(chunks - 1, last)
    finish(chunks - 1)
    each(chunks, lambda j: o_got(j).wait_recv())

    def settle(j):
        for w in range(2):
            w_swap(w, j).wait_send()
            c_send(w, j).wait_send()

            @pl.when(z > 0)
            def _():
                z_send(w, j, z, 0).wait_send()

            @pl.when(z < lines - 1)
            def _():
                z_send(w, j, z, 1).wait_send()
            for d in range(1, lines - 1):
                @pl.when(is_mid & (z + d < lines))
                def _():
                    z_send(w, j, z + d, 0).wait_send()

                @pl.when(is_mid & (z - d >= 0))
                def _():
                    z_send(w, j, z - d, 1).wait_send()
        te_swap(j).wait_send()
        o_send(j).wait_send()

    each(chunks, settle)

    def settle_exchange(jj):
        t_own(jj).wait_send()
        h_own(jj, 0).wait_send()
        for dx, dy in peers:
            t_send(dx, dy, jj).wait_send()
            h_send(dx, dy, jj, 0).wait_send()
            t_pass(dx, dy, jj).wait_send()
            h_pass(dx, dy, jj).wait_send()

    each(halves, settle_exchange)

    @pl.when(pos < 2 * lines - 1)
    def _():
        chain_send().wait_send()


def per_device(shards, parts, tokens, decay_rate, angle, in_coef, out_coef, skip_coef, gate_weight, out_weight):
    rows, width = tokens.shape
    dims = decay_rate.shape[1]
    lines = shards // 4
    bw = gate_weight.shape[0]
    blk = 2 * bw
    chunks = width // blk
    assert shards % 4 == 0 and lines > 1 and dims % 2 == 0
    assert chunks % 2 == 0 and bw % LANES == 0 and chunks * 2 * parts == shards
    sub = chunks * bw // LANES
    two = 2 * rows
    depth = lines * blk
    skip = skip_coef.reshape(2 * sub, LANES)

    hbm = pl.BlockSpec(memory_space=pltpu.HBM)
    vmem = pl.BlockSpec(memory_space=pltpu.VMEM)
    dma = pltpu.SemaphoreType.DMA
    halves = chunks // 2
    n = 2 * parts
    flops = 2 * 2 * 4 * rows * depth * chunks * bw
    return pl.pallas_call(
        functools.partial(mixer_kernel, lines, parts, dims),
        in_specs=[hbm] * 7 + [vmem],
        out_specs=vmem,
        out_shape=jax.ShapeDtypeStruct((rows, width), BF16),
        scratch_shapes=[
            pltpu.VMEM((5, dims, chunks * bw), F32),
        ] + [pltpu.VMEM((dims * sub, LANES), F32)] * 6 + [
            pltpu.VMEM((sub, LANES), F32),
            pltpu.VMEM((two, chunks * bw), BF16),
            pltpu.VMEM((two * sub, LANES), F32),
            pltpu.VMEM((two * sub, LANES), F32),
            pltpu.VMEM((2, dims * sub, LANES), F32),
            pltpu.VMEM((2, dims * sub, LANES), BF16),
            pltpu.VMEM((2, dims * sub, LANES), BF16),
            pltpu.VMEM((2, 4 * rows, depth), BF16),
            pltpu.VMEM((2, chunks, depth, bw), BF16),
            pltpu.VMEM((chunks, two, bw), F32),
            pltpu.VMEM((2, chunks, two, bw), BF16),
            pltpu.VMEM((2, chunks, two, bw), BF16),
            pltpu.VMEM((chunks, two, bw), BF16),
            pltpu.VMEM((chunks, rows, bw), BF16),
            dma((2, chunks)),
            dma((chunks,)),
            dma((halves,)),
            dma((5, chunks)),
            dma((2, chunks)),
            dma((2, chunks)),
            dma((chunks,)),
            dma((chunks,)),
            dma((2, 2, chunks, lines)),
            dma((2, chunks, lines)),
            dma((2, n, halves)),
            dma((2, n, halves)),
            dma((2, n, halves)),
            dma((2, n, halves)),
            dma((halves,)),
            dma,
            dma,
            dma((2, chunks)),
            dma((2, chunks)),
            dma((chunks,)),
            dma((chunks,)),
        ],
        compiler_params=pltpu.CompilerParams(
            collective_id=0, has_side_effects=True, vmem_limit_bytes=56 * 1024 * 1024
        ),
        cost_estimate=pl.CostEstimate(flops=flops, bytes_accessed=4 * tokens.size, transcendentals=0),
        name="mixer",
    )(
        tokens, gate_weight, out_weight, decay_rate.T, angle.T, in_coef.T, out_coef.swapaxes(1, 2), skip,
    )


def solution(mesh):
    in_specs = (
        P("seq", "tp"),
        P("tp", None),
        P("tp", None),
        P("tp", None),
        P(None, "tp", None),
        P("tp"),
        P("seq", "tp"),
        P("seq", "tp"),
    )
    body = functools.partial(per_device, mesh.shape["seq"], mesh.shape["tp"])
    return jax.shard_map(body, mesh=mesh, in_specs=in_specs, out_specs=P("seq", "tp"), check_vma=False)
```

```python
import functools

import jax
import jax.numpy as jnp
from jax import lax
from jax.experimental import pallas as pl
from jax.experimental.pallas import tpu as pltpu
from jax.sharding import PartitionSpec as P

LANES = 128
UNROLL = 8
GUESTS = 2
MESH = pl.DeviceIdType.MESH
F32, BF16 = jnp.float32, jnp.bfloat16


def mixer_kernel(
    lines, parts, dims, guests,
    tok, gate_w, out_w, decay, angle, in_coef, out_coef, skip_in,
    out_ref,
    raw, q_re_ref, q_im_ref, c_re_ref, c_im_ref, s_re_ref, s_im_ref, skip_ref, te, x2d, y2d, st, cin, cout, A, W, own, own_g, cs, cr, hid, ost, G, bs,
    l_w, l_te, l_a, l_raw, sw_s, sw_r, te_s, te_r, z_s, z_r, x_s, x_r, p_s, p_r, g_s, g_r, b_s, ch_s, ch_r, c_s, c_r, o_s, o_r,
):
    rows, width = tok.shape
    bw = gate_w.shape[0]
    blk = 2 * bw
    chunks = width // blk
    halves = chunks // 2
    sub = chunks * bw // LANES
    tiles = bw // LANES
    two = 2 * rows

    s = lax.axis_index("seq")
    y = lax.axis_index("tp")
    z, x, c = s // 4, (s // 2) % 2, s % 2
    pos = z * 2 + x

    def dev(zz, xx, cc, yy):
        return ((zz * 2 + xx) * 2 + cc, yy)

    partner = dev(z, x, 1 - c, y)
    is_mid = (z > 0) & (z < lines - 1)
    is_end = jnp.logical_not(is_mid)
    is_host = (z == 1) | (z == lines - 2)
    end_z = jnp.where(z == 1, 0, lines - 1)
    host_z = jnp.where(z == 0, 1, lines - 2)

    def hint(v, m):
        return v if isinstance(v, int) else pl.multiple_of(v, m)

    def ds(start, size, m):
        return pl.ds(hint(start, m), size)

    def remote(src, dst, ssem, rsem, where):
        return pltpu.make_async_remote_copy(src, dst, ssem, rsem, device_id=where, device_id_type=MESH)

    weights = (gate_w, out_w)
    others = [(xx, yy) for yy in range(parts) for xx in range(2)]
    peers = others[1:]

    def w_local(w, j):
        return pltpu.make_async_copy(
            weights[w].at[:, ds(j * blk + c * bw, bw, bw)],
            W.at[w, j, ds(z * blk + c * bw, bw, bw)], l_w.at[w, j])

    def w_swap(w, j):
        return remote(
            weights[w].at[:, ds(j * blk + (1 - c) * bw, bw, bw)],
            W.at[w, j, ds(z * blk + c * bw, bw, bw)], sw_s.at[w, j], sw_r.at[w, j], partner)

    def te_local(j):
        return pltpu.make_async_copy(
            tok.at[:, ds(j * blk + c * bw, bw, bw)], te.at[ds(c * rows, rows, rows), ds(j * bw, bw, bw)], l_te.at[j])

    def raw_local(t, j):
        source = (decay, angle, in_coef, out_coef.at[0], out_coef.at[1])[t]
        return pltpu.make_async_copy(
            source.at[:, ds(j * blk + c * bw, bw, bw)], raw.at[t, :, ds(j * bw, bw, bw)], l_raw.at[t, j])

    def te_swap(j):
        return remote(
            tok.at[:, ds(j * blk + (1 - c) * bw, bw, bw)],
            te.at[ds(c * rows, rows, rows), ds(j * bw, bw, bw)], te_s.at[j], te_r.at[j], partner)

    def piece(w, j, o):
        return W.at[w, j, ds(o * blk, blk, blk)]

    def z_send(w, j, o, side):
        where = dev(z + (1 if side else -1), x, c, y)
        return remote(piece(w, j, o), piece(w, j, o), z_s.at[side, w, j, o], z_r.at[w, j, o], where)

    def at_peer(dx, dy):
        return (x + dx) % 2, (y + dy) % parts

    def a_cols(yy, jj):
        return ds((yy * halves + jj) * blk, blk, blk)

    def slot(dx, yy):
        return dx * parts + yy

    def t_from(g, block):
        return (G if g else tok).at[:, ds(block * blk, blk, blk)]

    def t_ref(g, xx, cc, yy, jj):
        return A.at[g, ds((xx * 2 + cc) * rows, rows, rows), a_cols(yy, jj)]

    def t_send(g, dx, dy, jj):
        xx, yy = at_peer(dx, dy)
        return remote(
            t_from(g, 2 * jj + xx), t_ref(g, x, c, y, jj),
            x_s.at[g, dx * parts + dy, jj], x_r.at[g, slot(dx, y), jj], dev(z, xx, c, yy))

    def t_relay(g, dy, jj):
        xx, yy = at_peer(1, dy)
        ref = t_ref(g, xx, c, y, jj)
        return remote(ref, ref, x_s.at[g, parts + dy, jj], x_r.at[g, slot(1, y), jj], dev(z, x, c, yy))

    def t_got(g, dx, dy, jj):
        xx, yy = at_peer(dx, dy)
        ref = t_ref(g, xx, c, yy, jj)
        return remote(ref, ref, x_s.at[g, dx * parts + dy, jj], x_r.at[g, slot(dx, yy), jj], partner)

    def t_local(jj):
        return pltpu.make_async_copy(t_from(0, 2 * jj + x), t_ref(0, x, c, y, jj), l_a.at[jj])

    def t_own(g, jj):
        return remote(
            t_from(g, 2 * jj + x), t_ref(g, x, c, y, jj), p_s.at[g, 0, jj], p_r.at[g, slot(0, y), jj], partner)

    def t_pass(g, dx, dy, jj):
        xx, yy = at_peer(dx, dy)
        ref = t_ref(g, xx, c, yy, jj)
        return remote(ref, ref, p_s.at[g, dx * parts + dy, jj], p_r.at[g, slot(dx, yy), jj], partner)

    def t_passed(g, dx, dy, jj):
        xx, yy = at_peer(dx, dy)
        ref = t_ref(g, xx, 1 - c, yy, jj)
        return remote(ref, ref, p_s.at[g, dx * parts + dy, jj], p_r.at[g, slot(dx, yy), jj], partner)

    def g_send(k):
        ref = G.at[:, ds(k * blk, blk, blk)]
        return remote(t_from(0, k), ref, g_s.at[k], g_r.at[k], dev(host_z, x, c, y))

    def back_send(j):
        return remote(bs.at[j], cr.at[0, j], b_s.at[j], c_r.at[0, j], dev(end_z, x, c, y))

    def h_ref(xx, yy, jj, cc):
        cols = ds((yy * halves + jj) * blk + cc * bw, bw, bw)
        return A.at[1, ds(xx * two, two, two), cols]

    def h_send(dx, dy, jj, j):
        xx, yy = at_peer(dx, dy)
        return remote(
            hid.at[j], h_ref(x, y, jj, c), x_s.at[1, dx * parts + dy, jj], x_r.at[1, slot(dx, y), jj],
            dev(z, xx, c, yy))

    def h_got(dx, dy, jj):
        xx, yy = at_peer(dx, dy)
        ref = h_ref(xx, yy, jj, c)
        return remote(ref, ref, x_s.at[1, dx * parts + dy, jj], x_r.at[1, slot(dx, yy), jj], dev(z, xx, c, yy))

    def h_relay(dy, jj):
        xx, yy = at_peer(1, dy)
        ref = h_ref(xx, y, jj, c)
        return remote(ref, ref, x_s.at[1, parts + dy, jj], x_r.at[1, slot(1, y), jj], dev(z, x, c, yy))

    def h_own(jj, j):
        return remote(hid.at[j], h_ref(x, y, jj, c), p_s.at[1, 0, jj], p_r.at[1, slot(0, y), jj], partner)

    def h_pass(dx, dy, jj):
        xx, yy = at_peer(dx, dy)
        ref = h_ref(xx, yy, jj, c)
        return remote(ref, ref, p_s.at[1, dx * parts + dy, jj], p_r.at[1, slot(dx, yy), jj], partner)

    def h_passed(dx, dy, jj):
        xx, yy = at_peer(dx, dy)
        ref = h_ref(xx, yy, jj, 1 - c)
        return remote(ref, ref, p_s.at[1, dx * parts + dy, jj], p_r.at[1, slot(dx, yy), jj], partner)

    def c_send(w, j):
        return remote(cs.at[w, j], cr.at[w, j], c_s.at[w, j], c_r.at[w, j], dev(z, 1 - x, c, y))

    def chain_send():
        nxt = pos + 1
        return remote(cout, cin, ch_s, ch_r, dev(nxt // 2, nxt % 2, c, y))

    def o_send(j):
        return remote(ost.at[j], out_ref.at[:, ds(j * blk + c * bw, bw, bw)], o_s.at[j], o_r.at[j], partner)

    def o_got(j):
        ref = out_ref.at[:, ds(j * blk + (1 - c) * bw, bw, bw)]
        return remote(ost.at[j], ref, o_s.at[j], o_r.at[j], partner)

    def each(n, f):
        def body(i, carry):
            f(i)
            return carry
        lax.fori_loop(0, n, body, 0)

    each(chunks, lambda j: w_local(0, j).start())
    each(chunks, lambda j: te_local(j).start())
    for t in range(5):
        each(chunks, lambda j: raw_local(t, j).start())
    each(halves, lambda jj: t_local(jj).start())
    each(chunks, lambda j: w_local(1, j).start())

    barrier = pltpu.get_barrier_semaphore()

    def greet(where):
        pl.semaphore_signal(barrier, inc=1, device_id=where, device_id_type=MESH)

    greet(partner)
    for dx, dy in peers:
        xx, yy = at_peer(dx, dy)
        greet(dev(z, xx, c, yy))
    line_peers = [
        (z > 0, dev(z - 1, x, c, y)),
        (z < lines - 1, dev(z + 1, x, c, y)),
        ((x == 1) & (z < lines - 1), dev(z + 1, 0, c, y)),
        ((x == 0) & (z > 0), dev(z - 1, 1, c, y)),
    ]
    for there, where in line_peers:
        @pl.when(there)
        def _():
            greet(where)
    pl.semaphore_wait(barrier, 1 + len(peers) + sum(there.astype(jnp.int32) for there, _ in line_peers))

    each(chunks, lambda j: w_swap(0, j).start())

    @pl.when(is_end)
    def _():
        each(chunks, lambda k: g_send(k).start())

    def t_start(g):
        def go(jj):
            t_send(g, 1, 0, jj).start()
            for dy in range(1, parts):
                t_send(g, 0, dy, jj).start()
            t_own(g, jj).start()
        each(halves, go)

    t_start(0)
    each(chunks, lambda j: te_swap(j).start())
    each(chunks, lambda j: w_swap(1, j).start())

    def own_ready(w, j):
        w_local(w, j).wait()
        w_swap(w, j).wait_recv()

    def wanted(w, j, side):
        target = z + (1 if side else -1)
        inside = (target >= 0) & (target < lines)
        if w == 0:
            inside = inside & (((target > 0) & (target < lines - 1)) | (j >= guests))
        return inside

    def outer_side(side):
        target = z + (1 if side else -1)
        return is_end | (target == 0) | (target == lines - 1)

    def own_outer(w, j):
        for side in range(2):
            @pl.when(wanted(w, j, side) & outer_side(side))
            def _():
                z_send(w, j, z, side).start()

    def own_inner(w, j):
        for side in range(2):
            @pl.when(wanted(w, j, side) & jnp.logical_not(outer_side(side)))
            def _():
                z_send(w, j, z, side).start()

    def hop(w, j, o, side, there):
        @pl.when(there)
        def _():
            z_send(w, j, o, side).wait_recv()

            @pl.when(wanted(w, j, side))
            def _():
                z_send(w, j, o, side).start()

    def relay_cases(d, from_end):
        low, high = z - d, z + d
        if d == 1:
            at_low = (low == 0) if from_end else (low > 0)
            at_high = (high == lines - 1) if from_end else (high < lines - 1)
        else:
            at_low, at_high = low >= 0, high < lines
        return (low, 1, is_mid & at_low), (high, 0, is_mid & at_high)

    def forward_end(w, j):
        for o, side, there in relay_cases(1, True):
            hop(w, j, o, side, there)

    def forward(w, j, d):
        for o, side, there in relay_cases(d, False):
            hop(w, j, o, side, there)

    def forward_far(w, j):
        for d in range(2, lines - 1):
            forward(w, j, d)

    def at_end(w, j):
        for d in range(1, lines):
            @pl.when(z == 0)
            def _():
                z_send(w, j, d, 0).wait_recv()

            @pl.when(z == lines - 1)
            def _():
                z_send(w, j, lines - 1 - d, 0).wait_recv()

    def first_sends(j):
        own_ready(0, j)
        own_outer(0, j)
        own_inner(0, j)

    each(chunks, first_sends)

    for t in range(5):
        each(chunks, lambda j: raw_local(t, j).wait())
    for e in range(sub):
        band = slice(e * LANES, (e + 1) * LANES)
        rate, theta, scale, o_re, o_im = (raw[t, :, band] for t in range(5))
        magnitude = 1.0 - rate
        scale = scale * jnp.sqrt(1.0 - magnitude * magnitude)
        at = pl.ds(e, dims, stride=sub)
        c_re_ref[at, :] = scale * o_re
        c_im_ref[at, :] = scale * o_im
        q_re_ref[at, :] = magnitude * jnp.cos(theta)
        q_im_ref[at, :] = magnitude * jnp.sin(theta)
        k, lane = e // tiles, e % tiles
        row = 2 * k * tiles + lane
        skip_ref[e:e + 1, :] = jnp.where(c == 0, skip_in[row:row + 1, :], skip_in[row + tiles:row + tiles + 1, :])

    def span_of():
        base = q_re_ref[...], q_im_ref[...]
        total = None
        count = two
        while count:
            if count % 2:
                total = base if total is None else (
                    total[0] * base[0] - total[1] * base[1], total[0] * base[1] + total[1] * base[0])
            base = base[0] * base[0] - base[1] * base[1], 2.0 * base[0] * base[1]
            count //= 2
        s_re_ref[...] = total[0]
        s_im_ref[...] = total[1]

    span_of()

    def te_ready(j):
        te_local(j).wait()
        te_swap(j).wait_recv()

    each(chunks, te_ready)

    def lay(i, carry):
        for e in range(sub):
            v = te[pl.ds(i * 16, 16), e * LANES:(e + 1) * LANES].astype(F32)
            x2d[pl.ds(i * 16 * sub + e, 16, stride=sub), :] = v
        return carry

    lax.fori_loop(0, two // 16, lay, 0)

    def second_own(j):
        own_ready(1, j)
        own_outer(1, j)

    each(chunks, second_own)
    each(halves, lambda j: own_inner(1, j))

    half = dims // 2

    def tile(ref, h):
        return ref[h * sub:(h + 1) * sub, :]

    def step(state, v, q_re, q_im):
        return [(a * re - b * im + v, a * im + b * re) for (re, im), a, b in zip(state, q_re, q_im)]

    def end_half(k):
        hs = range(k * half, (k + 1) * half)
        q_re = [tile(q_re_ref, h) for h in hs]
        q_im = [tile(q_im_ref, h) for h in hs]
        zero = jnp.zeros((sub, LANES), F32)

        def body(i, state):
            for u in range(UNROLL):
                state = step(state, x2d[ds((i * UNROLL + u) * sub, sub, sub), :], q_re, q_im)
            return state

        state = lax.fori_loop(0, two // UNROLL, body, [(zero, zero)] * half)
        for h, (re, im) in zip(hs, state):
            st[0, h * sub:(h + 1) * sub, :] = re
            st[1, h * sub:(h + 1) * sub, :] = im

    def took_x(g):
        def go(jj):
            t_got(g, 1, 0, jj).wait_recv()
            for dy in range(1, parts):
                t_relay(g, dy, jj).start()
            t_pass(g, 1, 0, jj).start()
        each(halves, go)

    def took_y(g, dx):
        def go(jj):
            for dy in range(1, parts):
                t_got(g, dx, dy, jj).wait_recv()
                t_pass(g, dx, dy, jj).start()
        each(halves, go)

    end_half(0)
    took_x(0)
    end_half(1)

    @pl.when(pos == 0)
    def _():
        cin[...] = jnp.zeros_like(cin)

    @pl.when(pos > 0)
    def _():
        chain_send().wait_recv()

    i_re, i_im = cin[0].astype(F32), cin[1].astype(F32)
    a, b = s_re_ref[...], s_im_ref[...]
    cout[0] = (a * i_re - b * i_im + st[0]).astype(BF16)
    cout[1] = (a * i_im + b * i_re + st[1]).astype(BF16)
    st[0] = i_re
    st[1] = i_im

    @pl.when(pos < 2 * lines - 1)
    def _():
        chain_send().start()

    took_y(0, 0)

    @pl.when(is_host)
    def _():
        each(chunks, lambda k: g_send(k).wait_recv())
        t_start(2)

        def keep(jj):
            t_ref(2, x, c, y, jj)[...] = t_from(2, 2 * jj + x)[...]
        each(halves, keep)

    def smooth_half(k):
        hs = range(k * half, (k + 1) * half)
        q_re = [tile(q_re_ref, h) for h in hs]
        q_im = [tile(q_im_ref, h) for h in hs]
        c_re = [tile(c_re_ref, h) for h in hs]
        c_im = [tile(c_im_ref, h) for h in hs]
        skip = skip_ref[...]
        state = [(tile(st.at[0], h), tile(st.at[1], h)) for h in hs]

        def body(i, state):
            for u in range(UNROLL):
                at = ds((i * UNROLL + u) * sub, sub, sub)
                v = x2d[at, :]
                state = step(state, v, q_re, q_im)
                sums = [c_re[h] * state[h][0] - c_im[h] * state[h][1] for h in range(half)]
                while len(sums) > 1:
                    sums = [sum(sums[m:m + 2]) for m in range(0, len(sums), 2)]
                before = v * skip if k == 0 else y2d[at, :]
                y2d[at, :] = before + sums[0]
            return state

        lax.fori_loop(0, two // UNROLL, body, state)

    smooth_half(0)
    took_y(0, 1)
    each(chunks, lambda j: forward(0, j, 1))
    smooth_half(1)
    each(halves, lambda j: forward(1, j, 1))

    @pl.when(is_host)
    def _():
        took_x(2)
        took_y(2, 0)

    def all_tokens(g):
        def go(jj):
            for dx, dy in others:
                t_passed(g, dx, dy, jj).wait_recv()
        each(halves, go)

    each(halves, lambda jj: t_local(jj).wait())
    all_tokens(0)

    def multiply(w, g, k, j, mine):
        right = W[w, j]
        away = jnp.dot(A[g, ds((1 - x) * two, two, two), :], right, preferred_element_type=F32)
        cs[k, j] = away.astype(BF16)
        c_send(k, j).start()
        mine[j] = jnp.dot(A[g, ds(x * two, two, two), :], right, preferred_element_type=F32)

    def project(j):
        forward_far(0, j)

        @pl.when(is_end & (j >= guests))
        def _():
            at_end(0, j)

        @pl.when(is_mid | (j >= guests))
        def _():
            multiply(0, 0, 0, j, own)

        @pl.when(is_end & (j < guests))
        def _():
            own[j] = jnp.zeros((two, bw), F32)

    each(halves, lambda j: forward_end(0, j))

    def first_project(j):
        @pl.when(halves + j < chunks)
        def _():
            forward_end(0, halves + j)
        project(j)

    each(guests, first_project)

    @pl.when(is_host)
    def _():
        took_y(2, 1)
        all_tokens(2)
        each(guests, lambda j: multiply(0, 2, 2, j, own_g))

    def guest_back(j):
        @pl.when(is_host)
        def _():
            c_send(2, j).wait_recv()
            bs[j] = (own_g[j] + cr[2, j].astype(F32)).astype(BF16)
            back_send(j).start()

    def later_project(j):
        @pl.when((halves + j >= halves + guests) & (halves + j < chunks))
        def _():
            forward_end(0, halves + j)
        project(j)

    each(1, guest_back)
    lax.fori_loop(guests, chunks, lambda j, n: (later_project(j), n)[1], 0)
    lax.fori_loop(1, guests, lambda j, n: (guest_back(j), n)[1], 0)
    each(halves, lambda j: forward_end(1, j))
    own_inner(1, halves)

    def hidden(j):
        c_send(0, j).wait_recv()
        jj = j // 2
        target = j % 2

        def band(i, carry):
            at = pl.ds(pl.multiple_of(i * 16, 16), 16)
            for e in range(tiles):
                lane = slice(e * LANES, (e + 1) * LANES)
                smooth = y2d[pl.ds(i * 16 * sub + j * tiles + e, 16, stride=sub), :]
                gate = own[j, at, lane] + cr[0, j, at, lane].astype(F32)
                value = smooth * jax.nn.sigmoid(smooth) * jax.nn.sigmoid(gate)
                hid[j, at, lane] = value.astype(BF16)
            return carry

        lax.fori_loop(0, two // 16, band, 0)

        @pl.when(target == x)
        def _():
            h_own(jj, j).start()
            for dy in range(1, parts):
                h_send(0, dy, jj, j).start()
            h_ref(x, y, jj, c)[...] = hid[j]

        @pl.when(target != x)
        def _():
            h_send(1, 0, jj, j).start()

    each(halves, hidden)
    forward_end(1, halves)
    lax.fori_loop(halves + 1, chunks, lambda j, n: (own_inner(1, j), n)[1], 0)
    each(halves, lambda j: hidden(halves + j))
    lax.fori_loop(halves + 1, chunks, lambda j, n: (forward_end(1, j), n)[1], 0)

    def hidden_x(jj):
        h_got(1, 0, jj).wait_recv()
        for dy in range(1, parts):
            h_relay(dy, jj).start()
        h_pass(1, 0, jj).start()

    def hidden_y(dx):
        def go(jj):
            for dy in range(1, parts):
                h_got(dx, dy, jj).wait_recv()
                h_pass(dx, dy, jj).start()
        each(halves, go)

    each(halves, hidden_x)
    each(halves, lambda j: forward_far(1, j))
    hidden_y(0)
    hidden_y(1)

    def all_hidden(jj):
        for dx, dy in others:
            h_passed(dx, dy, jj).wait_recv()

    each(halves, all_hidden)

    def finish(j):
        c_send(1, j).wait_recv()
        mine = ds(c * rows, rows, rows)
        theirs = ds((1 - c) * rows, rows, rows)
        ost[j] = (own[j, theirs, :] + cr[1, j, theirs, :].astype(F32)).astype(BF16)
        o_send(j).start()
        out_ref[:, ds(j * blk + c * bw, bw, bw)] = (own[j, mine, :] + cr[1, j, mine, :].astype(F32)).astype(BF16)

    def mix(j):
        @pl.when(j >= halves)
        def _():
            forward(1, j, 1)
            forward_far(1, j)

        @pl.when(is_end)
        def _():
            at_end(1, j)
        multiply(1, 1, 1, j, own)

    mix(0)

    def last(j):
        mix(j + 1)
        finish(j)

    each(chunks - 1, last)
    finish(chunks - 1)
    each(chunks, lambda j: o_got(j).wait_recv())

    def settle(j):
        for w in range(2):
            w_swap(w, j).wait_send()
            for side in range(2):
                @pl.when(wanted(w, j, side))
                def _():
                    z_send(w, j, z, side).wait_send()
            for d in range(1, lines - 1):
                for o, side, there in ((z - d, 1, z - d >= 0), (z + d, 0, z + d < lines)):
                    @pl.when(is_mid & there & wanted(w, j, side))
                    def _():
                        z_send(w, j, o, side).wait_send()
        te_swap(j).wait_send()
        o_send(j).wait_send()
        c_send(1, j).wait_send()

        @pl.when(is_mid | (j >= guests))
        def _():
            c_send(0, j).wait_send()

        @pl.when(is_host & (j < guests))
        def _():
            c_send(2, j).wait_send()
            back_send(j).wait_send()

        @pl.when(is_end)
        def _():
            g_send(j).wait_send()

    each(chunks, settle)

    def settle_tokens(g):
        def go(jj):
            t_own(g, jj).wait_send()
            t_send(g, 1, 0, jj).wait_send()
            for dy in range(1, parts):
                t_send(g, 0, dy, jj).wait_send()
                t_relay(g, dy, jj).wait_send()
            for dx, dy in peers:
                t_pass(g, dx, dy, jj).wait_send()
        each(halves, go)

    settle_tokens(0)

    @pl.when(is_host)
    def _():
        settle_tokens(2)

    def settle_hidden(jj):
        h_own(jj, 0).wait_send()
        h_send(1, 0, jj, 0).wait_send()
        for dy in range(1, parts):
            h_send(0, dy, jj, 0).wait_send()
            h_relay(dy, jj).wait_send()
        for dx, dy in peers:
            h_pass(dx, dy, jj).wait_send()

    each(halves, settle_hidden)

    @pl.when(pos < 2 * lines - 1)
    def _():
        chain_send().wait_send()


def per_device(shards, parts, tokens, decay_rate, angle, in_coef, out_coef, skip_coef, gate_weight, out_weight):
    rows, width = tokens.shape
    dims = decay_rate.shape[1]
    lines = shards // 4
    bw = gate_weight.shape[0]
    blk = 2 * bw
    chunks = width // blk
    assert shards % 4 == 0 and lines > 3 and dims % 2 == 0
    assert chunks % 2 == 0 and bw % LANES == 0 and chunks * 2 * parts == shards
    sub = chunks * bw // LANES
    two = 2 * rows
    depth = lines * blk
    skip = skip_coef.reshape(2 * sub, LANES)

    hbm = pl.BlockSpec(memory_space=pltpu.HBM)
    vmem = pl.BlockSpec(memory_space=pltpu.VMEM)
    dma = pltpu.SemaphoreType.DMA
    halves = chunks // 2
    n = 2 * parts
    flops = 2 * 2 * 4 * rows * depth * chunks * bw
    return pl.pallas_call(
        functools.partial(mixer_kernel, lines, parts, dims, max(1, chunks * GUESTS // 4)),
        in_specs=[hbm] * 7 + [vmem],
        out_specs=vmem,
        out_shape=jax.ShapeDtypeStruct((rows, width), BF16),
        scratch_shapes=[
            pltpu.VMEM((5, dims, chunks * bw), F32),
        ] + [pltpu.VMEM((dims * sub, LANES), F32)] * 6 + [
            pltpu.VMEM((sub, LANES), F32),
            pltpu.VMEM((two, chunks * bw), BF16),
            pltpu.VMEM((two * sub, LANES), F32),
            pltpu.VMEM((two * sub, LANES), F32),
            pltpu.VMEM((2, dims * sub, LANES), F32),
            pltpu.VMEM((2, dims * sub, LANES), BF16),
            pltpu.VMEM((2, dims * sub, LANES), BF16),
            pltpu.VMEM((3, 4 * rows, depth), BF16),
            pltpu.VMEM((2, chunks, depth, bw), BF16),
            pltpu.VMEM((chunks, two, bw), F32),
            pltpu.VMEM((chunks, two, bw), F32),
            pltpu.VMEM((3, chunks, two, bw), BF16),
            pltpu.VMEM((3, chunks, two, bw), BF16),
            pltpu.VMEM((chunks, two, bw), BF16),
            pltpu.VMEM((chunks, rows, bw), BF16),
            pltpu.VMEM((rows, width), BF16),
            pltpu.VMEM((chunks, two, bw), BF16),
            dma((2, chunks)),
            dma((chunks,)),
            dma((halves,)),
            dma((5, chunks)),
            dma((2, chunks)),
            dma((2, chunks)),
            dma((chunks,)),
            dma((chunks,)),
            dma((2, 2, chunks, lines)),
            dma((2, chunks, lines)),
            dma((3, n, halves)),
            dma((3, n, halves)),
            dma((3, n, halves)),
            dma((3, n, halves)),
            dma((chunks,)),
            dma((chunks,)),
            dma((chunks,)),
            dma,
            dma,
            dma((3, chunks)),
            dma((3, chunks)),
            dma((chunks,)),
            dma((chunks,)),
        ],
        compiler_params=pltpu.CompilerParams(
            collective_id=0, has_side_effects=True, vmem_limit_bytes=56 * 1024 * 1024
        ),
        cost_estimate=pl.CostEstimate(flops=flops, bytes_accessed=4 * tokens.size, transcendentals=0),
        name="mixer",
    )(
        tokens, gate_weight, out_weight, decay_rate.T, angle.T, in_coef.T, out_coef.swapaxes(1, 2), skip,
    )


def solution(mesh):
    in_specs = (
        P("seq", "tp"),
        P("tp", None),
        P("tp", None),
        P("tp", None),
        P(None, "tp", None),
        P("tp"),
        P("seq", "tp"),
        P("seq", "tp"),
    )
    body = functools.partial(per_device, mesh.shape["seq"], mesh.shape["tp"])
    return jax.shard_map(body, mesh=mesh, in_specs=in_specs, out_specs=P("seq", "tp"), check_vma=False)
```

```python
import functools

import jax
import jax.numpy as jnp
from jax import lax
from jax.experimental import pallas as pl
from jax.experimental.pallas import tpu as pltpu
from jax.sharding import PartitionSpec as P

LANES = 128
UNROLL = 8
GUESTS = 2
MESH = pl.DeviceIdType.MESH
F32, BF16 = jnp.float32, jnp.bfloat16


def mixer_kernel(
    lines, parts, dims, kept,
    tok, gate_w, out_w, decay, angle, in_coef, out_coef, skip_in,
    out_ref,
    raw, q_re_ref, q_im_ref, c_re_ref, c_im_ref, s_re_ref, s_im_ref, skip_ref, te, x2d, y2d, st, cin, cout, A, W, own, own_g, cs, cr, hid, ost, G, bs,
    l_w, l_te, l_a, l_raw, sw_s, sw_r, te_s, te_r, z_s, z_r, x_s, x_r, p_s, p_r, g_s, g_r, b_s, ch_s, ch_r, c_s, c_r, o_s, o_r,
):
    rows, width = tok.shape
    bw = gate_w.shape[0]
    blk = 2 * bw
    chunks = width // blk
    halves = chunks // 2
    sub = chunks * bw // LANES
    tiles = bw // LANES
    two = 2 * rows

    s = lax.axis_index("seq")
    y = lax.axis_index("tp")
    z, x, c = s // 4, (s // 2) % 2, s % 2
    pos = z * 2 + x

    def dev(zz, xx, cc, yy):
        return ((zz * 2 + xx) * 2 + cc, yy)

    partner = dev(z, x, 1 - c, y)
    is_mid = (z > 0) & (z < lines - 1)
    is_end = jnp.logical_not(is_mid)
    is_host = (z == 1) | (z == lines - 2)
    end_z = jnp.where(z == 1, 0, lines - 1)
    host_z = jnp.where(z == 0, 1, lines - 2)

    def hint(v, m):
        return v if isinstance(v, int) else pl.multiple_of(v, m)

    def ds(start, size, m):
        return pl.ds(hint(start, m), size)

    def remote(src, dst, ssem, rsem, where):
        return pltpu.make_async_remote_copy(src, dst, ssem, rsem, device_id=where, device_id_type=MESH)

    weights = (gate_w, out_w)
    others = [(xx, yy) for yy in range(parts) for xx in range(2)]
    peers = others[1:]

    def w_local(w, j):
        return pltpu.make_async_copy(
            weights[w].at[:, ds(j * blk + c * bw, bw, bw)],
            W.at[w, j, ds(z * blk + c * bw, bw, bw)], l_w.at[w, j])

    def w_swap(w, j):
        return remote(
            weights[w].at[:, ds(j * blk + (1 - c) * bw, bw, bw)],
            W.at[w, j, ds(z * blk + c * bw, bw, bw)], sw_s.at[w, j], sw_r.at[w, j], partner)

    def te_local(j):
        return pltpu.make_async_copy(
            tok.at[:, ds(j * blk + c * bw, bw, bw)], te.at[ds(c * rows, rows, rows), ds(j * bw, bw, bw)], l_te.at[j])

    def raw_local(t, j):
        source = (decay, angle, in_coef, out_coef.at[0], out_coef.at[1])[t]
        return pltpu.make_async_copy(
            source.at[:, ds(j * blk + c * bw, bw, bw)], raw.at[t, :, ds(j * bw, bw, bw)], l_raw.at[t, j])

    def te_swap(j):
        return remote(
            tok.at[:, ds(j * blk + (1 - c) * bw, bw, bw)],
            te.at[ds(c * rows, rows, rows), ds(j * bw, bw, bw)], te_s.at[j], te_r.at[j], partner)

    def piece(w, j, o):
        return W.at[w, j, ds(o * blk, blk, blk)]

    def z_send(w, j, o, side):
        where = dev(z + (1 if side else -1), x, c, y)
        return remote(piece(w, j, o), piece(w, j, o), z_s.at[side, w, j, o], z_r.at[w, j, o], where)

    def at_peer(dx, dy):
        return (x + dx) % 2, (y + dy) % parts

    def a_cols(yy, jj):
        return ds((yy * halves + jj) * blk, blk, blk)

    def slot(dx, yy):
        return dx * parts + yy

    def t_from(g, block):
        return (G if g else tok).at[:, ds(block * blk, blk, blk)]

    def t_ref(g, xx, cc, yy, jj):
        return A.at[g, ds((xx * 2 + cc) * rows, rows, rows), a_cols(yy, jj)]

    def t_send(g, dx, dy, jj):
        xx, yy = at_peer(dx, dy)
        return remote(
            t_from(g, 2 * jj + xx), t_ref(g, x, c, y, jj),
            x_s.at[g, dx * parts + dy, jj], x_r.at[g, slot(dx, y), jj], dev(z, xx, c, yy))

    def t_relay(g, dy, jj):
        xx, yy = at_peer(1, dy)
        ref = t_ref(g, xx, c, y, jj)
        return remote(ref, ref, x_s.at[g, parts + dy, jj], x_r.at[g, slot(1, y), jj], dev(z, x, c, yy))

    def t_got(g, dx, dy, jj):
        xx, yy = at_peer(dx, dy)
        ref = t_ref(g, xx, c, yy, jj)
        return remote(ref, ref, x_s.at[g, dx * parts + dy, jj], x_r.at[g, slot(dx, yy), jj], partner)

    def t_local(jj):
        return pltpu.make_async_copy(t_from(0, 2 * jj + x), t_ref(0, x, c, y, jj), l_a.at[jj])

    def t_own(g, jj):
        return remote(
            t_from(g, 2 * jj + x), t_ref(g, x, c, y, jj), p_s.at[g, 0, jj], p_r.at[g, slot(0, y), jj], partner)

    def t_pass(g, dx, dy, jj):
        xx, yy = at_peer(dx, dy)
        ref = t_ref(g, xx, c, yy, jj)
        return remote(ref, ref, p_s.at[g, dx * parts + dy, jj], p_r.at[g, slot(dx, yy), jj], partner)

    def t_passed(g, dx, dy, jj):
        xx, yy = at_peer(dx, dy)
        ref = t_ref(g, xx, 1 - c, yy, jj)
        return remote(ref, ref, p_s.at[g, dx * parts + dy, jj], p_r.at[g, slot(dx, yy), jj], partner)

    def g_send(k):
        ref = G.at[:, ds(k * blk, blk, blk)]
        return remote(t_from(0, k), ref, g_s.at[k], g_r.at[k], dev(host_z, x, c, y))

    def back_send(j):
        return remote(bs.at[j], cr.at[0, j], b_s.at[j], c_r.at[0, j], dev(end_z, x, c, y))

    def h_ref(xx, yy, jj, cc):
        cols = ds((yy * halves + jj) * blk + cc * bw, bw, bw)
        return A.at[1, ds(xx * two, two, two), cols]

    def h_send(dx, dy, jj, j):
        xx, yy = at_peer(dx, dy)
        return remote(
            hid.at[j], h_ref(x, y, jj, c), x_s.at[1, dx * parts + dy, jj], x_r.at[1, slot(dx, y), jj],
            dev(z, xx, c, yy))

    def h_got(dx, dy, jj):
        xx, yy = at_peer(dx, dy)
        ref = h_ref(xx, yy, jj, c)
        return remote(ref, ref, x_s.at[1, dx * parts + dy, jj], x_r.at[1, slot(dx, yy), jj], dev(z, xx, c, yy))

    def h_relay(dy, jj):
        xx, yy = at_peer(1, dy)
        ref = h_ref(xx, y, jj, c)
        return remote(ref, ref, x_s.at[1, parts + dy, jj], x_r.at[1, slot(1, y), jj], dev(z, x, c, yy))

    def h_own(jj, j):
        return remote(hid.at[j], h_ref(x, y, jj, c), p_s.at[1, 0, jj], p_r.at[1, slot(0, y), jj], partner)

    def h_pass(dx, dy, jj):
        xx, yy = at_peer(dx, dy)
        ref = h_ref(xx, yy, jj, c)
        return remote(ref, ref, p_s.at[1, dx * parts + dy, jj], p_r.at[1, slot(dx, yy), jj], partner)

    def h_passed(dx, dy, jj):
        xx, yy = at_peer(dx, dy)
        ref = h_ref(xx, yy, jj, 1 - c)
        return remote(ref, ref, p_s.at[1, dx * parts + dy, jj], p_r.at[1, slot(dx, yy), jj], partner)

    def c_send(w, j):
        return remote(cs.at[w, j], cr.at[w, j], c_s.at[w, j], c_r.at[w, j], dev(z, 1 - x, c, y))

    def chain_send():
        nxt = pos + 1
        return remote(cout, cin, ch_s, ch_r, dev(nxt // 2, nxt % 2, c, y))

    def o_send(j):
        return remote(ost.at[j], out_ref.at[:, ds(j * blk + c * bw, bw, bw)], o_s.at[j], o_r.at[j], partner)

    def o_got(j):
        ref = out_ref.at[:, ds(j * blk + (1 - c) * bw, bw, bw)]
        return remote(ost.at[j], ref, o_s.at[j], o_r.at[j], partner)

    def each(n, f):
        def body(i, carry):
            f(i)
            return carry
        lax.fori_loop(0, n, body, 0)

    each(chunks, lambda j: w_local(0, j).start())
    each(chunks, lambda j: te_local(j).start())
    for t in range(5):
        each(chunks, lambda j: raw_local(t, j).start())
    each(halves, lambda jj: t_local(jj).start())
    each(chunks, lambda j: w_local(1, j).start())

    barrier = pltpu.get_barrier_semaphore()

    def greet(where):
        pl.semaphore_signal(barrier, inc=1, device_id=where, device_id_type=MESH)

    greet(partner)
    for dx, dy in peers:
        xx, yy = at_peer(dx, dy)
        greet(dev(z, xx, c, yy))
    line_peers = [
        (z > 0, dev(z - 1, x, c, y)),
        (z < lines - 1, dev(z + 1, x, c, y)),
        ((x == 1) & (z < lines - 1), dev(z + 1, 0, c, y)),
        ((x == 0) & (z > 0), dev(z - 1, 1, c, y)),
    ]
    for there, where in line_peers:
        @pl.when(there)
        def _():
            greet(where)
    pl.semaphore_wait(barrier, 1 + len(peers) + sum(there.astype(jnp.int32) for there, _ in line_peers))

    each(chunks, lambda j: w_swap(0, j).start())

    def t_start(g, jj):
        t_send(g, 1, 0, jj).start()
        for dy in range(1, parts):
            t_send(g, 0, dy, jj).start()
        t_own(g, jj).start()

    each(halves, lambda jj: t_start(0, jj))
    each(chunks, lambda j: te_swap(j).start())
    each(chunks, lambda j: w_swap(1, j).start())

    def own_ready(w, j):
        w_local(w, j).wait()
        w_swap(w, j).wait_recv()

    def wanted(w, j, side):
        target = z + (1 if side else -1)
        inside = (target >= 0) & (target < lines)
        if w == 0:
            inside = inside & (((target > 0) & (target < lines - 1)) | (j < kept))
        return inside

    def outer_side(side):
        target = z + (1 if side else -1)
        return is_end | (target == 0) | (target == lines - 1)

    def own_at(w, j, side, there):
        @pl.when(wanted(w, j, side) & there)
        def _():
            z_send(w, j, z, side).start()

    def own_inner(w, j):
        for side in range(2):
            @pl.when(wanted(w, j, side) & jnp.logical_not(outer_side(side)))
            def _():
                z_send(w, j, z, side).start()

    def hop(w, j, o, side, there):
        @pl.when(there)
        def _():
            z_send(w, j, o, side).wait_recv()

            @pl.when(wanted(w, j, side))
            def _():
                z_send(w, j, o, side).start()

    def relay_cases(d, from_end):
        low, high = z - d, z + d
        if d == 1:
            at_low = (low == 0) if from_end else (low > 0)
            at_high = (high == lines - 1) if from_end else (high < lines - 1)
        else:
            at_low, at_high = low >= 0, high < lines
        return (low, 1, is_mid & at_low), (high, 0, is_mid & at_high)

    def forward_end(w, j, sides=(0, 1)):
        for o, side, there in relay_cases(1, True):
            if side in sides:
                hop(w, j, o, side, there)

    def forward(w, j, d):
        for o, side, there in relay_cases(d, False):
            hop(w, j, o, side, there)

    def forward_far(w, j):
        for d in range(2, lines - 1):
            forward(w, j, d)

    def at_end(w, j):
        for d in range(1, lines):
            @pl.when(z == 0)
            def _():
                z_send(w, j, d, 0).wait_recv()

            @pl.when(z == lines - 1)
            def _():
                z_send(w, j, lines - 1 - d, 0).wait_recv()

    def span(start, stop, f):
        def body(j, carry):
            f(j)
            return carry
        lax.fori_loop(start, stop, body, 0)

    def first_sends(j):
        own_ready(0, j)
        own_at(0, j, 0, z >= 0)
        own_at(0, j, 1, z >= 0)

    each(halves, first_sends)

    @pl.when(z == lines - 1)
    def _():
        each(chunks, lambda k: g_send(k).start())

    def next_sends(j):
        own_ready(0, j)
        own_at(0, j, 0, outer_side(0))
        own_at(0, j, 1, is_mid & outer_side(1))

    span(halves, chunks, next_sends)

    for t in range(5):
        each(chunks, lambda j: raw_local(t, j).wait())
    for e in range(sub):
        band = slice(e * LANES, (e + 1) * LANES)
        rate, theta, scale, o_re, o_im = (raw[t, :, band] for t in range(5))
        magnitude = 1.0 - rate
        scale = scale * jnp.sqrt(1.0 - magnitude * magnitude)
        at = pl.ds(e, dims, stride=sub)
        c_re_ref[at, :] = scale * o_re
        c_im_ref[at, :] = scale * o_im
        q_re_ref[at, :] = magnitude * jnp.cos(theta)
        q_im_ref[at, :] = magnitude * jnp.sin(theta)
        k, lane = e // tiles, e % tiles
        row = 2 * k * tiles + lane
        skip_ref[e:e + 1, :] = jnp.where(c == 0, skip_in[row:row + 1, :], skip_in[row + tiles:row + tiles + 1, :])

    def span_of():
        base = q_re_ref[...], q_im_ref[...]
        total = None
        count = two
        while count:
            if count % 2:
                total = base if total is None else (
                    total[0] * base[0] - total[1] * base[1], total[0] * base[1] + total[1] * base[0])
            base = base[0] * base[0] - base[1] * base[1], 2.0 * base[0] * base[1]
            count //= 2
        s_re_ref[...] = total[0]
        s_im_ref[...] = total[1]

    span_of()

    def te_ready(j):
        te_local(j).wait()
        te_swap(j).wait_recv()

    each(chunks, te_ready)

    def lay(i, carry):
        for e in range(sub):
            v = te[pl.ds(i * 16, 16), e * LANES:(e + 1) * LANES].astype(F32)
            x2d[pl.ds(i * 16 * sub + e, 16, stride=sub), :] = v
        return carry

    lax.fori_loop(0, two // 16, lay, 0)

    def second_own(j):
        own_ready(1, j)
        for side in range(2):
            own_at(1, j, side, is_mid & outer_side(side) & (j == 0))
        own_at(1, j, 0, z == lines - 1)

    each(chunks, second_own)

    half = dims // 2

    def tile(ref, h):
        return ref[h * sub:(h + 1) * sub, :]

    def step(state, v, q_re, q_im):
        return [(a * re - b * im + v, a * im + b * re) for (re, im), a, b in zip(state, q_re, q_im)]

    def end_half(k):
        hs = range(k * half, (k + 1) * half)
        q_re = [tile(q_re_ref, h) for h in hs]
        q_im = [tile(q_im_ref, h) for h in hs]
        zero = jnp.zeros((sub, LANES), F32)

        def body(i, state):
            for u in range(UNROLL):
                state = step(state, x2d[ds((i * UNROLL + u) * sub, sub, sub), :], q_re, q_im)
            return state

        state = lax.fori_loop(0, two // UNROLL, body, [(zero, zero)] * half)
        for h, (re, im) in zip(hs, state):
            st[0, h * sub:(h + 1) * sub, :] = re
            st[1, h * sub:(h + 1) * sub, :] = im

    def took_x(g):
        def go(jj):
            t_got(g, 1, 0, jj).wait_recv()
            for dy in range(1, parts):
                t_relay(g, dy, jj).start()
            t_pass(g, 1, 0, jj).start()
        each(halves, go)

    def took_y(g, dx):
        def go(jj):
            for dy in range(1, parts):
                t_got(g, dx, dy, jj).wait_recv()
                t_pass(g, dx, dy, jj).start()
        each(halves, go)

    end_half(0)
    end_half(1)
    took_x(0)
    inner_left = jnp.logical_not(outer_side(0))
    each(halves, lambda j: forward_end(0, j, (0,)))
    span(halves, chunks, lambda j: own_at(0, j, 0, inner_left))
    own_at(1, 0, 0, is_mid & inner_left)

    @pl.when(pos == 0)
    def _():
        cin[...] = jnp.zeros_like(cin)

    @pl.when(pos > 0)
    def _():
        chain_send().wait_recv()

    i_re, i_im = cin[0].astype(F32), cin[1].astype(F32)
    a, b = s_re_ref[...], s_im_ref[...]
    cout[0] = (a * i_re - b * i_im + st[0]).astype(BF16)
    cout[1] = (a * i_im + b * i_re + st[1]).astype(BF16)
    st[0] = i_re
    st[1] = i_im

    @pl.when(pos < 2 * lines - 1)
    def _():
        chain_send().start()

    @pl.when(z == 0)
    def _():
        each(chunks, lambda k: g_send(k).start())

    inner_right = is_mid & jnp.logical_not(outer_side(1))
    each(halves, lambda j: forward_end(0, j, (1,)))
    span(halves, chunks, lambda j: own_at(0, j, 1, (z == 0) | inner_right))
    each(chunks, lambda j: own_at(1, j, 1, (z == 0) | (inner_right & (j == 0))))
    each(halves, lambda j: forward(0, j, 1))
    took_y(0, 0)

    def guest_tokens(jj):
        @pl.when(is_host)
        def _():
            g_send(2 * jj).wait_recv()
            g_send(2 * jj + 1).wait_recv()
            t_start(2, jj)
            t_ref(2, x, c, y, jj)[...] = t_from(2, 2 * jj + x)[...]

    def smooth_half(k):
        hs = range(k * half, (k + 1) * half)
        q_re = [tile(q_re_ref, h) for h in hs]
        q_im = [tile(q_im_ref, h) for h in hs]
        c_re = [tile(c_re_ref, h) for h in hs]
        c_im = [tile(c_im_ref, h) for h in hs]
        skip = skip_ref[...]
        state = [(tile(st.at[0], h), tile(st.at[1], h)) for h in hs]

        def body(i, state):
            for u in range(UNROLL):
                at = ds((i * UNROLL + u) * sub, sub, sub)
                v = x2d[at, :]
                state = step(state, v, q_re, q_im)
                sums = [c_re[h] * state[h][0] - c_im[h] * state[h][1] for h in range(half)]
                while len(sums) > 1:
                    sums = [sum(sums[m:m + 2]) for m in range(0, len(sums), 2)]
                before = v * skip if k == 0 else y2d[at, :]
                y2d[at, :] = before + sums[0]
            return state

        lax.fori_loop(0, two // UNROLL, body, state)

    smooth_half(0)
    took_y(0, 1)
    each(halves, lambda j: forward_far(0, j))

    def rest_outer(j):
        for side in range(2):
            own_at(1, j, side, is_mid & outer_side(side))

    span(1, chunks, rest_outer)
    guest_tokens(0)
    smooth_half(1)
    span(1, halves, guest_tokens)
    span(halves, chunks, lambda j: forward(0, j, 1))

    def all_tokens(g):
        def go(jj):
            for dx, dy in others:
                t_passed(g, dx, dy, jj).wait_recv()
        each(halves, go)

    each(halves, lambda jj: t_local(jj).wait())
    all_tokens(0)

    def multiply(w, g, k, j, mine):
        right = W[w, j]
        away = jnp.dot(A[g, ds((1 - x) * two, two, two), :], right, preferred_element_type=F32)
        cs[k, j] = away.astype(BF16)
        c_send(k, j).start()
        mine[j] = jnp.dot(A[g, ds(x * two, two, two), :], right, preferred_element_type=F32)

    def project(j):
        @pl.when(is_end & (j < kept))
        def _():
            at_end(0, j)

        @pl.when(is_mid | (j < kept))
        def _():
            multiply(0, 0, 0, j, own)

        @pl.when(is_end & (j >= kept))
        def _():
            own[j] = jnp.zeros((two, bw), F32)

    each(halves, project)

    @pl.when(is_host)
    def _():
        took_x(2)

    span(halves, chunks, lambda j: forward_end(0, j))
    span(1, chunks, lambda j: own_inner(1, j))

    @pl.when(is_host)
    def _():
        took_y(2, 0)

    forward(1, 0, 1)

    def later_project(j):
        forward_far(0, j)
        project(j)

    span(halves, kept, later_project)
    forward_far(0, kept)

    @pl.when(is_host)
    def _():
        took_y(2, 1)
        all_tokens(2)
        multiply(0, 2, 2, kept, own_g)

    def guest_sums(j):
        forward_far(0, j)

        @pl.when(is_host)
        def _():
            multiply(0, 2, 2, j, own_g)

    span(kept + 1, chunks, guest_sums)
    span(1, halves, lambda j: forward(1, j, 1))
    each(halves, lambda j: forward_end(1, j))
    span(kept, chunks, project)

    def guest_back(j):
        @pl.when(is_host)
        def _():
            c_send(2, j).wait_recv()
            bs[j] = (own_g[j] + cr[2, j].astype(F32)).astype(BF16)
            back_send(j).start()

    def hidden(j):
        c_send(0, j).wait_recv()
        jj = j // 2
        target = j % 2

        def band(i, carry):
            at = pl.ds(pl.multiple_of(i * 16, 16), 16)
            for e in range(tiles):
                lane = slice(e * LANES, (e + 1) * LANES)
                smooth = y2d[pl.ds(i * 16 * sub + j * tiles + e, 16, stride=sub), :]
                gate = own[j, at, lane] + cr[0, j, at, lane].astype(F32)
                value = smooth * jax.nn.sigmoid(smooth) * jax.nn.sigmoid(gate)
                hid[j, at, lane] = value.astype(BF16)
            return carry

        lax.fori_loop(0, two // 16, band, 0)

        @pl.when(target == x)
        def _():
            h_own(jj, j).start()
            for dy in range(1, parts):
                h_send(0, dy, jj, j).start()
            h_ref(x, y, jj, c)[...] = hid[j]

        @pl.when(target != x)
        def _():
            h_send(1, 0, jj, j).start()

    def hidden_x(jj):
        h_got(1, 0, jj).wait_recv()
        for dy in range(1, parts):
            h_relay(dy, jj).start()
        h_pass(1, 0, jj).start()

    def hidden_y(dx, jj):
        for dy in range(1, parts):
            h_got(dx, dy, jj).wait_recv()
            h_pass(dx, dy, jj).start()

    each(halves, hidden)
    span(kept, chunks, guest_back)
    span(halves, chunks, lambda j: forward(1, j, 1))
    span(halves, chunks, lambda j: forward_end(1, j))
    span(0, halves // 2, hidden_x)
    forward_far(1, 0)
    span(0, halves // 2, lambda jj: hidden_y(0, jj))
    span(halves, chunks, hidden)
    span(1, halves, lambda j: forward_far(1, j))
    span(halves // 2, halves, hidden_x)
    span(0, halves // 2, lambda jj: hidden_y(1, jj))
    span(halves // 2, halves, lambda jj: hidden_y(0, jj))
    forward_far(1, halves)
    span(halves // 2, halves, lambda jj: hidden_y(1, jj))
    span(halves + 1, chunks, lambda j: forward_far(1, j))

    def all_hidden(jj):
        for dx, dy in others:
            h_passed(dx, dy, jj).wait_recv()

    each(halves, all_hidden)

    def finish(j):
        c_send(1, j).wait_recv()
        mine = ds(c * rows, rows, rows)
        theirs = ds((1 - c) * rows, rows, rows)
        ost[j] = (own[j, theirs, :] + cr[1, j, theirs, :].astype(F32)).astype(BF16)
        o_send(j).start()
        out_ref[:, ds(j * blk + c * bw, bw, bw)] = (own[j, mine, :] + cr[1, j, mine, :].astype(F32)).astype(BF16)

    def mix(j):
        @pl.when(is_end)
        def _():
            at_end(1, j)
        multiply(1, 1, 1, j, own)

    mix(0)

    def last(j):
        mix(j + 1)
        finish(j)

    each(chunks - 1, last)
    finish(chunks - 1)
    each(chunks, lambda j: o_got(j).wait_recv())

    def settle(j):
        for w in range(2):
            w_swap(w, j).wait_send()
            for side in range(2):
                @pl.when(wanted(w, j, side))
                def _():
                    z_send(w, j, z, side).wait_send()
            for d in range(1, lines - 1):
                for o, side, there in ((z - d, 1, z - d >= 0), (z + d, 0, z + d < lines)):
                    @pl.when(is_mid & there & wanted(w, j, side))
                    def _():
                        z_send(w, j, o, side).wait_send()
        te_swap(j).wait_send()
        o_send(j).wait_send()
        c_send(1, j).wait_send()

        @pl.when(is_mid | (j < kept))
        def _():
            c_send(0, j).wait_send()

        @pl.when(is_host & (j >= kept))
        def _():
            c_send(2, j).wait_send()
            back_send(j).wait_send()

        @pl.when(is_end)
        def _():
            g_send(j).wait_send()

    each(chunks, settle)

    def settle_tokens(g):
        def go(jj):
            t_own(g, jj).wait_send()
            t_send(g, 1, 0, jj).wait_send()
            for dy in range(1, parts):
                t_send(g, 0, dy, jj).wait_send()
                t_relay(g, dy, jj).wait_send()
            for dx, dy in peers:
                t_pass(g, dx, dy, jj).wait_send()
        each(halves, go)

    settle_tokens(0)

    @pl.when(is_host)
    def _():
        settle_tokens(2)

    def settle_hidden(jj):
        h_own(jj, 0).wait_send()
        h_send(1, 0, jj, 0).wait_send()
        for dy in range(1, parts):
            h_send(0, dy, jj, 0).wait_send()
            h_relay(dy, jj).wait_send()
        for dx, dy in peers:
            h_pass(dx, dy, jj).wait_send()

    each(halves, settle_hidden)

    @pl.when(pos < 2 * lines - 1)
    def _():
        chain_send().wait_send()


def per_device(shards, parts, tokens, decay_rate, angle, in_coef, out_coef, skip_coef, gate_weight, out_weight):
    rows, width = tokens.shape
    dims = decay_rate.shape[1]
    lines = shards // 4
    bw = gate_weight.shape[0]
    blk = 2 * bw
    chunks = width // blk
    assert shards % 4 == 0 and lines > 3 and dims % 2 == 0
    assert chunks % 2 == 0 and bw % LANES == 0 and chunks * 2 * parts == shards
    sub = chunks * bw // LANES
    two = 2 * rows
    depth = lines * blk
    skip = skip_coef.reshape(2 * sub, LANES)

    hbm = pl.BlockSpec(memory_space=pltpu.HBM)
    vmem = pl.BlockSpec(memory_space=pltpu.VMEM)
    dma = pltpu.SemaphoreType.DMA
    halves = chunks // 2
    n = 2 * parts
    flops = 2 * 2 * 4 * rows * depth * chunks * bw
    return pl.pallas_call(
        functools.partial(mixer_kernel, lines, parts, dims, chunks - max(1, chunks * GUESTS // 4)),
        in_specs=[hbm] * 7 + [vmem],
        out_specs=vmem,
        out_shape=jax.ShapeDtypeStruct((rows, width), BF16),
        scratch_shapes=[
            pltpu.VMEM((5, dims, chunks * bw), F32),
        ] + [pltpu.VMEM((dims * sub, LANES), F32)] * 6 + [
            pltpu.VMEM((sub, LANES), F32),
            pltpu.VMEM((two, chunks * bw), BF16),
            pltpu.VMEM((two * sub, LANES), F32),
            pltpu.VMEM((two * sub, LANES), F32),
            pltpu.VMEM((2, dims * sub, LANES), F32),
            pltpu.VMEM((2, dims * sub, LANES), BF16),
            pltpu.VMEM((2, dims * sub, LANES), BF16),
            pltpu.VMEM((3, 4 * rows, depth), BF16),
            pltpu.VMEM((2, chunks, depth, bw), BF16),
            pltpu.VMEM((chunks, two, bw), F32),
            pltpu.VMEM((chunks, two, bw), F32),
            pltpu.VMEM((3, chunks, two, bw), BF16),
            pltpu.VMEM((3, chunks, two, bw), BF16),
            pltpu.VMEM((chunks, two, bw), BF16),
            pltpu.VMEM((chunks, rows, bw), BF16),
            pltpu.VMEM((rows, width), BF16),
            pltpu.VMEM((chunks, two, bw), BF16),
            dma((2, chunks)),
            dma((chunks,)),
            dma((halves,)),
            dma((5, chunks)),
            dma((2, chunks)),
            dma((2, chunks)),
            dma((chunks,)),
            dma((chunks,)),
            dma((2, 2, chunks, lines)),
            dma((2, chunks, lines)),
            dma((3, n, halves)),
            dma((3, n, halves)),
            dma((3, n, halves)),
            dma((3, n, halves)),
            dma((chunks,)),
            dma((chunks,)),
            dma((chunks,)),
            dma,
            dma,
            dma((3, chunks)),
            dma((3, chunks)),
            dma((chunks,)),
            dma((chunks,)),
        ],
        compiler_params=pltpu.CompilerParams(
            collective_id=0, has_side_effects=True, vmem_limit_bytes=56 * 1024 * 1024
        ),
        cost_estimate=pl.CostEstimate(flops=flops, bytes_accessed=4 * tokens.size, transcendentals=0),
        name="mixer",
    )(
        tokens, gate_weight, out_weight, decay_rate.T, angle.T, in_coef.T, out_coef.swapaxes(1, 2), skip,
    )


def solution(mesh):
    in_specs = (
        P("seq", "tp"),
        P("tp", None),
        P("tp", None),
        P("tp", None),
        P(None, "tp", None),
        P("tp"),
        P("seq", "tp"),
        P("seq", "tp"),
    )
    body = functools.partial(per_device, mesh.shape["seq"], mesh.shape["tp"])
    return jax.shard_map(body, mesh=mesh, in_specs=in_specs, out_specs=P("seq", "tp"), check_vma=False)
```

```python
import functools

import jax
import jax.numpy as jnp
from jax import lax
from jax.experimental import pallas as pl
from jax.experimental.pallas import tpu as pltpu
from jax.sharding import PartitionSpec as P

LANES = 128
UNROLL = 8
GUESTS = 2
MESH = pl.DeviceIdType.MESH
F32, BF16 = jnp.float32, jnp.bfloat16


def mixer_kernel(
    lines, parts, dims, kept,
    tok, gate_w, out_w, decay, angle, in_coef, out_coef, skip_in,
    out_ref,
    raw, q_re_ref, q_im_ref, c_re_ref, c_im_ref, s_re_ref, s_im_ref, skip_ref, te, x2d, y2d, st, ein, eout, cin, cout, A, W, own, own_g, cs, cr, hid, ost, G, bs,
    l_w, l_te, l_a, l_raw, sw_s, sw_r, te_s, te_r, z_s, z_r, x_s, x_r, p_s, p_r, g_s, g_r, b_s, e_s, e_r, ch_s, ch_r, c_s, c_r, o_s, o_r,
):
    rows, width = tok.shape
    bw = gate_w.shape[0]
    blk = 2 * bw
    chunks = width // blk
    halves = chunks // 2
    sub = chunks * bw // LANES
    tiles = bw // LANES
    two = 2 * rows

    s = lax.axis_index("seq")
    y = lax.axis_index("tp")
    z, x, c = s // 4, (s // 2) % 2, s % 2

    def dev(zz, xx, cc, yy):
        return ((zz * 2 + xx) * 2 + cc, yy)

    partner = dev(z, x, 1 - c, y)
    is_mid = (z > 0) & (z < lines - 1)
    is_end = jnp.logical_not(is_mid)
    is_host = (z == 1) | (z == lines - 2)
    end_z = jnp.where(z == 1, 0, lines - 1)
    host_z = jnp.where(z == 0, 1, lines - 2)

    def hint(v, m):
        return v if isinstance(v, int) else pl.multiple_of(v, m)

    def ds(start, size, m):
        return pl.ds(hint(start, m), size)

    def remote(src, dst, ssem, rsem, where):
        return pltpu.make_async_remote_copy(src, dst, ssem, rsem, device_id=where, device_id_type=MESH)

    weights = (gate_w, out_w)
    others = [(xx, yy) for yy in range(parts) for xx in range(2)]
    peers = others[1:]

    def w_local(w, j):
        return pltpu.make_async_copy(
            weights[w].at[:, ds(j * blk + c * bw, bw, bw)],
            W.at[w, j, ds(z * blk + c * bw, bw, bw)], l_w.at[w, j])

    def w_swap(w, j):
        return remote(
            weights[w].at[:, ds(j * blk + (1 - c) * bw, bw, bw)],
            W.at[w, j, ds(z * blk + c * bw, bw, bw)], sw_s.at[w, j], sw_r.at[w, j], partner)

    def te_local(j):
        return pltpu.make_async_copy(
            tok.at[:, ds(j * blk + c * bw, bw, bw)], te.at[ds(c * rows, rows, rows), ds(j * bw, bw, bw)], l_te.at[j])

    def raw_local(t, j):
        source = (decay, angle, in_coef, out_coef.at[0], out_coef.at[1])[t]
        return pltpu.make_async_copy(
            source.at[:, ds(j * blk + c * bw, bw, bw)], raw.at[t, :, ds(j * bw, bw, bw)], l_raw.at[t, j])

    def te_swap(j):
        return remote(
            tok.at[:, ds(j * blk + (1 - c) * bw, bw, bw)],
            te.at[ds(c * rows, rows, rows), ds(j * bw, bw, bw)], te_s.at[j], te_r.at[j], partner)

    def piece(w, j, o):
        return W.at[w, j, ds(o * blk, blk, blk)]

    def z_send(w, j, o, side):
        where = dev(z + (1 if side else -1), x, c, y)
        return remote(piece(w, j, o), piece(w, j, o), z_s.at[side, w, j, o], z_r.at[w, j, o], where)

    def at_peer(dx, dy):
        return (x + dx) % 2, (y + dy) % parts

    def a_cols(yy, jj):
        return ds((yy * halves + jj) * blk, blk, blk)

    def slot(dx, yy):
        return dx * parts + yy

    def t_from(g, block):
        return (G if g else tok).at[:, ds(block * blk, blk, blk)]

    def t_ref(g, xx, cc, yy, jj):
        return A.at[g, ds((xx * 2 + cc) * rows, rows, rows), a_cols(yy, jj)]

    def t_send(g, dx, dy, jj):
        xx, yy = at_peer(dx, dy)
        return remote(
            t_from(g, 2 * jj + xx), t_ref(g, x, c, y, jj),
            x_s.at[g, dx * parts + dy, jj], x_r.at[g, slot(dx, y), jj], dev(z, xx, c, yy))

    def t_relay(g, dy, jj):
        xx, yy = at_peer(1, dy)
        ref = t_ref(g, xx, c, y, jj)
        return remote(ref, ref, x_s.at[g, parts + dy, jj], x_r.at[g, slot(1, y), jj], dev(z, x, c, yy))

    def t_got(g, dx, dy, jj):
        xx, yy = at_peer(dx, dy)
        ref = t_ref(g, xx, c, yy, jj)
        return remote(ref, ref, x_s.at[g, dx * parts + dy, jj], x_r.at[g, slot(dx, yy), jj], partner)

    def t_local(jj):
        return pltpu.make_async_copy(t_from(0, 2 * jj + x), t_ref(0, x, c, y, jj), l_a.at[jj])

    def t_own(g, jj):
        return remote(
            t_from(g, 2 * jj + x), t_ref(g, x, c, y, jj), p_s.at[g, 0, jj], p_r.at[g, slot(0, y), jj], partner)

    def t_pass(g, dx, dy, jj):
        xx, yy = at_peer(dx, dy)
        ref = t_ref(g, xx, c, yy, jj)
        return remote(ref, ref, p_s.at[g, dx * parts + dy, jj], p_r.at[g, slot(dx, yy), jj], partner)

    def t_passed(g, dx, dy, jj):
        xx, yy = at_peer(dx, dy)
        ref = t_ref(g, xx, 1 - c, yy, jj)
        return remote(ref, ref, p_s.at[g, dx * parts + dy, jj], p_r.at[g, slot(dx, yy), jj], partner)

    def g_send(k):
        ref = G.at[:, ds(k * blk, blk, blk)]
        return remote(t_from(0, k), ref, g_s.at[k], g_r.at[k], dev(host_z, x, c, y))

    def back_send(j):
        return remote(bs.at[j], cr.at[0, j], b_s.at[j], c_r.at[0, j], dev(end_z, x, c, y))

    def h_ref(xx, yy, jj, cc):
        cols = ds((yy * halves + jj) * blk + cc * bw, bw, bw)
        return A.at[1, ds(xx * two, two, two), cols]

    def h_send(dx, dy, jj, j):
        xx, yy = at_peer(dx, dy)
        return remote(
            hid.at[j], h_ref(x, y, jj, c), x_s.at[1, dx * parts + dy, jj], x_r.at[1, slot(dx, y), jj],
            dev(z, xx, c, yy))

    def h_got(dx, dy, jj):
        xx, yy = at_peer(dx, dy)
        ref = h_ref(xx, yy, jj, c)
        return remote(ref, ref, x_s.at[1, dx * parts + dy, jj], x_r.at[1, slot(dx, yy), jj], dev(z, xx, c, yy))

    def h_relay(dy, jj):
        xx, yy = at_peer(1, dy)
        ref = h_ref(xx, y, jj, c)
        return remote(ref, ref, x_s.at[1, parts + dy, jj], x_r.at[1, slot(1, y), jj], dev(z, x, c, yy))

    def h_own(jj, j):
        return remote(hid.at[j], h_ref(x, y, jj, c), p_s.at[1, 0, jj], p_r.at[1, slot(0, y), jj], partner)

    def h_pass(dx, dy, jj):
        xx, yy = at_peer(dx, dy)
        ref = h_ref(xx, yy, jj, c)
        return remote(ref, ref, p_s.at[1, dx * parts + dy, jj], p_r.at[1, slot(dx, yy), jj], partner)

    def h_passed(dx, dy, jj):
        xx, yy = at_peer(dx, dy)
        ref = h_ref(xx, yy, jj, 1 - c)
        return remote(ref, ref, p_s.at[1, dx * parts + dy, jj], p_r.at[1, slot(dx, yy), jj], partner)

    def c_send(w, j):
        return remote(cs.at[w, j], cr.at[w, j], c_s.at[w, j], c_r.at[w, j], dev(z, 1 - x, c, y))

    def e_send():
        return remote(eout, ein, e_s, e_r, dev(z, 1 - x, c, y))

    def chain_send():
        return remote(cout, cin, ch_s, ch_r, dev(z + 1, x, c, y))

    def o_send(j):
        return remote(ost.at[j], out_ref.at[:, ds(j * blk + c * bw, bw, bw)], o_s.at[j], o_r.at[j], partner)

    def o_got(j):
        ref = out_ref.at[:, ds(j * blk + (1 - c) * bw, bw, bw)]
        return remote(ost.at[j], ref, o_s.at[j], o_r.at[j], partner)

    def each(n, f):
        def body(i, carry):
            f(i)
            return carry
        lax.fori_loop(0, n, body, 0)

    each(chunks, lambda j: w_local(0, j).start())
    each(chunks, lambda j: te_local(j).start())
    for t in range(5):
        each(chunks, lambda j: raw_local(t, j).start())
    each(halves, lambda jj: t_local(jj).start())
    each(chunks, lambda j: w_local(1, j).start())

    barrier = pltpu.get_barrier_semaphore()

    def greet(where):
        pl.semaphore_signal(barrier, inc=1, device_id=where, device_id_type=MESH)

    greet(partner)
    for dx, dy in peers:
        xx, yy = at_peer(dx, dy)
        greet(dev(z, xx, c, yy))
    line_peers = [
        (z > 0, dev(z - 1, x, c, y)),
        (z < lines - 1, dev(z + 1, x, c, y)),
    ]
    for there, where in line_peers:
        @pl.when(there)
        def _():
            greet(where)
    pl.semaphore_wait(barrier, 1 + len(peers) + sum(there.astype(jnp.int32) for there, _ in line_peers))

    each(chunks, lambda j: w_swap(0, j).start())

    @pl.when(z == 0)
    def _():
        each(halves, lambda k: g_send(k).start())

    @pl.when(z == lines - 1)
    def _():
        each(chunks, lambda k: g_send(k).start())

    def t_start(g, jj):
        t_send(g, 1, 0, jj).start()
        for dy in range(1, parts):
            t_send(g, 0, dy, jj).start()
        t_own(g, jj).start()

    each(halves, lambda jj: t_start(0, jj))
    each(chunks, lambda j: te_swap(j).start())
    each(chunks, lambda j: w_swap(1, j).start())

    def own_ready(w, j):
        w_local(w, j).wait()
        w_swap(w, j).wait_recv()

    def wanted(w, j, side):
        target = z + (1 if side else -1)
        inside = (target >= 0) & (target < lines)
        if w == 0:
            inside = inside & (((target > 0) & (target < lines - 1)) | (j < kept))
        return inside

    def outer_side(side):
        target = z + (1 if side else -1)
        return is_end | (target == 0) | (target == lines - 1)

    def own_at(w, j, side, there):
        @pl.when(wanted(w, j, side) & there)
        def _():
            z_send(w, j, z, side).start()

    def own_inner(w, j):
        for side in range(2):
            @pl.when(wanted(w, j, side) & jnp.logical_not(outer_side(side)))
            def _():
                z_send(w, j, z, side).start()

    def hop(w, j, o, side, there):
        @pl.when(there)
        def _():
            z_send(w, j, o, side).wait_recv()

            @pl.when(wanted(w, j, side))
            def _():
                z_send(w, j, o, side).start()

    def relay_cases(d, from_end):
        low, high = z - d, z + d
        if d == 1:
            at_low = (low == 0) if from_end else (low > 0)
            at_high = (high == lines - 1) if from_end else (high < lines - 1)
        else:
            at_low, at_high = low >= 0, high < lines
        return (low, 1, is_mid & at_low), (high, 0, is_mid & at_high)

    def forward_end(w, j, sides=(0, 1)):
        for o, side, there in relay_cases(1, True):
            if side in sides:
                hop(w, j, o, side, there)

    def forward(w, j, d):
        for o, side, there in relay_cases(d, False):
            hop(w, j, o, side, there)

    def forward_far(w, j):
        for d in range(2, lines - 1):
            forward(w, j, d)

    def at_end(w, j):
        for d in range(1, lines):
            @pl.when(z == 0)
            def _():
                z_send(w, j, d, 0).wait_recv()

            @pl.when(z == lines - 1)
            def _():
                z_send(w, j, lines - 1 - d, 0).wait_recv()

    def span(start, stop, f):
        def body(j, carry):
            f(j)
            return carry
        lax.fori_loop(start, stop, body, 0)

    def first_sends(j):
        own_ready(0, j)
        own_at(0, j, 0, z >= 0)
        own_at(0, j, 1, is_mid & (outer_side(1) | (j < halves)))

    each(chunks, first_sends)

    for t in range(5):
        each(chunks, lambda j: raw_local(t, j).wait())
    for e in range(sub):
        band = slice(e * LANES, (e + 1) * LANES)
        rate, theta, scale, o_re, o_im = (raw[t, :, band] for t in range(5))
        magnitude = 1.0 - rate
        scale = scale * jnp.sqrt(1.0 - magnitude * magnitude)
        at = pl.ds(e, dims, stride=sub)
        c_re_ref[at, :] = scale * o_re
        c_im_ref[at, :] = scale * o_im
        q_re_ref[at, :] = magnitude * jnp.cos(theta)
        q_im_ref[at, :] = magnitude * jnp.sin(theta)
        k, lane = e // tiles, e % tiles
        row = 2 * k * tiles + lane
        skip_ref[e:e + 1, :] = jnp.where(c == 0, skip_in[row:row + 1, :], skip_in[row + tiles:row + tiles + 1, :])

    def span_of():
        base = q_re_ref[...], q_im_ref[...]
        total = None
        count = two
        while count:
            if count % 2:
                total = base if total is None else (
                    total[0] * base[0] - total[1] * base[1], total[0] * base[1] + total[1] * base[0])
            base = base[0] * base[0] - base[1] * base[1], 2.0 * base[0] * base[1]
            count //= 2
        s_re_ref[...] = total[0]
        s_im_ref[...] = total[1]

    span_of()

    def te_ready(j):
        te_local(j).wait()
        te_swap(j).wait_recv()

    each(chunks, te_ready)

    def lay(i, carry):
        for e in range(sub):
            v = te[pl.ds(i * 16, 16), e * LANES:(e + 1) * LANES].astype(F32)
            x2d[pl.ds(i * 16 * sub + e, 16, stride=sub), :] = v
        return carry

    lax.fori_loop(0, two // 16, lay, 0)

    def second_own(j):
        own_ready(1, j)
        for side in range(2):
            own_at(1, j, side, is_mid & outer_side(side) & (j == 0))
        own_at(1, j, 0, z == lines - 1)

    each(chunks, second_own)

    half = dims // 2

    def tile(ref, h):
        return ref[h * sub:(h + 1) * sub, :]

    def step(state, v, q_re, q_im):
        return [(a * re - b * im + v, a * im + b * re) for (re, im), a, b in zip(state, q_re, q_im)]

    def end_half(k):
        hs = range(k * half, (k + 1) * half)
        q_re = [tile(q_re_ref, h) for h in hs]
        q_im = [tile(q_im_ref, h) for h in hs]
        zero = jnp.zeros((sub, LANES), F32)

        def body(i, state):
            for u in range(UNROLL):
                state = step(state, x2d[ds((i * UNROLL + u) * sub, sub, sub), :], q_re, q_im)
            return state

        state = lax.fori_loop(0, two // UNROLL, body, [(zero, zero)] * half)
        for h, (re, im) in zip(hs, state):
            st[0, h * sub:(h + 1) * sub, :] = re
            st[1, h * sub:(h + 1) * sub, :] = im

    def took_x(g):
        def go(jj):
            t_got(g, 1, 0, jj).wait_recv()
            for dy in range(1, parts):
                t_relay(g, dy, jj).start()
            t_pass(g, 1, 0, jj).start()
        each(halves, go)

    def took_y(g, dx):
        def go(jj):
            for dy in range(1, parts):
                t_got(g, dx, dy, jj).wait_recv()
                t_pass(g, dx, dy, jj).start()
        each(halves, go)

    end_half(0)
    end_half(1)
    eout[...] = st[...].astype(BF16)
    e_send().start()
    took_x(0)
    inner_left = jnp.logical_not(outer_side(0))
    own_at(1, 0, 0, inner_left)

    def cmul(a, b):
        return a[0] * b[0] - a[1] * b[1], a[0] * b[1] + a[1] * b[0]

    span_q = s_re_ref[...], s_im_ref[...]
    e_send().wait_recv()
    mine = st[0], st[1]
    other = ein[0].astype(F32), ein[1].astype(F32)
    first = [jnp.where(x == 0, m, o) for m, o in zip(mine, other)]
    second = [jnp.where(x == 0, o, m) for m, o in zip(mine, other)]
    plane = [a + b for a, b in zip(cmul(span_q, first), second)]

    @pl.when(z == 0)
    def _():
        cin[...] = jnp.zeros_like(cin)

    @pl.when(z > 0)
    def _():
        chain_send().wait_recv()

    carry = cin[0].astype(F32), cin[1].astype(F32)
    moved = cmul(span_q, carry)
    onward = [a + b for a, b in zip(cmul(span_q, moved), plane)]
    cout[0] = onward[0].astype(BF16)
    cout[1] = onward[1].astype(BF16)

    @pl.when(z < lines - 1)
    def _():
        chain_send().start()

    for k in range(2):
        st[k] = jnp.where(x == 0, carry[k], moved[k] + first[k])

    inner_right = is_mid & jnp.logical_not(outer_side(1))

    @pl.when(z == 0)
    def _():
        each(halves, lambda k: g_send(halves + k).start())

    each(chunks, lambda j: own_at(0, j, 1, (z == 0) | (inner_right & (j >= halves))))
    each(chunks, lambda j: own_at(1, j, 1, (z == 0) | (inner_right & (j == 0))))
    each(halves, lambda j: forward(0, j, 1))
    took_y(0, 0)

    def guest_tokens(jj):
        @pl.when(is_host)
        def _():
            g_send(2 * jj).wait_recv()
            g_send(2 * jj + 1).wait_recv()
            t_start(2, jj)
            t_ref(2, x, c, y, jj)[...] = t_from(2, 2 * jj + x)[...]

    def smooth_half(k):
        hs = range(k * half, (k + 1) * half)
        q_re = [tile(q_re_ref, h) for h in hs]
        q_im = [tile(q_im_ref, h) for h in hs]
        c_re = [tile(c_re_ref, h) for h in hs]
        c_im = [tile(c_im_ref, h) for h in hs]
        skip = skip_ref[...]
        state = [(tile(st.at[0], h), tile(st.at[1], h)) for h in hs]

        def body(i, state):
            for u in range(UNROLL):
                at = ds((i * UNROLL + u) * sub, sub, sub)
                v = x2d[at, :]
                state = step(state, v, q_re, q_im)
                sums = [c_re[h] * state[h][0] - c_im[h] * state[h][1] for h in range(half)]
                while len(sums) > 1:
                    sums = [sum(sums[m:m + 2]) for m in range(0, len(sums), 2)]
                before = v * skip if k == 0 else y2d[at, :]
                y2d[at, :] = before + sums[0]
            return state

        lax.fori_loop(0, two // UNROLL, body, state)

    def all_tokens(g):
        def go(jj):
            for dx, dy in others:
                t_passed(g, dx, dy, jj).wait_recv()
        each(halves, go)

    def multiply(w, g, k, j, mine):
        right = W[w, j]
        away = jnp.dot(A[g, ds((1 - x) * two, two, two), :], right, preferred_element_type=F32)
        cs[k, j] = away.astype(BF16)
        c_send(k, j).start()
        mine[j] = jnp.dot(A[g, ds(x * two, two, two), :], right, preferred_element_type=F32)

    def project(j):
        @pl.when(is_end & (j < kept))
        def _():
            at_end(0, j)

        @pl.when(is_mid | (j < kept))
        def _():
            multiply(0, 0, 0, j, own)

        @pl.when(is_end & (j >= kept))
        def _():
            own[j] = jnp.zeros((two, bw), F32)

    guest_tokens(0)
    smooth_half(0)
    took_y(0, 1)

    def rest_outer(j):
        for side in range(2):
            own_at(1, j, side, is_mid & outer_side(side))

    rest_outer(1)
    each(halves, lambda j: forward_end(0, j, (0,)))
    span(1, halves, guest_tokens)
    smooth_half(1)

    forward_end(0, 0, (1,))

    @pl.when(is_host)
    def _():
        took_x(2)
        took_y(2, 0)

    forward(1, 0, 1)
    span(1, halves, lambda j: forward_end(0, j, (1,)))
    each(halves, lambda jj: t_local(jj).wait())
    all_tokens(0)

    def guest_back(j):
        @pl.when(is_host)
        def _():
            c_send(2, j).wait_recv()
            bs[j] = (own_g[j] + cr[2, j].astype(F32)).astype(BF16)
            back_send(j).start()

    def hidden(j):
        c_send(0, j).wait_recv()
        jj = j // 2
        target = j % 2

        def band(i, carry):
            at = pl.ds(pl.multiple_of(i * 16, 16), 16)
            for e in range(tiles):
                lane = slice(e * LANES, (e + 1) * LANES)
                smooth = y2d[pl.ds(i * 16 * sub + j * tiles + e, 16, stride=sub), :]
                gate = own[j, at, lane] + cr[0, j, at, lane].astype(F32)
                value = smooth * jax.nn.sigmoid(smooth) * jax.nn.sigmoid(gate)
                hid[j, at, lane] = value.astype(BF16)
            return carry

        lax.fori_loop(0, two // 16, band, 0)

        @pl.when(target == x)
        def _():
            h_own(jj, j).start()
            for dy in range(1, parts):
                h_send(0, dy, jj, j).start()
            h_ref(x, y, jj, c)[...] = hid[j]

        @pl.when(target != x)
        def _():
            h_send(1, 0, jj, j).start()

    def hidden_x(jj):
        h_got(1, 0, jj).wait_recv()
        for dy in range(1, parts):
            h_relay(dy, jj).start()
        h_pass(1, 0, jj).start()

    def hidden_y(dx, jj):
        for dy in range(1, parts):
            h_got(dx, dy, jj).wait_recv()
            h_pass(dx, dy, jj).start()

    def early_project(j):
        forward_far(0, j)
        project(j)
        forward_end(0, halves + j)

    each(halves, early_project)
    span(2, chunks, rest_outer)
    own_inner(1, 1)
    span(halves, chunks, lambda j: forward(0, j, 1))

    @pl.when(is_host)
    def _():
        took_y(2, 1)
        all_tokens(2)

    @pl.when(is_end)
    def _():
        each(halves, hidden)

    def guest_sums(j):
        forward_far(0, j)

        @pl.when(is_host & (j >= kept))
        def _():
            multiply(0, 2, 2, j, own_g)

    def guest_step(j):
        guest_sums(j)
        forward_end(1, j - halves)

    span(halves, chunks, guest_step)
    span(2, chunks, lambda j: own_inner(1, j))

    @pl.when(is_mid)
    def _():
        each(halves, hidden)

    def late_project(j):
        project(j)

        @pl.when(j >= kept)
        def _():
            guest_back(j)

    span(halves, chunks, late_project)
    span(1, halves, lambda j: forward(1, j, 1))

    each(halves, lambda j: forward_far(1, j))
    span(halves, chunks, lambda j: forward_end(1, j))
    span(0, halves // 2, hidden_x)
    span(0, halves // 2, lambda jj: hidden_y(0, jj))
    span(0, halves // 2, lambda jj: hidden_y(1, jj))


    def gate_done(j):
        hidden(j)
        forward(1, j, 1)

    span(halves, chunks, gate_done)
    span(halves // 2, halves, hidden_x)
    span(halves // 2, halves, lambda jj: hidden_y(0, jj))
    span(halves // 2, halves, lambda jj: hidden_y(1, jj))

    def all_hidden(jj):
        for dx, dy in others:
            h_passed(dx, dy, jj).wait_recv()

    each(halves, all_hidden)

    def finish(j):
        c_send(1, j).wait_recv()
        mine = ds(c * rows, rows, rows)
        theirs = ds((1 - c) * rows, rows, rows)
        ost[j] = (own[j, theirs, :] + cr[1, j, theirs, :].astype(F32)).astype(BF16)
        o_send(j).start()
        out_ref[:, ds(j * blk + c * bw, bw, bw)] = (own[j, mine, :] + cr[1, j, mine, :].astype(F32)).astype(BF16)

    def mix(j):
        @pl.when(halves + j < chunks)
        def _():
            forward_far(1, halves + j)

        @pl.when(is_end)
        def _():
            at_end(1, j)
        multiply(1, 1, 1, j, own)

    mix(0)

    def last(j):
        mix(j + 1)
        finish(j)

    each(chunks - 1, last)
    finish(chunks - 1)
    each(chunks, lambda j: o_got(j).wait_recv())

    def settle(j):
        for w in range(2):
            w_swap(w, j).wait_send()
            for side in range(2):
                @pl.when(wanted(w, j, side))
                def _():
                    z_send(w, j, z, side).wait_send()
            for d in range(1, lines - 1):
                for o, side, there in ((z - d, 1, z - d >= 0), (z + d, 0, z + d < lines)):
                    @pl.when(is_mid & there & wanted(w, j, side))
                    def _():
                        z_send(w, j, o, side).wait_send()
        te_swap(j).wait_send()
        o_send(j).wait_send()
        c_send(1, j).wait_send()

        @pl.when(is_mid | (j < kept))
        def _():
            c_send(0, j).wait_send()

        @pl.when(is_host & (j >= kept))
        def _():
            c_send(2, j).wait_send()
            back_send(j).wait_send()

        @pl.when(is_end)
        def _():
            g_send(j).wait_send()

    each(chunks, settle)

    def settle_tokens(g):
        def go(jj):
            t_own(g, jj).wait_send()
            t_send(g, 1, 0, jj).wait_send()
            for dy in range(1, parts):
                t_send(g, 0, dy, jj).wait_send()
                t_relay(g, dy, jj).wait_send()
            for dx, dy in peers:
                t_pass(g, dx, dy, jj).wait_send()
        each(halves, go)

    settle_tokens(0)

    @pl.when(is_host)
    def _():
        settle_tokens(2)

    def settle_hidden(jj):
        h_own(jj, 0).wait_send()
        h_send(1, 0, jj, 0).wait_send()
        for dy in range(1, parts):
            h_send(0, dy, jj, 0).wait_send()
            h_relay(dy, jj).wait_send()
        for dx, dy in peers:
            h_pass(dx, dy, jj).wait_send()

    each(halves, settle_hidden)

    e_send().wait_send()

    @pl.when(z < lines - 1)
    def _():
        chain_send().wait_send()


def per_device(shards, parts, tokens, decay_rate, angle, in_coef, out_coef, skip_coef, gate_weight, out_weight):
    rows, width = tokens.shape
    dims = decay_rate.shape[1]
    lines = shards // 4
    bw = gate_weight.shape[0]
    blk = 2 * bw
    chunks = width // blk
    assert shards % 4 == 0 and lines > 3 and dims % 2 == 0
    assert chunks % 2 == 0 and bw % LANES == 0 and chunks * 2 * parts == shards
    sub = chunks * bw // LANES
    two = 2 * rows
    depth = lines * blk
    skip = skip_coef.reshape(2 * sub, LANES)

    hbm = pl.BlockSpec(memory_space=pltpu.HBM)
    vmem = pl.BlockSpec(memory_space=pltpu.VMEM)
    dma = pltpu.SemaphoreType.DMA
    halves = chunks // 2
    n = 2 * parts
    flops = 2 * 2 * 4 * rows * depth * chunks * bw
    return pl.pallas_call(
        functools.partial(mixer_kernel, lines, parts, dims, chunks - max(1, chunks * GUESTS // 4)),
        in_specs=[hbm] * 7 + [vmem],
        out_specs=vmem,
        out_shape=jax.ShapeDtypeStruct((rows, width), BF16),
        scratch_shapes=[
            pltpu.VMEM((5, dims, chunks * bw), F32),
        ] + [pltpu.VMEM((dims * sub, LANES), F32)] * 6 + [
            pltpu.VMEM((sub, LANES), F32),
            pltpu.VMEM((two, chunks * bw), BF16),
            pltpu.VMEM((two * sub, LANES), F32),
            pltpu.VMEM((two * sub, LANES), F32),
            pltpu.VMEM((2, dims * sub, LANES), F32),
            pltpu.VMEM((2, dims * sub, LANES), BF16),
            pltpu.VMEM((2, dims * sub, LANES), BF16),
            pltpu.VMEM((2, dims * sub, LANES), BF16),
            pltpu.VMEM((2, dims * sub, LANES), BF16),
            pltpu.VMEM((3, 4 * rows, depth), BF16),
            pltpu.VMEM((2, chunks, depth, bw), BF16),
            pltpu.VMEM((chunks, two, bw), F32),
            pltpu.VMEM((chunks, two, bw), F32),
            pltpu.VMEM((3, chunks, two, bw), BF16),
            pltpu.VMEM((3, chunks, two, bw), BF16),
            pltpu.VMEM((chunks, two, bw), BF16),
            pltpu.VMEM((chunks, rows, bw), BF16),
            pltpu.VMEM((rows, width), BF16),
            pltpu.VMEM((chunks, two, bw), BF16),
            dma((2, chunks)),
            dma((chunks,)),
            dma((halves,)),
            dma((5, chunks)),
            dma((2, chunks)),
            dma((2, chunks)),
            dma((chunks,)),
            dma((chunks,)),
            dma((2, 2, chunks, lines)),
            dma((2, chunks, lines)),
            dma((3, n, halves)),
            dma((3, n, halves)),
            dma((3, n, halves)),
            dma((3, n, halves)),
            dma((chunks,)),
            dma((chunks,)),
            dma((chunks,)),
            dma,
            dma,
            dma,
            dma,
            dma((3, chunks)),
            dma((3, chunks)),
            dma((chunks,)),
            dma((chunks,)),
        ],
        compiler_params=pltpu.CompilerParams(
            collective_id=0, has_side_effects=True, vmem_limit_bytes=56 * 1024 * 1024
        ),
        cost_estimate=pl.CostEstimate(flops=flops, bytes_accessed=4 * tokens.size, transcendentals=0),
        name="mixer",
    )(
        tokens, gate_weight, out_weight, decay_rate.T, angle.T, in_coef.T, out_coef.swapaxes(1, 2), skip,
    )


def solution(mesh):
    in_specs = (
        P("seq", "tp"),
        P("tp", None),
        P("tp", None),
        P("tp", None),
        P(None, "tp", None),
        P("tp"),
        P("seq", "tp"),
        P("seq", "tp"),
    )
    body = functools.partial(per_device, mesh.shape["seq"], mesh.shape["tp"])
    return jax.shard_map(body, mesh=mesh, in_specs=in_specs, out_specs=P("seq", "tp"), check_vma=False)
```

```python
import functools

import jax
import jax.numpy as jnp
from jax import lax
from jax.experimental import pallas as pl
from jax.experimental.pallas import tpu as pltpu
from jax.sharding import PartitionSpec as P

LANES = 128
UNROLL = 8
GUESTS = 2
MESH = pl.DeviceIdType.MESH
F32, BF16 = jnp.float32, jnp.bfloat16


def mixer_kernel(
    lines, parts, dims, kept,
    tok, gate_w, out_w, decay, angle, in_coef, out_coef, skip_in,
    out_ref,
    raw, q_re_ref, q_im_ref, c_re_ref, c_im_ref, s_re_ref, s_im_ref, skip_ref, te, x2d, y2d, st, ein, eout, cin, cout, A, W, own, own_g, cs, cr, hid, ost, G, bs,
    l_w, l_te, l_a, l_raw, sw_s, sw_r, te_s, te_r, z_s, z_r, x_s, x_r, p_s, p_r, g_s, g_r, b_s, e_s, e_r, ch_s, ch_r, c_s, c_r, o_s, o_r,
):
    rows, width = tok.shape
    bw = gate_w.shape[0]
    blk = 2 * bw
    chunks = width // blk
    halves = chunks // 2
    sub = chunks * bw // LANES
    tiles = bw // LANES
    two = 2 * rows

    s = lax.axis_index("seq")
    y = lax.axis_index("tp")
    z, x, c = s // 4, (s // 2) % 2, s % 2

    def dev(zz, xx, cc, yy):
        return ((zz * 2 + xx) * 2 + cc, yy)

    partner = dev(z, x, 1 - c, y)
    is_mid = (z > 0) & (z < lines - 1)
    is_end = jnp.logical_not(is_mid)
    is_host = (z == 1) | (z == lines - 2)
    end_z = jnp.where(z == 1, 0, lines - 1)
    host_z = jnp.where(z == 0, 1, lines - 2)

    def hint(v, m):
        return v if isinstance(v, int) else pl.multiple_of(v, m)

    def ds(start, size, m):
        return pl.ds(hint(start, m), size)

    def remote(src, dst, ssem, rsem, where):
        return pltpu.make_async_remote_copy(src, dst, ssem, rsem, device_id=where, device_id_type=MESH)

    weights = (gate_w, out_w)
    others = [(xx, yy) for yy in range(parts) for xx in range(2)]
    peers = others[1:]

    def w_local(w, j):
        return pltpu.make_async_copy(
            weights[w].at[:, ds(j * blk + c * bw, bw, bw)],
            W.at[w, j, ds(z * blk + c * bw, bw, bw)], l_w.at[w, j])

    def w_swap(w, j):
        return remote(
            weights[w].at[:, ds(j * blk + (1 - c) * bw, bw, bw)],
            W.at[w, j, ds(z * blk + c * bw, bw, bw)], sw_s.at[w, j], sw_r.at[w, j], partner)

    def te_local(j):
        return pltpu.make_async_copy(
            tok.at[:, ds(j * blk + c * bw, bw, bw)], te.at[ds(c * rows, rows, rows), ds(j * bw, bw, bw)], l_te.at[j])

    def raw_local(t, j):
        source = (decay, angle, in_coef, out_coef.at[0], out_coef.at[1])[t]
        return pltpu.make_async_copy(
            source.at[:, ds(j * blk + c * bw, bw, bw)], raw.at[t, :, ds(j * bw, bw, bw)], l_raw.at[t, j])

    def te_swap(j):
        return remote(
            tok.at[:, ds(j * blk + (1 - c) * bw, bw, bw)],
            te.at[ds(c * rows, rows, rows), ds(j * bw, bw, bw)], te_s.at[j], te_r.at[j], partner)

    def piece(w, j, o):
        return W.at[w, j, ds(o * blk, blk, blk)]

    def z_send(w, j, o, side):
        where = dev(z + (1 if side else -1), x, c, y)
        return remote(piece(w, j, o), piece(w, j, o), z_s.at[side, w, j, o], z_r.at[w, j, o], where)

    def at_peer(dx, dy):
        return (x + dx) % 2, (y + dy) % parts

    def a_cols(yy, jj):
        return ds((yy * halves + jj) * blk, blk, blk)

    def slot(dx, yy):
        return dx * parts + yy

    def t_from(g, block):
        return (G if g else tok).at[:, ds(block * blk, blk, blk)]

    def t_ref(g, xx, cc, yy, jj):
        return A.at[g, ds((xx * 2 + cc) * rows, rows, rows), a_cols(yy, jj)]

    def t_send(g, dx, dy, jj):
        xx, yy = at_peer(dx, dy)
        return remote(
            t_from(g, 2 * jj + xx), t_ref(g, x, c, y, jj),
            x_s.at[g, dx * parts + dy, jj], x_r.at[g, slot(dx, y), jj], dev(z, xx, c, yy))

    def t_relay(g, dy, jj):
        xx, yy = at_peer(1, dy)
        ref = t_ref(g, xx, c, y, jj)
        return remote(ref, ref, x_s.at[g, parts + dy, jj], x_r.at[g, slot(1, y), jj], dev(z, x, c, yy))

    def t_got(g, dx, dy, jj):
        xx, yy = at_peer(dx, dy)
        ref = t_ref(g, xx, c, yy, jj)
        return remote(ref, ref, x_s.at[g, dx * parts + dy, jj], x_r.at[g, slot(dx, yy), jj], partner)

    def t_local(jj):
        return pltpu.make_async_copy(t_from(0, 2 * jj + x), t_ref(0, x, c, y, jj), l_a.at[jj])

    def t_own(g, jj):
        return remote(
            t_from(g, 2 * jj + x), t_ref(g, x, c, y, jj), p_s.at[g, 0, jj], p_r.at[g, slot(0, y), jj], partner)

    def t_pass(g, dx, dy, jj):
        xx, yy = at_peer(dx, dy)
        ref = t_ref(g, xx, c, yy, jj)
        return remote(ref, ref, p_s.at[g, dx * parts + dy, jj], p_r.at[g, slot(dx, yy), jj], partner)

    def t_passed(g, dx, dy, jj):
        xx, yy = at_peer(dx, dy)
        ref = t_ref(g, xx, 1 - c, yy, jj)
        return remote(ref, ref, p_s.at[g, dx * parts + dy, jj], p_r.at[g, slot(dx, yy), jj], partner)

    def g_send(k):
        ref = G.at[:, ds(k * blk, blk, blk)]
        return remote(t_from(0, k), ref, g_s.at[k], g_r.at[k], dev(host_z, x, c, y))

    def back_send(j):
        return remote(bs.at[j], cr.at[0, j], b_s.at[j], c_r.at[0, j], dev(end_z, x, c, y))

    def h_ref(xx, yy, jj, cc):
        cols = ds((yy * halves + jj) * blk + cc * bw, bw, bw)
        return A.at[1, ds(xx * two, two, two), cols]

    def h_send(dx, dy, jj, j):
        xx, yy = at_peer(dx, dy)
        return remote(
            hid.at[j], h_ref(x, y, jj, c), x_s.at[1, dx * parts + dy, jj], x_r.at[1, slot(dx, y), jj],
            dev(z, xx, c, yy))

    def h_got(dx, dy, jj):
        xx, yy = at_peer(dx, dy)
        ref = h_ref(xx, yy, jj, c)
        return remote(ref, ref, x_s.at[1, dx * parts + dy, jj], x_r.at[1, slot(dx, yy), jj], dev(z, xx, c, yy))

    def h_relay(dy, jj):
        xx, yy = at_peer(1, dy)
        ref = h_ref(xx, y, jj, c)
        return remote(ref, ref, x_s.at[1, parts + dy, jj], x_r.at[1, slot(1, y), jj], dev(z, x, c, yy))

    def h_own(jj, j):
        return remote(hid.at[j], h_ref(x, y, jj, c), p_s.at[1, 0, jj], p_r.at[1, slot(0, y), jj], partner)

    def h_pass(dx, dy, jj):
        xx, yy = at_peer(dx, dy)
        ref = h_ref(xx, yy, jj, c)
        return remote(ref, ref, p_s.at[1, dx * parts + dy, jj], p_r.at[1, slot(dx, yy), jj], partner)

    def h_passed(dx, dy, jj):
        xx, yy = at_peer(dx, dy)
        ref = h_ref(xx, yy, jj, 1 - c)
        return remote(ref, ref, p_s.at[1, dx * parts + dy, jj], p_r.at[1, slot(dx, yy), jj], partner)

    def c_send(w, j):
        return remote(cs.at[w, j], cr.at[w, j], c_s.at[w, j], c_r.at[w, j], dev(z, 1 - x, c, y))

    def e_send():
        return remote(eout, ein, e_s, e_r, dev(z, 1 - x, c, y))

    def chain_send():
        return remote(cout, cin, ch_s, ch_r, dev(z + 1, x, c, y))

    def o_send(j):
        return remote(ost.at[j], out_ref.at[:, ds(j * blk + c * bw, bw, bw)], o_s.at[j], o_r.at[j], partner)

    def o_got(j):
        ref = out_ref.at[:, ds(j * blk + (1 - c) * bw, bw, bw)]
        return remote(ost.at[j], ref, o_s.at[j], o_r.at[j], partner)

    def each(n, f):
        def body(i, carry):
            f(i)
            return carry
        lax.fori_loop(0, n, body, 0)

    each(chunks, lambda j: w_local(0, j).start())
    each(chunks, lambda j: te_local(j).start())
    for t in range(5):
        each(chunks, lambda j: raw_local(t, j).start())
    each(halves, lambda jj: t_local(jj).start())
    each(chunks, lambda j: w_local(1, j).start())

    barrier = pltpu.get_barrier_semaphore()

    def greet(where):
        pl.semaphore_signal(barrier, inc=1, device_id=where, device_id_type=MESH)

    greet(partner)
    for dx, dy in peers:
        xx, yy = at_peer(dx, dy)
        greet(dev(z, xx, c, yy))
    line_peers = [
        (z > 0, dev(z - 1, x, c, y)),
        (z < lines - 1, dev(z + 1, x, c, y)),
    ]
    for there, where in line_peers:
        @pl.when(there)
        def _():
            greet(where)
    pl.semaphore_wait(barrier, 1 + len(peers) + sum(there.astype(jnp.int32) for there, _ in line_peers))

    each(chunks, lambda j: w_swap(0, j).start())

    @pl.when(z == 0)
    def _():
        each(chunks - 1, lambda k: g_send(k).start())

    @pl.when(z == lines - 1)
    def _():
        each(chunks, lambda k: g_send(k).start())

    def t_start(g, jj):
        t_send(g, 1, 0, jj).start()
        for dy in range(1, parts):
            t_send(g, 0, dy, jj).start()
        t_own(g, jj).start()

    each(halves, lambda jj: t_start(0, jj))
    each(chunks, lambda j: te_swap(j).start())
    each(chunks, lambda j: w_swap(1, j).start())

    def own_ready(w, j):
        w_local(w, j).wait()
        w_swap(w, j).wait_recv()

    def wanted(w, j, side):
        target = z + (1 if side else -1)
        inside = (target >= 0) & (target < lines)
        if w == 0:
            inside = inside & (((target > 0) & (target < lines - 1)) | (j < kept))
        return inside

    def outer_side(side):
        target = z + (1 if side else -1)
        return is_end | (target == 0) | (target == lines - 1)

    def own_at(w, j, side, there):
        @pl.when(wanted(w, j, side) & there)
        def _():
            z_send(w, j, z, side).start()

    def own_inner(w, j):
        for side in range(2):
            @pl.when(wanted(w, j, side) & jnp.logical_not(outer_side(side)))
            def _():
                z_send(w, j, z, side).start()

    def hop(w, j, o, side, there):
        @pl.when(there)
        def _():
            z_send(w, j, o, side).wait_recv()

            @pl.when(wanted(w, j, side))
            def _():
                z_send(w, j, o, side).start()

    def relay_cases(d, from_end):
        low, high = z - d, z + d
        if d == 1:
            at_low = (low == 0) if from_end else (low > 0)
            at_high = (high == lines - 1) if from_end else (high < lines - 1)
        else:
            at_low, at_high = low >= 0, high < lines
        return (low, 1, is_mid & at_low), (high, 0, is_mid & at_high)

    def forward_end(w, j, sides=(0, 1)):
        for o, side, there in relay_cases(1, True):
            if side in sides:
                hop(w, j, o, side, there)

    def forward(w, j, d, sides=(0, 1)):
        for o, side, there in relay_cases(d, False):
            if side in sides:
                hop(w, j, o, side, there)

    def forward_far(w, j):
        for d in range(2, lines - 1):
            forward(w, j, d)

    def at_end(w, j):
        for d in range(1, lines):
            @pl.when(z == 0)
            def _():
                z_send(w, j, d, 0).wait_recv()

            @pl.when(z == lines - 1)
            def _():
                z_send(w, j, lines - 1 - d, 0).wait_recv()

    def span(start, stop, f):
        def body(j, carry):
            f(j)
            return carry
        lax.fori_loop(start, stop, body, 0)

    def first_sends(j):
        own_ready(0, j)
        own_at(0, j, 0, z >= 0)
        own_at(0, j, 1, is_mid & (outer_side(1) | (j < halves)))

    each(chunks, first_sends)

    for t in range(5):
        each(chunks, lambda j: raw_local(t, j).wait())
    for e in range(sub):
        band = slice(e * LANES, (e + 1) * LANES)
        rate, theta, scale, o_re, o_im = (raw[t, :, band] for t in range(5))
        magnitude = 1.0 - rate
        scale = scale * jnp.sqrt(1.0 - magnitude * magnitude)
        at = pl.ds(e, dims, stride=sub)
        c_re_ref[at, :] = scale * o_re
        c_im_ref[at, :] = scale * o_im
        q_re_ref[at, :] = magnitude * jnp.cos(theta)
        q_im_ref[at, :] = magnitude * jnp.sin(theta)
        k, lane = e // tiles, e % tiles
        row = 2 * k * tiles + lane
        skip_ref[e:e + 1, :] = jnp.where(c == 0, skip_in[row:row + 1, :], skip_in[row + tiles:row + tiles + 1, :])

    def span_of():
        base = q_re_ref[...], q_im_ref[...]
        total = None
        count = two
        while count:
            if count % 2:
                total = base if total is None else (
                    total[0] * base[0] - total[1] * base[1], total[0] * base[1] + total[1] * base[0])
            base = base[0] * base[0] - base[1] * base[1], 2.0 * base[0] * base[1]
            count //= 2
        s_re_ref[...] = total[0]
        s_im_ref[...] = total[1]

    span_of()

    def te_ready(j):
        te_local(j).wait()
        te_swap(j).wait_recv()

    each(chunks, te_ready)

    def lay(i, carry):
        for e in range(sub):
            v = te[pl.ds(i * 16, 16), e * LANES:(e + 1) * LANES].astype(F32)
            x2d[pl.ds(i * 16 * sub + e, 16, stride=sub), :] = v
        return carry

    lax.fori_loop(0, two // 16, lay, 0)

    def second_own(j):
        own_ready(1, j)
        for side in range(2):
            own_at(1, j, side, is_mid & outer_side(side) & (j < halves))
        own_at(1, j, 0, z == lines - 1)

    each(chunks, second_own)

    half = dims // 2

    def tile(ref, h):
        return ref[h * sub:(h + 1) * sub, :]

    def step(state, v, q_re, q_im):
        return [(a * re - b * im + v, a * im + b * re) for (re, im), a, b in zip(state, q_re, q_im)]

    def end_half(k):
        hs = range(k * half, (k + 1) * half)
        q_re = [tile(q_re_ref, h) for h in hs]
        q_im = [tile(q_im_ref, h) for h in hs]
        zero = jnp.zeros((sub, LANES), F32)

        def body(i, state):
            for u in range(UNROLL):
                state = step(state, x2d[ds((i * UNROLL + u) * sub, sub, sub), :], q_re, q_im)
            return state

        state = lax.fori_loop(0, two // UNROLL, body, [(zero, zero)] * half)
        for h, (re, im) in zip(hs, state):
            st[0, h * sub:(h + 1) * sub, :] = re
            st[1, h * sub:(h + 1) * sub, :] = im

    def took_x(g):
        def go(jj):
            t_got(g, 1, 0, jj).wait_recv()
            for dy in range(1, parts):
                t_relay(g, dy, jj).start()
            t_pass(g, 1, 0, jj).start()
        each(halves, go)

    def took_y(g, dx):
        def go(jj):
            for dy in range(1, parts):
                t_got(g, dx, dy, jj).wait_recv()
                t_pass(g, dx, dy, jj).start()
        each(halves, go)

    end_half(0)
    end_half(1)
    eout[...] = st[...].astype(BF16)
    e_send().start()
    took_x(0)
    inner_left = jnp.logical_not(outer_side(0))
    own_at(1, 0, 0, inner_left)

    def cmul(a, b):
        return a[0] * b[0] - a[1] * b[1], a[0] * b[1] + a[1] * b[0]

    span_q = s_re_ref[...], s_im_ref[...]
    e_send().wait_recv()
    mine = st[0], st[1]
    other = ein[0].astype(F32), ein[1].astype(F32)
    first = [jnp.where(x == 0, m, o) for m, o in zip(mine, other)]
    second = [jnp.where(x == 0, o, m) for m, o in zip(mine, other)]
    plane = [a + b for a, b in zip(cmul(span_q, first), second)]

    @pl.when(z == 0)
    def _():
        cin[...] = jnp.zeros_like(cin)

    @pl.when(z > 0)
    def _():
        chain_send().wait_recv()

    carry = cin[0].astype(F32), cin[1].astype(F32)
    moved = cmul(span_q, carry)
    onward = [a + b for a, b in zip(cmul(span_q, moved), plane)]
    cout[0] = onward[0].astype(BF16)
    cout[1] = onward[1].astype(BF16)

    @pl.when(z < lines - 1)
    def _():
        chain_send().start()

    for k in range(2):
        st[k] = jnp.where(x == 0, carry[k], moved[k] + first[k])

    inner_right = is_mid & jnp.logical_not(outer_side(1))

    @pl.when(z == 0)
    def _():
        g_send(chunks - 1).start()

    each(chunks, lambda j: own_at(0, j, 1, (z == 0) | (inner_right & (j >= halves))))
    each(chunks, lambda j: own_at(1, j, 1, z == 0))
    each(halves, lambda j: forward(0, j, 1))
    took_y(0, 0)

    def guest_tokens(jj):
        @pl.when(is_host)
        def _():
            g_send(2 * jj).wait_recv()
            g_send(2 * jj + 1).wait_recv()
            t_start(2, jj)
            t_ref(2, x, c, y, jj)[...] = t_from(2, 2 * jj + x)[...]

    def smooth_half(k, part, parts_of):
        hs = range(k * half, (k + 1) * half)
        q_re = [tile(q_re_ref, h) for h in hs]
        q_im = [tile(q_im_ref, h) for h in hs]
        c_re = [tile(c_re_ref, h) for h in hs]
        c_im = [tile(c_im_ref, h) for h in hs]
        skip = skip_ref[...]
        state = [(tile(st.at[0], h), tile(st.at[1], h)) for h in hs]

        def body(i, state):
            for u in range(UNROLL):
                at = ds((i * UNROLL + u) * sub, sub, sub)
                v = x2d[at, :]
                state = step(state, v, q_re, q_im)
                sums = [c_re[h] * state[h][0] - c_im[h] * state[h][1] for h in range(half)]
                while len(sums) > 1:
                    sums = [sum(sums[m:m + 2]) for m in range(0, len(sums), 2)]
                before = v * skip if k == 0 else y2d[at, :]
                y2d[at, :] = before + sums[0]
            return state

        steps = two // UNROLL // parts_of
        state = lax.fori_loop(part * steps, (part + 1) * steps, body, state)
        if part + 1 < parts_of:
            for h, (re, im) in zip(hs, state):
                st[0, h * sub:(h + 1) * sub, :] = re
                st[1, h * sub:(h + 1) * sub, :] = im

    def all_tokens(g):
        def go(jj):
            for dx, dy in others:
                t_passed(g, dx, dy, jj).wait_recv()
        each(halves, go)

    def multiply(w, g, k, j, mine):
        right = W[w, j]
        away = jnp.dot(A[g, ds((1 - x) * two, two, two), :], right, preferred_element_type=F32)
        cs[k, j] = away.astype(BF16)
        c_send(k, j).start()
        mine[j] = jnp.dot(A[g, ds(x * two, two, two), :], right, preferred_element_type=F32)

    def project(j):
        @pl.when(is_end & (j < kept))
        def _():
            at_end(0, j)

        @pl.when(is_mid | (j < kept))
        def _():
            multiply(0, 0, 0, j, own)

        @pl.when(is_end & (j >= kept))
        def _():
            own[j] = jnp.zeros((two, bw), F32)

    guest_tokens(0)
    smooth_half(0, 0, 1)
    took_y(0, 1)

    def rest_outer(j):
        for side in range(2):
            own_at(1, j, side, is_mid & outer_side(side))

    rest_outer(halves)
    forward_end(0, 0, (0,))
    span(1, halves, guest_tokens)
    smooth_half(1, 0, 2)
    span(1, halves, lambda j: forward_end(0, j, (0,)))
    forward_end(0, 0, (1,))
    smooth_half(1, 1, 2)

    @pl.when(is_host)
    def _():
        took_x(2)
        took_y(2, 0)

    span(1, halves, lambda j: forward_end(0, j, (1,)))
    each(halves, lambda jj: t_local(jj).wait())
    all_tokens(0)

    def guest_back(j):
        @pl.when(is_host)
        def _():
            c_send(2, j).wait_recv()
            bs[j] = (own_g[j] + cr[2, j].astype(F32)).astype(BF16)
            back_send(j).start()

    def hidden(j):
        c_send(0, j).wait_recv()
        jj = j // 2
        target = j % 2

        def band(i, carry):
            at = pl.ds(pl.multiple_of(i * 16, 16), 16)
            for e in range(tiles):
                lane = slice(e * LANES, (e + 1) * LANES)
                smooth = y2d[pl.ds(i * 16 * sub + j * tiles + e, 16, stride=sub), :]
                gate = own[j, at, lane] + cr[0, j, at, lane].astype(F32)
                value = smooth * jax.nn.sigmoid(smooth) * jax.nn.sigmoid(gate)
                hid[j, at, lane] = value.astype(BF16)
            return carry

        lax.fori_loop(0, two // 16, band, 0)

        @pl.when(target == x)
        def _():
            h_own(jj, j).start()
            for dy in range(1, parts):
                h_send(0, dy, jj, j).start()
            h_ref(x, y, jj, c)[...] = hid[j]

        @pl.when(target != x)
        def _():
            h_send(1, 0, jj, j).start()

    def hidden_x(jj):
        h_got(1, 0, jj).wait_recv()
        for dy in range(1, parts):
            h_relay(dy, jj).start()
        h_pass(1, 0, jj).start()

    def hidden_y(dx, jj):
        for dy in range(1, parts):
            h_got(dx, dy, jj).wait_recv()
            h_pass(dx, dy, jj).start()

    def early_project(j):
        forward_far(0, j)
        forward_end(0, halves + j)
        project(j)

    each(halves, early_project)
    span(halves + 1, chunks, rest_outer)
    own_at(1, 0, 1, inner_right)
    own_inner(1, 1)
    forward(1, 0, 1, (0,))
    span(halves, chunks, lambda j: forward(0, j, 1))

    @pl.when(is_host)
    def _():
        took_y(2, 1)
        all_tokens(2)

    @pl.when(is_end)
    def _():
        each(halves, hidden)

    def guest_sums(j):
        forward_far(0, j)

        @pl.when(is_host & (j >= kept))
        def _():
            multiply(0, 2, 2, j, own_g)

    def guest_step(j):
        guest_sums(j)
        forward_end(1, j - halves)

    span(halves, chunks, guest_step)
    forward(1, 0, 1, (1,))
    span(2, chunks, lambda j: own_inner(1, j))

    @pl.when(is_mid)
    def _():
        each(halves, hidden)

    def late_project(j):
        project(j)

        @pl.when(j >= kept)
        def _():
            guest_back(j)

    span(halves, chunks, late_project)
    span(1, halves, lambda j: forward(1, j, 1))
    forward_far(1, 0)
    span(0, halves // 2, hidden_x)
    hidden(halves)
    span(1, halves, lambda j: forward_far(1, j))
    span(halves + 1, chunks, hidden)
    span(halves, chunks, lambda j: forward_end(1, j))
    span(0, halves // 2, lambda jj: hidden_y(0, jj))
    span(0, halves // 2, lambda jj: hidden_y(1, jj))
    forward(1, halves, 1)
    span(halves // 2, halves, hidden_x)
    span(halves + 1, chunks, lambda j: forward(1, j, 1))
    span(halves // 2, halves, lambda jj: hidden_y(0, jj))
    span(halves // 2, halves, lambda jj: hidden_y(1, jj))

    def all_hidden(jj):
        for dx, dy in others:
            h_passed(dx, dy, jj).wait_recv()

    each(halves, all_hidden)

    def finish(j):
        c_send(1, j).wait_recv()
        mine = ds(c * rows, rows, rows)
        theirs = ds((1 - c) * rows, rows, rows)
        ost[j] = (own[j, theirs, :] + cr[1, j, theirs, :].astype(F32)).astype(BF16)
        o_send(j).start()
        out_ref[:, ds(j * blk + c * bw, bw, bw)] = (own[j, mine, :] + cr[1, j, mine, :].astype(F32)).astype(BF16)

    def mix(j):
        @pl.when(halves + j < chunks)
        def _():
            forward_far(1, halves + j)

        @pl.when(is_end)
        def _():
            at_end(1, j)
        multiply(1, 1, 1, j, own)

    mix(0)

    def last(j):
        mix(j + 1)
        finish(j)

    each(chunks - 1, last)
    finish(chunks - 1)
    each(chunks, lambda j: o_got(j).wait_recv())

    def settle(j):
        for w in range(2):
            w_swap(w, j).wait_send()
            for side in range(2):
                @pl.when(wanted(w, j, side))
                def _():
                    z_send(w, j, z, side).wait_send()
            for d in range(1, lines - 1):
                for o, side, there in ((z - d, 1, z - d >= 0), (z + d, 0, z + d < lines)):
                    @pl.when(is_mid & there & wanted(w, j, side))
                    def _():
                        z_send(w, j, o, side).wait_send()
        te_swap(j).wait_send()
        o_send(j).wait_send()
        c_send(1, j).wait_send()

        @pl.when(is_mid | (j < kept))
        def _():
            c_send(0, j).wait_send()

        @pl.when(is_host & (j >= kept))
        def _():
            c_send(2, j).wait_send()
            back_send(j).wait_send()

        @pl.when(is_end)
        def _():
            g_send(j).wait_send()

    each(chunks, settle)

    def settle_tokens(g):
        def go(jj):
            t_own(g, jj).wait_send()
            t_send(g, 1, 0, jj).wait_send()
            for dy in range(1, parts):
                t_send(g, 0, dy, jj).wait_send()
                t_relay(g, dy, jj).wait_send()
            for dx, dy in peers:
                t_pass(g, dx, dy, jj).wait_send()
        each(halves, go)

    settle_tokens(0)

    @pl.when(is_host)
    def _():
        settle_tokens(2)

    def settle_hidden(jj):
        h_own(jj, 0).wait_send()
        h_send(1, 0, jj, 0).wait_send()
        for dy in range(1, parts):
            h_send(0, dy, jj, 0).wait_send()
            h_relay(dy, jj).wait_send()
        for dx, dy in peers:
            h_pass(dx, dy, jj).wait_send()

    each(halves, settle_hidden)

    e_send().wait_send()

    @pl.when(z < lines - 1)
    def _():
        chain_send().wait_send()


def per_device(shards, parts, tokens, decay_rate, angle, in_coef, out_coef, skip_coef, gate_weight, out_weight):
    rows, width = tokens.shape
    dims = decay_rate.shape[1]
    lines = shards // 4
    bw = gate_weight.shape[0]
    blk = 2 * bw
    chunks = width // blk
    assert shards % 4 == 0 and lines > 3 and dims % 2 == 0
    assert chunks % 2 == 0 and bw % LANES == 0 and chunks * 2 * parts == shards
    sub = chunks * bw // LANES
    two = 2 * rows
    depth = lines * blk
    skip = skip_coef.reshape(2 * sub, LANES)

    hbm = pl.BlockSpec(memory_space=pltpu.HBM)
    vmem = pl.BlockSpec(memory_space=pltpu.VMEM)
    dma = pltpu.SemaphoreType.DMA
    halves = chunks // 2
    n = 2 * parts
    flops = 2 * 2 * 4 * rows * depth * chunks * bw
    return pl.pallas_call(
        functools.partial(mixer_kernel, lines, parts, dims, chunks - max(1, chunks * GUESTS // 4)),
        in_specs=[hbm] * 7 + [vmem],
        out_specs=vmem,
        out_shape=jax.ShapeDtypeStruct((rows, width), BF16),
        scratch_shapes=[
            pltpu.VMEM((5, dims, chunks * bw), F32),
        ] + [pltpu.VMEM((dims * sub, LANES), F32)] * 6 + [
            pltpu.VMEM((sub, LANES), F32),
            pltpu.VMEM((two, chunks * bw), BF16),
            pltpu.VMEM((two * sub, LANES), F32),
            pltpu.VMEM((two * sub, LANES), F32),
            pltpu.VMEM((2, dims * sub, LANES), F32),
            pltpu.VMEM((2, dims * sub, LANES), BF16),
            pltpu.VMEM((2, dims * sub, LANES), BF16),
            pltpu.VMEM((2, dims * sub, LANES), BF16),
            pltpu.VMEM((2, dims * sub, LANES), BF16),
            pltpu.VMEM((3, 4 * rows, depth), BF16),
            pltpu.VMEM((2, chunks, depth, bw), BF16),
            pltpu.VMEM((chunks, two, bw), F32),
            pltpu.VMEM((chunks, two, bw), F32),
            pltpu.VMEM((3, chunks, two, bw), BF16),
            pltpu.VMEM((3, chunks, two, bw), BF16),
            pltpu.VMEM((chunks, two, bw), BF16),
            pltpu.VMEM((chunks, rows, bw), BF16),
            pltpu.VMEM((rows, width), BF16),
            pltpu.VMEM((chunks, two, bw), BF16),
            dma((2, chunks)),
            dma((chunks,)),
            dma((halves,)),
            dma((5, chunks)),
            dma((2, chunks)),
            dma((2, chunks)),
            dma((chunks,)),
            dma((chunks,)),
            dma((2, 2, chunks, lines)),
            dma((2, chunks, lines)),
            dma((3, n, halves)),
            dma((3, n, halves)),
            dma((3, n, halves)),
            dma((3, n, halves)),
            dma((chunks,)),
            dma((chunks,)),
            dma((chunks,)),
            dma,
            dma,
            dma,
            dma,
            dma((3, chunks)),
            dma((3, chunks)),
            dma((chunks,)),
            dma((chunks,)),
        ],
        compiler_params=pltpu.CompilerParams(
            collective_id=0, has_side_effects=True, vmem_limit_bytes=56 * 1024 * 1024
        ),
        cost_estimate=pl.CostEstimate(flops=flops, bytes_accessed=4 * tokens.size, transcendentals=0),
        name="mixer",
    )(
        tokens, gate_weight, out_weight, decay_rate.T, angle.T, in_coef.T, out_coef.swapaxes(1, 2), skip,
    )


def solution(mesh):
    in_specs = (
        P("seq", "tp"),
        P("tp", None),
        P("tp", None),
        P("tp", None),
        P(None, "tp", None),
        P("tp"),
        P("seq", "tp"),
        P("seq", "tp"),
    )
    body = functools.partial(per_device, mesh.shape["seq"], mesh.shape["tp"])
    return jax.shard_map(body, mesh=mesh, in_specs=in_specs, out_specs=P("seq", "tp"), check_vma=False)
```

```python
import functools

import jax
import jax.numpy as jnp
from jax import lax
from jax.experimental import pallas as pl
from jax.experimental.pallas import tpu as pltpu
from jax.sharding import PartitionSpec as P

LANES = 128
UNROLL = 8
GUESTS = 2
MESH = pl.DeviceIdType.MESH
F32, BF16 = jnp.float32, jnp.bfloat16


def mixer_kernel(
    lines, parts, dims, kept,
    tok, gate_w, out_w, decay, angle, in_coef, out_coef, skip_in,
    out_ref,
    raw, q_re_ref, q_im_ref, c_re_ref, c_im_ref, s_re_ref, s_im_ref, skip_ref, te, x2d, y2d, st, ein, eout, cin, cout, A, W, own, own_g, cs, cr, hid, ost, omine, G, bs,
    l_w, l_te, l_a, l_raw, sw_s, sw_r, te_s, te_r, z_s, z_r, x_s, x_r, p_s, p_r, g_s, g_r, b_s, e_s, e_r, ch_s, ch_r, c_s, c_r, o_s, o_r, o_l,
):
    rows, width = tok.shape
    bw = gate_w.shape[0]
    blk = 2 * bw
    chunks = width // blk
    halves = chunks // 2
    sub = chunks * bw // LANES
    tiles = bw // LANES
    two = 2 * rows

    s = lax.axis_index("seq")
    y = lax.axis_index("tp")
    z, x, c = s // 4, (s // 2) % 2, s % 2

    def dev(zz, xx, cc, yy):
        return ((zz * 2 + xx) * 2 + cc, yy)

    partner = dev(z, x, 1 - c, y)
    is_mid = (z > 0) & (z < lines - 1)
    is_end = jnp.logical_not(is_mid)
    is_host = (z == 1) | (z == lines - 2)
    end_z = jnp.where(z == 1, 0, lines - 1)
    host_z = jnp.where(z == 0, 1, lines - 2)

    def hint(v, m):
        return v if isinstance(v, int) else pl.multiple_of(v, m)

    def ds(start, size, m):
        return pl.ds(hint(start, m), size)

    def remote(src, dst, ssem, rsem, where):
        return pltpu.make_async_remote_copy(src, dst, ssem, rsem, device_id=where, device_id_type=MESH)

    weights = (gate_w, out_w)
    others = [(xx, yy) for yy in range(parts) for xx in range(2)]
    peers = others[1:]

    def w_local(w, j):
        return pltpu.make_async_copy(
            weights[w].at[:, ds(j * blk + c * bw, bw, bw)],
            W.at[w, j, ds(z * blk + c * bw, bw, bw)], l_w.at[w, j])

    def w_swap(w, j):
        return remote(
            weights[w].at[:, ds(j * blk + (1 - c) * bw, bw, bw)],
            W.at[w, j, ds(z * blk + c * bw, bw, bw)], sw_s.at[w, j], sw_r.at[w, j], partner)

    def te_local(j):
        return pltpu.make_async_copy(
            tok.at[:, ds(j * blk + c * bw, bw, bw)], te.at[ds(c * rows, rows, rows), ds(j * bw, bw, bw)], l_te.at[j])

    def raw_local(t, j):
        source = (decay, angle, in_coef, out_coef.at[0], out_coef.at[1])[t]
        return pltpu.make_async_copy(
            source.at[:, ds(j * blk + c * bw, bw, bw)], raw.at[t, :, ds(j * bw, bw, bw)], l_raw.at[t, j])

    def te_swap(j):
        return remote(
            tok.at[:, ds(j * blk + (1 - c) * bw, bw, bw)],
            te.at[ds(c * rows, rows, rows), ds(j * bw, bw, bw)], te_s.at[j], te_r.at[j], partner)

    def piece(w, j, o):
        return W.at[w, j, ds(o * blk, blk, blk)]

    def z_send(w, j, o, side):
        where = dev(z + (1 if side else -1), x, c, y)
        return remote(piece(w, j, o), piece(w, j, o), z_s.at[side, w, j, o], z_r.at[w, j, o], where)

    def at_peer(dx, dy):
        return (x + dx) % 2, (y + dy) % parts

    def a_cols(yy, jj):
        return ds((yy * halves + jj) * blk, blk, blk)

    def slot(dx, yy):
        return dx * parts + yy

    def t_from(g, block):
        return (G if g else tok).at[:, ds(block * blk, blk, blk)]

    def t_ref(g, xx, cc, yy, jj):
        return A.at[g, ds((xx * 2 + cc) * rows, rows, rows), a_cols(yy, jj)]

    def t_send(g, dx, dy, jj):
        xx, yy = at_peer(dx, dy)
        return remote(
            t_from(g, 2 * jj + xx), t_ref(g, x, c, y, jj),
            x_s.at[g, dx * parts + dy, jj], x_r.at[g, slot(dx, y), jj], dev(z, xx, c, yy))

    def t_relay(g, dy, jj):
        xx, yy = at_peer(1, dy)
        ref = t_ref(g, xx, c, y, jj)
        return remote(ref, ref, x_s.at[g, parts + dy, jj], x_r.at[g, slot(1, y), jj], dev(z, x, c, yy))

    def t_got(g, dx, dy, jj):
        xx, yy = at_peer(dx, dy)
        ref = t_ref(g, xx, c, yy, jj)
        return remote(ref, ref, x_s.at[g, dx * parts + dy, jj], x_r.at[g, slot(dx, yy), jj], partner)

    def t_local(jj):
        return pltpu.make_async_copy(t_from(0, 2 * jj + x), t_ref(0, x, c, y, jj), l_a.at[jj])

    def t_own(g, jj):
        return remote(
            t_from(g, 2 * jj + x), t_ref(g, x, c, y, jj), p_s.at[g, 0, jj], p_r.at[g, slot(0, y), jj], partner)

    def t_pass(g, dx, dy, jj):
        xx, yy = at_peer(dx, dy)
        ref = t_ref(g, xx, c, yy, jj)
        return remote(ref, ref, p_s.at[g, dx * parts + dy, jj], p_r.at[g, slot(dx, yy), jj], partner)

    def t_passed(g, dx, dy, jj):
        xx, yy = at_peer(dx, dy)
        ref = t_ref(g, xx, 1 - c, yy, jj)
        return remote(ref, ref, p_s.at[g, dx * parts + dy, jj], p_r.at[g, slot(dx, yy), jj], partner)

    def g_send(k):
        ref = G.at[:, ds(k * blk, blk, blk)]
        return remote(t_from(0, k), ref, g_s.at[k], g_r.at[k], dev(host_z, x, c, y))

    def back_send(j):
        return remote(bs.at[j], cr.at[0, j], b_s.at[j], c_r.at[0, j], dev(end_z, x, c, y))

    def h_ref(xx, yy, jj, cc):
        cols = ds((yy * halves + jj) * blk + cc * bw, bw, bw)
        return A.at[1, ds(xx * two, two, two), cols]

    def h_band(xx, yy, jj, r):
        cols = ds((yy * halves + jj) * blk + c * bw, bw, bw)
        return A.at[1, ds(xx * two + r * rows, rows, rows), cols]

    def h_send(dx, dy, jj, j, r):
        xx, yy = at_peer(dx, dy)
        return remote(
            hid.at[j, ds(r * rows, rows, rows)], h_band(x, y, jj, r),
            x_s.at[1 + 2 * r, dx * parts + dy, jj], x_r.at[1 + 2 * r, slot(dx, y), jj], dev(z, xx, c, yy))

    def h_got(dx, dy, jj, r):
        xx, yy = at_peer(dx, dy)
        ref = h_band(xx, yy, jj, r)
        return remote(
            ref, ref, x_s.at[1 + 2 * r, dx * parts + dy, jj], x_r.at[1 + 2 * r, slot(dx, yy), jj], dev(z, xx, c, yy))

    def h_relay(dy, jj, r):
        xx, yy = at_peer(1, dy)
        ref = h_band(xx, y, jj, r)
        return remote(
            ref, ref, x_s.at[1 + 2 * r, parts + dy, jj], x_r.at[1 + 2 * r, slot(1, y), jj], dev(z, x, c, yy))

    def h_own(jj, j):
        return remote(hid.at[j], h_ref(x, y, jj, c), p_s.at[1, 0, jj], p_r.at[1, slot(0, y), jj], partner)

    def h_pass(dx, dy, jj):
        xx, yy = at_peer(dx, dy)
        ref = h_ref(xx, yy, jj, c)
        return remote(ref, ref, p_s.at[1, dx * parts + dy, jj], p_r.at[1, slot(dx, yy), jj], partner)

    def h_passed(dx, dy, jj):
        xx, yy = at_peer(dx, dy)
        ref = h_ref(xx, yy, jj, 1 - c)
        return remote(ref, ref, p_s.at[1, dx * parts + dy, jj], p_r.at[1, slot(dx, yy), jj], partner)

    def c_send(w, j):
        return remote(cs.at[w, j], cr.at[w, j], c_s.at[w, j], c_r.at[w, j], dev(z, 1 - x, c, y))

    def e_send():
        return remote(eout, ein, e_s, e_r, dev(z, 1 - x, c, y))

    def chain_send():
        return remote(cout, cin, ch_s, ch_r, dev(z + 1, x, c, y))

    def o_send(j):
        return remote(ost.at[j], out_ref.at[:, ds(j * blk + c * bw, bw, bw)], o_s.at[j], o_r.at[j], partner)

    def o_keep(j):
        return pltpu.make_async_copy(omine.at[j], out_ref.at[:, ds(j * blk + c * bw, bw, bw)], o_l.at[j])

    def o_got(j):
        ref = out_ref.at[:, ds(j * blk + (1 - c) * bw, bw, bw)]
        return remote(ost.at[j], ref, o_s.at[j], o_r.at[j], partner)

    def each(n, f):
        def body(i, carry):
            f(i)
            return carry
        lax.fori_loop(0, n, body, 0)

    each(chunks, lambda j: w_local(0, j).start())
    each(chunks, lambda j: te_local(j).start())
    for t in range(5):
        each(chunks, lambda j: raw_local(t, j).start())
    each(halves, lambda jj: t_local(jj).start())
    each(chunks, lambda j: w_local(1, j).start())

    barrier = pltpu.get_barrier_semaphore()

    def greet(where):
        pl.semaphore_signal(barrier, inc=1, device_id=where, device_id_type=MESH)

    greet(partner)
    for dx, dy in peers:
        xx, yy = at_peer(dx, dy)
        greet(dev(z, xx, c, yy))
    line_peers = [
        (z > 0, dev(z - 1, x, c, y)),
        (z < lines - 1, dev(z + 1, x, c, y)),
    ]
    for there, where in line_peers:
        @pl.when(there)
        def _():
            greet(where)
    pl.semaphore_wait(barrier, 1 + len(peers) + sum(there.astype(jnp.int32) for there, _ in line_peers))

    each(chunks, lambda j: w_swap(0, j).start())

    @pl.when(z == 0)
    def _():
        each(chunks - 1, lambda k: g_send(k).start())

    @pl.when(z == lines - 1)
    def _():
        each(chunks, lambda k: g_send(k).start())

    def t_start(g, jj):
        t_send(g, 1, 0, jj).start()
        for dy in range(1, parts):
            t_send(g, 0, dy, jj).start()
        t_own(g, jj).start()

    each(halves, lambda jj: t_start(0, jj))
    each(chunks, lambda j: te_swap(j).start())
    each(chunks, lambda j: w_swap(1, j).start())

    def own_ready(w, j):
        w_local(w, j).wait()
        w_swap(w, j).wait_recv()

    def wanted(w, j, side):
        target = z + (1 if side else -1)
        inside = (target >= 0) & (target < lines)
        if w == 0:
            inside = inside & (((target > 0) & (target < lines - 1)) | (j < kept))
        return inside

    def outer_side(side):
        target = z + (1 if side else -1)
        return is_end | (target == 0) | (target == lines - 1)

    def own_at(w, j, side, there):
        @pl.when(wanted(w, j, side) & there)
        def _():
            z_send(w, j, z, side).start()

    def own_inner(w, j):
        for side in range(2):
            @pl.when(wanted(w, j, side) & jnp.logical_not(outer_side(side)))
            def _():
                z_send(w, j, z, side).start()

    def hop(w, j, o, side, there):
        @pl.when(there)
        def _():
            z_send(w, j, o, side).wait_recv()

            @pl.when(wanted(w, j, side))
            def _():
                z_send(w, j, o, side).start()

    def relay_cases(d, from_end):
        low, high = z - d, z + d
        if d == 1:
            at_low = (low == 0) if from_end else (low > 0)
            at_high = (high == lines - 1) if from_end else (high < lines - 1)
        else:
            at_low, at_high = low >= 0, high < lines
        return (low, 1, is_mid & at_low), (high, 0, is_mid & at_high)

    def forward_end(w, j, sides=(0, 1)):
        for o, side, there in relay_cases(1, True):
            if side in sides:
                hop(w, j, o, side, there)

    def forward(w, j, d, sides=(0, 1)):
        for o, side, there in relay_cases(d, False):
            if side in sides:
                hop(w, j, o, side, there)

    def forward_far(w, j):
        for d in range(2, lines - 1):
            forward(w, j, d)

    def at_end(w, j):
        for d in range(1, lines):
            @pl.when(z == 0)
            def _():
                z_send(w, j, d, 0).wait_recv()

            @pl.when(z == lines - 1)
            def _():
                z_send(w, j, lines - 1 - d, 0).wait_recv()

    def span(start, stop, f):
        def body(j, carry):
            f(j)
            return carry
        lax.fori_loop(start, stop, body, 0)

    def first_sends(j):
        own_ready(0, j)
        own_at(0, j, 0, z >= 0)
        own_at(0, j, 1, is_mid & (outer_side(1) | (j < halves)))

    each(chunks, first_sends)

    for t in range(5):
        each(chunks, lambda j: raw_local(t, j).wait())
    for e in range(sub):
        band = slice(e * LANES, (e + 1) * LANES)
        rate, theta, scale, o_re, o_im = (raw[t, :, band] for t in range(5))
        magnitude = 1.0 - rate
        scale = scale * jnp.sqrt(1.0 - magnitude * magnitude)
        at = pl.ds(e, dims, stride=sub)
        c_re_ref[at, :] = scale * o_re
        c_im_ref[at, :] = scale * o_im
        q_re_ref[at, :] = magnitude * jnp.cos(theta)
        q_im_ref[at, :] = magnitude * jnp.sin(theta)
        k, lane = e // tiles, e % tiles
        row = 2 * k * tiles + lane
        skip_ref[e:e + 1, :] = jnp.where(c == 0, skip_in[row:row + 1, :], skip_in[row + tiles:row + tiles + 1, :])

    def span_of():
        base = q_re_ref[...], q_im_ref[...]
        total = None
        count = two
        while count:
            if count % 2:
                total = base if total is None else (
                    total[0] * base[0] - total[1] * base[1], total[0] * base[1] + total[1] * base[0])
            base = base[0] * base[0] - base[1] * base[1], 2.0 * base[0] * base[1]
            count //= 2
        s_re_ref[...] = total[0]
        s_im_ref[...] = total[1]

    span_of()

    def te_ready(j):
        te_local(j).wait()
        te_swap(j).wait_recv()

    each(chunks, te_ready)

    def lay(i, carry):
        for e in range(sub):
            v = te[pl.ds(i * 16, 16), e * LANES:(e + 1) * LANES].astype(F32)
            x2d[pl.ds(i * 16 * sub + e, 16, stride=sub), :] = v
        return carry

    lax.fori_loop(0, two // 16, lay, 0)

    def second_own(j):
        own_ready(1, j)
        for side in range(2):
            own_at(1, j, side, is_mid & outer_side(side) & (j < halves))
        own_at(1, j, 0, z == lines - 1)

    each(chunks, second_own)

    half = dims // 2

    def tile(ref, h):
        return ref[h * sub:(h + 1) * sub, :]

    def step(state, v, q_re, q_im):
        return [(a * re - b * im + v, a * im + b * re) for (re, im), a, b in zip(state, q_re, q_im)]

    def end_half(k):
        hs = range(k * half, (k + 1) * half)
        q_re = [tile(q_re_ref, h) for h in hs]
        q_im = [tile(q_im_ref, h) for h in hs]
        zero = jnp.zeros((sub, LANES), F32)

        def body(i, state):
            for u in range(UNROLL):
                state = step(state, x2d[ds((i * UNROLL + u) * sub, sub, sub), :], q_re, q_im)
            return state

        state = lax.fori_loop(0, two // UNROLL, body, [(zero, zero)] * half)
        for h, (re, im) in zip(hs, state):
            st[0, h * sub:(h + 1) * sub, :] = re
            st[1, h * sub:(h + 1) * sub, :] = im

    def took_x(g):
        def go(jj):
            t_got(g, 1, 0, jj).wait_recv()
            for dy in range(1, parts):
                t_relay(g, dy, jj).start()
            t_pass(g, 1, 0, jj).start()
        each(halves, go)

    def took_y(g, dx):
        def go(jj):
            for dy in range(1, parts):
                t_got(g, dx, dy, jj).wait_recv()
                t_pass(g, dx, dy, jj).start()
        each(halves, go)

    end_half(0)
    end_half(1)
    eout[...] = st[...].astype(BF16)
    e_send().start()
    took_x(0)
    inner_left = jnp.logical_not(outer_side(0))
    own_at(1, 0, 0, inner_left)

    def cmul(a, b):
        return a[0] * b[0] - a[1] * b[1], a[0] * b[1] + a[1] * b[0]

    span_q = s_re_ref[...], s_im_ref[...]
    e_send().wait_recv()
    mine = st[0], st[1]
    other = ein[0].astype(F32), ein[1].astype(F32)
    first = [jnp.where(x == 0, m, o) for m, o in zip(mine, other)]
    second = [jnp.where(x == 0, o, m) for m, o in zip(mine, other)]
    plane = [a + b for a, b in zip(cmul(span_q, first), second)]

    @pl.when(z == 0)
    def _():
        cin[...] = jnp.zeros_like(cin)

    @pl.when(z > 0)
    def _():
        chain_send().wait_recv()

    carry = cin[0].astype(F32), cin[1].astype(F32)
    moved = cmul(span_q, carry)
    onward = [a + b for a, b in zip(cmul(span_q, moved), plane)]
    cout[0] = onward[0].astype(BF16)
    cout[1] = onward[1].astype(BF16)

    @pl.when(z < lines - 1)
    def _():
        chain_send().start()

    for k in range(2):
        st[k] = jnp.where(x == 0, carry[k], moved[k] + first[k])

    inner_right = is_mid & jnp.logical_not(outer_side(1))

    @pl.when(z == 0)
    def _():
        g_send(chunks - 1).start()

    each(chunks, lambda j: own_at(0, j, 1, (z == 0) | (inner_right & (j >= halves))))
    each(chunks, lambda j: own_at(1, j, 1, z == 0))
    each(halves, lambda j: forward(0, j, 1))
    took_y(0, 0)

    def guest_tokens(jj):
        @pl.when(is_host)
        def _():
            g_send(2 * jj).wait_recv()
            g_send(2 * jj + 1).wait_recv()
            t_start(2, jj)
            t_ref(2, x, c, y, jj)[...] = t_from(2, 2 * jj + x)[...]

    def smooth_half(k, part, parts_of):
        hs = range(k * half, (k + 1) * half)
        q_re = [tile(q_re_ref, h) for h in hs]
        q_im = [tile(q_im_ref, h) for h in hs]
        c_re = [tile(c_re_ref, h) for h in hs]
        c_im = [tile(c_im_ref, h) for h in hs]
        skip = skip_ref[...]
        state = [(tile(st.at[0], h), tile(st.at[1], h)) for h in hs]

        def body(i, state):
            for u in range(UNROLL):
                at = ds((i * UNROLL + u) * sub, sub, sub)
                v = x2d[at, :]
                state = step(state, v, q_re, q_im)
                sums = [c_re[h] * state[h][0] - c_im[h] * state[h][1] for h in range(half)]
                while len(sums) > 1:
                    sums = [sum(sums[m:m + 2]) for m in range(0, len(sums), 2)]
                before = v * skip if k == 0 else y2d[at, :]
                y2d[at, :] = before + sums[0]
            return state

        steps = two // UNROLL // parts_of
        state = lax.fori_loop(part * steps, (part + 1) * steps, body, state)
        if part + 1 < parts_of:
            for h, (re, im) in zip(hs, state):
                st[0, h * sub:(h + 1) * sub, :] = re
                st[1, h * sub:(h + 1) * sub, :] = im

    def all_tokens(g):
        def go(jj):
            for dx, dy in others:
                t_passed(g, dx, dy, jj).wait_recv()
        each(halves, go)

    def multiply(w, g, k, j, mine):
        right = W[w, j]
        away = jnp.dot(A[g, ds((1 - x) * two, two, two), :], right, preferred_element_type=F32)
        cs[k, j] = away.astype(BF16)
        c_send(k, j).start()
        mine[j] = jnp.dot(A[g, ds(x * two, two, two), :], right, preferred_element_type=F32)

    def project(j):
        @pl.when(is_end & (j < kept))
        def _():
            at_end(0, j)

        @pl.when(is_mid | (j < kept))
        def _():
            multiply(0, 0, 0, j, own)

        @pl.when(is_end & (j >= kept))
        def _():
            own[j] = jnp.zeros((two, bw), F32)

    guest_tokens(0)
    smooth_half(0, 0, 1)
    took_y(0, 1)

    def rest_outer(j):
        for side in range(2):
            own_at(1, j, side, is_mid & outer_side(side))

    span(halves, chunks, rest_outer)
    forward_end(0, 0, (0,))
    span(1, halves, guest_tokens)
    smooth_half(1, 0, 2)
    span(1, halves, lambda j: forward_end(0, j, (0,)))
    forward_end(0, 0, (1,))
    smooth_half(1, 1, 2)

    @pl.when(is_host)
    def _():
        took_x(2)
        took_y(2, 0)

    span(1, halves, lambda j: forward_end(0, j, (1,)))
    each(halves, lambda jj: t_local(jj).wait())
    all_tokens(0)

    def guest_back(j):
        @pl.when(is_host)
        def _():
            c_send(2, j).wait_recv()
            bs[j] = (own_g[j] + cr[2, j].astype(F32)).astype(BF16)
            back_send(j).start()

    def hidden(j):
        c_send(0, j).wait_recv()
        jj = j // 2
        target = j % 2

        def band(i, carry):
            at = pl.ds(pl.multiple_of(i * 16, 16), 16)
            for e in range(tiles):
                lane = slice(e * LANES, (e + 1) * LANES)
                smooth = y2d[pl.ds(i * 16 * sub + j * tiles + e, 16, stride=sub), :]
                gate = own[j, at, lane] + cr[0, j, at, lane].astype(F32)
                value = smooth * jax.nn.sigmoid(smooth) * jax.nn.sigmoid(gate)
                hid[j, at, lane] = value.astype(BF16)
            return carry

        for r in range(2):
            lax.fori_loop(r * rows // 16, (r + 1) * rows // 16, band, 0)

            @pl.when(target == x)
            def _():
                for dy in range(1, parts):
                    h_send(0, dy, jj, j, r).start()

            @pl.when(target != x)
            def _():
                h_send(1, 0, jj, j, r).start()

        @pl.when(target == x)
        def _():
            h_own(jj, j).start()
            h_ref(x, y, jj, c)[...] = hid[j]

    def hidden_x(jj):
        for r in range(2):
            h_got(1, 0, jj, r).wait_recv()
            for dy in range(1, parts):
                h_relay(dy, jj, r).start()
        h_pass(1, 0, jj).start()

    def hidden_y(dx, jj):
        for dy in range(1, parts):
            for r in range(2):
                h_got(dx, dy, jj, r).wait_recv()
            h_pass(dx, dy, jj).start()

    def early_project(j):
        forward_far(0, j)
        forward_end(0, halves + j)
        project(j)

    each(halves, early_project)
    own_at(1, 0, 1, inner_right)
    own_inner(1, 1)
    forward(1, 0, 1, (0,))
    span(halves, chunks, lambda j: forward(0, j, 1))

    @pl.when(is_host)
    def _():
        took_y(2, 1)
        all_tokens(2)

    @pl.when(is_end)
    def _():
        each(halves, hidden)

    def guest_sums(j):
        forward_far(0, j)

        @pl.when(is_host & (j >= kept))
        def _():
            multiply(0, 2, 2, j, own_g)

    def guest_step(j):
        guest_sums(j)
        forward_end(1, j - halves)

    span(halves, chunks, guest_step)
    forward(1, 0, 1, (1,))
    span(2, chunks, lambda j: own_inner(1, j))

    @pl.when(is_mid)
    def _():
        each(halves, hidden)

    def late_project(j):
        project(j)

        @pl.when(j >= kept)
        def _():
            guest_back(j)

    span(halves, chunks, late_project)
    span(1, halves, lambda j: forward(1, j, 1))
    forward_far(1, 0)
    span(0, halves // 2, hidden_x)
    hidden(halves)
    span(1, halves, lambda j: forward_far(1, j))
    span(halves + 1, chunks, hidden)
    span(halves, chunks, lambda j: forward_end(1, j))
    span(0, halves // 2, lambda jj: hidden_y(0, jj))
    span(0, halves // 2, lambda jj: hidden_y(1, jj))
    forward(1, halves, 1)
    span(halves // 2, halves, hidden_x)
    span(halves + 1, chunks, lambda j: forward(1, j, 1))
    span(halves // 2, halves, lambda jj: hidden_y(0, jj))
    span(halves // 2, halves, lambda jj: hidden_y(1, jj))

    def all_hidden(jj):
        for dx, dy in others:
            h_passed(dx, dy, jj).wait_recv()

    each(halves, all_hidden)

    def finish(j):
        c_send(1, j).wait_recv()
        mine = ds(c * rows, rows, rows)
        theirs = ds((1 - c) * rows, rows, rows)
        ost[j] = (own[j, theirs, :] + cr[1, j, theirs, :].astype(F32)).astype(BF16)
        o_send(j).start()
        omine[j] = (own[j, mine, :] + cr[1, j, mine, :].astype(F32)).astype(BF16)
        o_keep(j).start()

    def mix(j):
        @pl.when(halves + j < chunks)
        def _():
            forward_far(1, halves + j)

        @pl.when(is_end)
        def _():
            at_end(1, j)
        multiply(1, 1, 1, j, own)

    mix(0)

    def last(j):
        mix(j + 1)
        finish(j)

    each(chunks - 1, last)
    finish(chunks - 1)
    each(chunks, lambda j: o_keep(j).wait())
    each(chunks, lambda j: o_got(j).wait_recv())

    def settle(j):
        for w in range(2):
            w_swap(w, j).wait_send()
            for side in range(2):
                @pl.when(wanted(w, j, side))
                def _():
                    z_send(w, j, z, side).wait_send()
            for d in range(1, lines - 1):
                for o, side, there in ((z - d, 1, z - d >= 0), (z + d, 0, z + d < lines)):
                    @pl.when(is_mid & there & wanted(w, j, side))
                    def _():
                        z_send(w, j, o, side).wait_send()
        te_swap(j).wait_send()
        o_send(j).wait_send()
        c_send(1, j).wait_send()

        @pl.when(is_mid | (j < kept))
        def _():
            c_send(0, j).wait_send()

        @pl.when(is_host & (j >= kept))
        def _():
            c_send(2, j).wait_send()
            back_send(j).wait_send()

        @pl.when(is_end)
        def _():
            g_send(j).wait_send()

    each(chunks, settle)

    def settle_tokens(g):
        def go(jj):
            t_own(g, jj).wait_send()
            t_send(g, 1, 0, jj).wait_send()
            for dy in range(1, parts):
                t_send(g, 0, dy, jj).wait_send()
                t_relay(g, dy, jj).wait_send()
            for dx, dy in peers:
                t_pass(g, dx, dy, jj).wait_send()
        each(halves, go)

    settle_tokens(0)

    @pl.when(is_host)
    def _():
        settle_tokens(2)

    def settle_hidden(jj):
        h_own(jj, 0).wait_send()
        for r in range(2):
            h_send(1, 0, jj, 0, r).wait_send()
            for dy in range(1, parts):
                h_send(0, dy, jj, 0, r).wait_send()
                h_relay(dy, jj, r).wait_send()
        for dx, dy in peers:
            h_pass(dx, dy, jj).wait_send()

    each(halves, settle_hidden)

    e_send().wait_send()

    @pl.when(z < lines - 1)
    def _():
        chain_send().wait_send()


def per_device(shards, parts, tokens, decay_rate, angle, in_coef, out_coef, skip_coef, gate_weight, out_weight):
    rows, width = tokens.shape
    dims = decay_rate.shape[1]
    lines = shards // 4
    bw = gate_weight.shape[0]
    blk = 2 * bw
    chunks = width // blk
    assert shards % 4 == 0 and lines > 3 and dims % 2 == 0
    assert chunks % 2 == 0 and bw % LANES == 0 and chunks * 2 * parts == shards
    sub = chunks * bw // LANES
    two = 2 * rows
    depth = lines * blk
    skip = skip_coef.reshape(2 * sub, LANES)

    hbm = pl.BlockSpec(memory_space=pltpu.HBM)
    vmem = pl.BlockSpec(memory_space=pltpu.VMEM)
    dma = pltpu.SemaphoreType.DMA
    halves = chunks // 2
    n = 2 * parts
    flops = 2 * 2 * 4 * rows * depth * chunks * bw
    return pl.pallas_call(
        functools.partial(mixer_kernel, lines, parts, dims, chunks - max(1, chunks * GUESTS // 4)),
        in_specs=[hbm] * 7 + [vmem],
        out_specs=hbm,
        out_shape=jax.ShapeDtypeStruct((rows, width), BF16),
        scratch_shapes=[
            pltpu.VMEM((5, dims, chunks * bw), F32),
        ] + [pltpu.VMEM((dims * sub, LANES), F32)] * 6 + [
            pltpu.VMEM((sub, LANES), F32),
            pltpu.VMEM((two, chunks * bw), BF16),
            pltpu.VMEM((two * sub, LANES), F32),
            pltpu.VMEM((two * sub, LANES), F32),
            pltpu.VMEM((2, dims * sub, LANES), F32),
            pltpu.VMEM((2, dims * sub, LANES), BF16),
            pltpu.VMEM((2, dims * sub, LANES), BF16),
            pltpu.VMEM((2, dims * sub, LANES), BF16),
            pltpu.VMEM((2, dims * sub, LANES), BF16),
            pltpu.VMEM((3, 4 * rows, depth), BF16),
            pltpu.VMEM((2, chunks, depth, bw), BF16),
            pltpu.VMEM((chunks, two, bw), F32),
            pltpu.VMEM((chunks, two, bw), F32),
            pltpu.VMEM((3, chunks, two, bw), BF16),
            pltpu.VMEM((3, chunks, two, bw), BF16),
            pltpu.VMEM((chunks, two, bw), BF16),
            pltpu.VMEM((chunks, rows, bw), BF16),
            pltpu.VMEM((chunks, rows, bw), BF16),
            pltpu.VMEM((rows, width), BF16),
            pltpu.VMEM((chunks, two, bw), BF16),
            dma((2, chunks)),
            dma((chunks,)),
            dma((halves,)),
            dma((5, chunks)),
            dma((2, chunks)),
            dma((2, chunks)),
            dma((chunks,)),
            dma((chunks,)),
            dma((2, 2, chunks, lines)),
            dma((2, chunks, lines)),
            dma((4, n, halves)),
            dma((4, n, halves)),
            dma((3, n, halves)),
            dma((3, n, halves)),
            dma((chunks,)),
            dma((chunks,)),
            dma((chunks,)),
            dma,
            dma,
            dma,
            dma,
            dma((3, chunks)),
            dma((3, chunks)),
            dma((chunks,)),
            dma((chunks,)),
            dma((chunks,)),
        ],
        compiler_params=pltpu.CompilerParams(
            collective_id=0, has_side_effects=True, vmem_limit_bytes=56 * 1024 * 1024
        ),
        cost_estimate=pl.CostEstimate(flops=flops, bytes_accessed=4 * tokens.size, transcendentals=0),
        name="mixer",
    )(
        tokens, gate_weight, out_weight, decay_rate.T, angle.T, in_coef.T, out_coef.swapaxes(1, 2), skip,
    )


def solution(mesh):
    in_specs = (
        P("seq", "tp"),
        P("tp", None),
        P("tp", None),
        P("tp", None),
        P(None, "tp", None),
        P("tp"),
        P("seq", "tp"),
        P("seq", "tp"),
    )
    body = functools.partial(per_device, mesh.shape["seq"], mesh.shape["tp"])
    return jax.shard_map(body, mesh=mesh, in_specs=in_specs, out_specs=P("seq", "tp"), check_vma=False)
```

```python
import functools

import jax
import jax.numpy as jnp
from jax import lax
from jax.experimental import pallas as pl
from jax.experimental.pallas import tpu as pltpu
from jax.sharding import PartitionSpec as P

LANES = 128
UNROLL = 8
GUESTS = 2
MESH = pl.DeviceIdType.MESH
F32, BF16 = jnp.float32, jnp.bfloat16


def mixer_kernel(
    lines, parts, dims, kept,
    tok, gate_w, out_w, decay, angle, in_coef, out_coef, skip_in,
    out_ref,
    raw, q_re_ref, q_im_ref, c_re_ref, c_im_ref, s_re_ref, s_im_ref, skip_ref, te, x2d, y2d, st, ein, eout, cin, cout, A, W, own, own_g, cs, cr, hid, ost, omine, G, bs,
    l_w, l_te, l_a, l_raw, sw_s, sw_r, te_s, te_r, z_s, z_r, x_s, x_r, p_s, p_r, g_s, g_r, b_s, e_s, e_r, ch_s, ch_r, c_s, c_r, o_s, o_r, o_l,
):
    rows, width = tok.shape
    bw = gate_w.shape[0]
    blk = 2 * bw
    chunks = width // blk
    halves = chunks // 2
    sub = chunks * bw // LANES
    tiles = bw // LANES
    two = 2 * rows

    s = lax.axis_index("seq")
    y = lax.axis_index("tp")
    z, x, c = s // 4, (s // 2) % 2, s % 2

    def dev(zz, xx, cc, yy):
        return ((zz * 2 + xx) * 2 + cc, yy)

    partner = dev(z, x, 1 - c, y)
    is_mid = (z > 0) & (z < lines - 1)
    is_end = jnp.logical_not(is_mid)
    is_host = (z == 1) | (z == lines - 2)
    end_z = jnp.where(z == 1, 0, lines - 1)
    host_z = jnp.where(z == 0, 1, lines - 2)

    def hint(v, m):
        return v if isinstance(v, int) else pl.multiple_of(v, m)

    def ds(start, size, m):
        return pl.ds(hint(start, m), size)

    def remote(src, dst, ssem, rsem, where):
        return pltpu.make_async_remote_copy(src, dst, ssem, rsem, device_id=where, device_id_type=MESH)

    weights = (gate_w, out_w)
    others = [(xx, yy) for yy in range(parts) for xx in range(2)]
    peers = others[1:]

    def w_local(w, j):
        return pltpu.make_async_copy(
            weights[w].at[:, ds(j * blk + c * bw, bw, bw)],
            W.at[w, j, ds(z * blk + c * bw, bw, bw)], l_w.at[w, j])

    def w_swap(w, j):
        return remote(
            weights[w].at[:, ds(j * blk + (1 - c) * bw, bw, bw)],
            W.at[w, j, ds(z * blk + c * bw, bw, bw)], sw_s.at[w], sw_r.at[w, j], partner)

    def te_local(j):
        return pltpu.make_async_copy(
            tok.at[:, ds(j * blk + c * bw, bw, bw)], te.at[ds(c * rows, rows, rows), ds(j * bw, bw, bw)], l_te)

    def raw_local(t, j):
        source = (decay, angle, in_coef, out_coef.at[0], out_coef.at[1])[t]
        return pltpu.make_async_copy(
            source.at[:, ds(j * blk + c * bw, bw, bw)], raw.at[t, :, ds(j * bw, bw, bw)], l_raw)

    def te_swap(j):
        return remote(
            tok.at[:, ds(j * blk + (1 - c) * bw, bw, bw)],
            te.at[ds(c * rows, rows, rows), ds(j * bw, bw, bw)], te_s, te_r, partner)

    def piece(w, j, o):
        return W.at[w, j, ds(o * blk, blk, blk)]

    def z_send(w, j, o, side):
        where = dev(z + (1 if side else -1), x, c, y)
        return remote(piece(w, j, o), piece(w, j, o), z_s.at[side, w], z_r.at[w, j, o], where)

    def at_peer(dx, dy):
        return (x + dx) % 2, (y + dy) % parts

    def a_cols(yy, jj):
        return ds((yy * halves + jj) * blk, blk, blk)

    def slot(dx, yy):
        return dx * parts + yy

    def t_from(g, block):
        return (G if g else tok).at[:, ds(block * blk, blk, blk)]

    def t_ref(g, xx, cc, yy, jj):
        return A.at[g, ds((xx * 2 + cc) * rows, rows, rows), a_cols(yy, jj)]

    def t_send(g, dx, dy, jj):
        xx, yy = at_peer(dx, dy)
        return remote(
            t_from(g, 2 * jj + xx), t_ref(g, x, c, y, jj),
            x_s.at[g, dx * parts + dy, jj], x_r.at[g, slot(dx, y), jj], dev(z, xx, c, yy))

    def t_relay(g, dy, jj):
        xx, yy = at_peer(1, dy)
        ref = t_ref(g, xx, c, y, jj)
        return remote(ref, ref, x_s.at[g, parts + dy, jj], x_r.at[g, slot(1, y), jj], dev(z, x, c, yy))

    def t_got(g, dx, dy, jj):
        xx, yy = at_peer(dx, dy)
        ref = t_ref(g, xx, c, yy, jj)
        return remote(ref, ref, x_s.at[g, dx * parts + dy, jj], x_r.at[g, slot(dx, yy), jj], partner)

    def t_local(jj):
        return pltpu.make_async_copy(t_from(0, 2 * jj + x), t_ref(0, x, c, y, jj), l_a.at[jj])

    def t_own(g, jj):
        return remote(
            t_from(g, 2 * jj + x), t_ref(g, x, c, y, jj), p_s.at[g, 0, jj], p_r.at[g, slot(0, y), jj], partner)

    def t_pass(g, dx, dy, jj):
        xx, yy = at_peer(dx, dy)
        ref = t_ref(g, xx, c, yy, jj)
        return remote(ref, ref, p_s.at[g, dx * parts + dy, jj], p_r.at[g, slot(dx, yy), jj], partner)

    def t_passed(g, dx, dy, jj):
        xx, yy = at_peer(dx, dy)
        ref = t_ref(g, xx, 1 - c, yy, jj)
        return remote(ref, ref, p_s.at[g, dx * parts + dy, jj], p_r.at[g, slot(dx, yy), jj], partner)

    def g_send(k):
        ref = G.at[:, ds(k * blk, blk, blk)]
        return remote(t_from(0, k), ref, g_s, g_r.at[k], dev(host_z, x, c, y))

    def back_send(j):
        return remote(bs.at[j], cr.at[0, j], b_s, c_r.at[0, j], dev(end_z, x, c, y))

    def h_ref(xx, yy, jj, cc):
        cols = ds((yy * halves + jj) * blk + cc * bw, bw, bw)
        return A.at[1, ds(xx * two, two, two), cols]

    def h_band(xx, yy, jj, r):
        cols = ds((yy * halves + jj) * blk + c * bw, bw, bw)
        return A.at[1, ds(xx * two + r * rows, rows, rows), cols]

    def h_send(dx, dy, jj, j, r):
        xx, yy = at_peer(dx, dy)
        return remote(
            hid.at[j, ds(r * rows, rows, rows)], h_band(x, y, jj, r),
            x_s.at[1 + 2 * r, dx * parts + dy, jj], x_r.at[1 + 2 * r, slot(dx, y), jj], dev(z, xx, c, yy))

    def h_got(dx, dy, jj, r):
        xx, yy = at_peer(dx, dy)
        ref = h_band(xx, yy, jj, r)
        return remote(
            ref, ref, x_s.at[1 + 2 * r, dx * parts + dy, jj], x_r.at[1 + 2 * r, slot(dx, yy), jj], dev(z, xx, c, yy))

    def h_relay(dy, jj, r):
        xx, yy = at_peer(1, dy)
        ref = h_band(xx, y, jj, r)
        return remote(
            ref, ref, x_s.at[1 + 2 * r, parts + dy, jj], x_r.at[1 + 2 * r, slot(1, y), jj], dev(z, x, c, yy))

    def h_own(jj, j):
        return remote(hid.at[j], h_ref(x, y, jj, c), p_s.at[1, 0, jj], p_r.at[1, slot(0, y), jj], partner)

    def h_pass(dx, dy, jj):
        xx, yy = at_peer(dx, dy)
        ref = h_ref(xx, yy, jj, c)
        return remote(ref, ref, p_s.at[1, dx * parts + dy, jj], p_r.at[1, slot(dx, yy), jj], partner)

    def h_passed(dx, dy, jj):
        xx, yy = at_peer(dx, dy)
        ref = h_ref(xx, yy, jj, 1 - c)
        return remote(ref, ref, p_s.at[1, dx * parts + dy, jj], p_r.at[1, slot(dx, yy), jj], partner)

    def c_send(w, j):
        return remote(cs.at[w, j], cr.at[w, j], c_s.at[w], c_r.at[w, j], dev(z, 1 - x, c, y))

    def e_send():
        return remote(eout, ein, e_s, e_r, dev(z, 1 - x, c, y))

    def chain_send():
        return remote(cout, cin, ch_s, ch_r, dev(z + 1, x, c, y))

    def o_send(j):
        return remote(ost.at[j], out_ref.at[:, ds(j * blk + c * bw, bw, bw)], o_s, o_r, partner)

    def o_keep(j):
        return pltpu.make_async_copy(omine.at[j], out_ref.at[:, ds(j * blk + c * bw, bw, bw)], o_l)

    def o_got(j):
        ref = out_ref.at[:, ds(j * blk + (1 - c) * bw, bw, bw)]
        return remote(ost.at[j], ref, o_s, o_r, partner)

    def each(n, f):
        def body(i, carry):
            f(i)
            return carry
        lax.fori_loop(0, n, body, 0)

    each(chunks, lambda j: w_local(0, j).start())
    each(chunks, lambda j: te_local(j).start())
    for t in range(5):
        each(chunks, lambda j: raw_local(t, j).start())
    each(halves, lambda jj: t_local(jj).start())
    each(chunks, lambda j: w_local(1, j).start())

    barrier = pltpu.get_barrier_semaphore()

    def greet(where):
        pl.semaphore_signal(barrier, inc=1, device_id=where, device_id_type=MESH)

    greet(partner)
    for dx, dy in peers:
        xx, yy = at_peer(dx, dy)
        greet(dev(z, xx, c, yy))
    line_peers = [
        (z > 0, dev(z - 1, x, c, y)),
        (z < lines - 1, dev(z + 1, x, c, y)),
    ]
    for there, where in line_peers:
        @pl.when(there)
        def _():
            greet(where)
    pl.semaphore_wait(barrier, 1 + len(peers) + sum(there.astype(jnp.int32) for there, _ in line_peers))

    each(chunks, lambda j: w_swap(0, j).start())

    @pl.when(z == 0)
    def _():
        each(chunks - 1, lambda k: g_send(k).start())

    @pl.when(z == lines - 1)
    def _():
        each(chunks, lambda k: g_send(k).start())

    def t_start(g, jj):
        t_send(g, 1, 0, jj).start()
        for dy in range(1, parts):
            t_send(g, 0, dy, jj).start()
        t_own(g, jj).start()

    each(halves, lambda jj: t_start(0, jj))
    each(chunks, lambda j: te_swap(j).start())
    each(chunks, lambda j: w_swap(1, j).start())

    def own_ready(w, j):
        w_local(w, j).wait()
        w_swap(w, j).wait_recv()

    def wanted(w, j, side):
        target = z + (1 if side else -1)
        inside = (target >= 0) & (target < lines)
        if w == 0:
            inside = inside & (((target > 0) & (target < lines - 1)) | (j < kept))
        return inside

    def outer_side(side):
        target = z + (1 if side else -1)
        return is_end | (target == 0) | (target == lines - 1)

    def own_at(w, j, side, there):
        @pl.when(wanted(w, j, side) & there)
        def _():
            z_send(w, j, z, side).start()

    def own_inner(w, j):
        for side in range(2):
            @pl.when(wanted(w, j, side) & jnp.logical_not(outer_side(side)))
            def _():
                z_send(w, j, z, side).start()

    def hop(w, j, o, side, there):
        @pl.when(there)
        def _():
            z_send(w, j, o, side).wait_recv()

            @pl.when(wanted(w, j, side))
            def _():
                z_send(w, j, o, side).start()

    def relay_cases(d, from_end):
        low, high = z - d, z + d
        if d == 1:
            at_low = (low == 0) if from_end else (low > 0)
            at_high = (high == lines - 1) if from_end else (high < lines - 1)
        else:
            at_low, at_high = low >= 0, high < lines
        return (low, 1, is_mid & at_low), (high, 0, is_mid & at_high)

    def forward_end(w, j, sides=(0, 1)):
        for o, side, there in relay_cases(1, True):
            if side in sides:
                hop(w, j, o, side, there)

    def forward(w, j, d, sides=(0, 1)):
        for o, side, there in relay_cases(d, False):
            if side in sides:
                hop(w, j, o, side, there)

    def forward_far(w, j):
        for d in range(2, lines - 1):
            forward(w, j, d)

    def at_end(w, j):
        for d in range(1, lines):
            @pl.when(z == 0)
            def _():
                z_send(w, j, d, 0).wait_recv()

            @pl.when(z == lines - 1)
            def _():
                z_send(w, j, lines - 1 - d, 0).wait_recv()

    def span(start, stop, f):
        def body(j, carry):
            f(j)
            return carry
        lax.fori_loop(start, stop, body, 0)

    def first_sends(j):
        own_ready(0, j)
        own_at(0, j, 0, z >= 0)
        own_at(0, j, 1, is_mid & (outer_side(1) | (j < halves)))

    each(chunks, first_sends)

    pltpu.make_async_copy(raw, raw, l_raw).wait()
    for e in range(sub):
        band = slice(e * LANES, (e + 1) * LANES)
        rate, theta, scale, o_re, o_im = (raw[t, :, band] for t in range(5))
        magnitude = 1.0 - rate
        scale = scale * jnp.sqrt(1.0 - magnitude * magnitude)
        at = pl.ds(e, dims, stride=sub)
        c_re_ref[at, :] = scale * o_re
        c_im_ref[at, :] = scale * o_im
        q_re_ref[at, :] = magnitude * jnp.cos(theta)
        q_im_ref[at, :] = magnitude * jnp.sin(theta)
        k, lane = e // tiles, e % tiles
        row = 2 * k * tiles + lane
        skip_ref[e:e + 1, :] = jnp.where(c == 0, skip_in[row:row + 1, :], skip_in[row + tiles:row + tiles + 1, :])

    def span_of():
        base = q_re_ref[...], q_im_ref[...]
        total = None
        count = two
        while count:
            if count % 2:
                total = base if total is None else (
                    total[0] * base[0] - total[1] * base[1], total[0] * base[1] + total[1] * base[0])
            base = base[0] * base[0] - base[1] * base[1], 2.0 * base[0] * base[1]
            count //= 2
        s_re_ref[...] = total[0]
        s_im_ref[...] = total[1]

    span_of()

    te_mine = te.at[ds(c * rows, rows, rows), :]
    te_theirs = te.at[ds((1 - c) * rows, rows, rows), :]
    pltpu.make_async_copy(te_mine, te_mine, l_te).wait()
    remote(te_theirs, te_theirs, te_s, te_r, partner).wait_recv()

    def lay(i, carry):
        for e in range(sub):
            v = te[pl.ds(i * 16, 16), e * LANES:(e + 1) * LANES].astype(F32)
            x2d[pl.ds(i * 16 * sub + e, 16, stride=sub), :] = v
        return carry

    lax.fori_loop(0, two // 16, lay, 0)

    def second_own(j):
        own_ready(1, j)
        for side in range(2):
            own_at(1, j, side, is_mid & outer_side(side) & (j < halves))
        own_at(1, j, 0, z == lines - 1)

    each(chunks, second_own)

    half = dims // 2

    def tile(ref, h):
        return ref[h * sub:(h + 1) * sub, :]

    def step(state, v, q_re, q_im):
        return [(a * re - b * im + v, a * im + b * re) for (re, im), a, b in zip(state, q_re, q_im)]

    def end_half(k):
        hs = range(k * half, (k + 1) * half)
        q_re = [tile(q_re_ref, h) for h in hs]
        q_im = [tile(q_im_ref, h) for h in hs]
        zero = jnp.zeros((sub, LANES), F32)

        def body(i, state):
            for u in range(UNROLL):
                state = step(state, x2d[ds((i * UNROLL + u) * sub, sub, sub), :], q_re, q_im)
            return state

        state = lax.fori_loop(0, two // UNROLL, body, [(zero, zero)] * half)
        for h, (re, im) in zip(hs, state):
            st[0, h * sub:(h + 1) * sub, :] = re
            st[1, h * sub:(h + 1) * sub, :] = im

    def took_x(g):
        def go(jj):
            t_got(g, 1, 0, jj).wait_recv()
            for dy in range(1, parts):
                t_relay(g, dy, jj).start()
            t_pass(g, 1, 0, jj).start()
        each(halves, go)

    def took_y(g, dx):
        def go(jj):
            for dy in range(1, parts):
                t_got(g, dx, dy, jj).wait_recv()
                t_pass(g, dx, dy, jj).start()
        each(halves, go)

    end_half(0)
    end_half(1)
    eout[...] = st[...].astype(BF16)
    e_send().start()
    took_x(0)
    inner_left = jnp.logical_not(outer_side(0))
    own_at(1, 0, 0, inner_left)

    def cmul(a, b):
        return a[0] * b[0] - a[1] * b[1], a[0] * b[1] + a[1] * b[0]

    span_q = s_re_ref[...], s_im_ref[...]
    e_send().wait_recv()
    mine = st[0], st[1]
    other = ein[0].astype(F32), ein[1].astype(F32)
    first = [jnp.where(x == 0, m, o) for m, o in zip(mine, other)]
    second = [jnp.where(x == 0, o, m) for m, o in zip(mine, other)]
    plane = [a + b for a, b in zip(cmul(span_q, first), second)]

    @pl.when(z == 0)
    def _():
        cin[...] = jnp.zeros_like(cin)

    @pl.when(z > 0)
    def _():
        chain_send().wait_recv()

    carry = cin[0].astype(F32), cin[1].astype(F32)
    moved = cmul(span_q, carry)
    onward = [a + b for a, b in zip(cmul(span_q, moved), plane)]
    cout[0] = onward[0].astype(BF16)
    cout[1] = onward[1].astype(BF16)

    @pl.when(z < lines - 1)
    def _():
        chain_send().start()

    for k in range(2):
        st[k] = jnp.where(x == 0, carry[k], moved[k] + first[k])

    inner_right = is_mid & jnp.logical_not(outer_side(1))

    @pl.when(z == 0)
    def _():
        g_send(chunks - 1).start()

    each(chunks, lambda j: own_at(0, j, 1, (z == 0) | (inner_right & (j >= halves))))
    each(chunks, lambda j: own_at(1, j, 1, z == 0))
    each(halves, lambda j: forward(0, j, 1))
    took_y(0, 0)

    def guest_tokens(jj):
        @pl.when(is_host)
        def _():
            g_send(2 * jj).wait_recv()
            g_send(2 * jj + 1).wait_recv()
            t_start(2, jj)
            t_ref(2, x, c, y, jj)[...] = t_from(2, 2 * jj + x)[...]

    def smooth_half(k, part, parts_of):
        hs = range(k * half, (k + 1) * half)
        q_re = [tile(q_re_ref, h) for h in hs]
        q_im = [tile(q_im_ref, h) for h in hs]
        c_re = [tile(c_re_ref, h) for h in hs]
        c_im = [tile(c_im_ref, h) for h in hs]
        skip = skip_ref[...]
        state = [(tile(st.at[0], h), tile(st.at[1], h)) for h in hs]

        def body(i, state):
            for u in range(UNROLL):
                at = ds((i * UNROLL + u) * sub, sub, sub)
                v = x2d[at, :]
                state = step(state, v, q_re, q_im)
                sums = [c_re[h] * state[h][0] - c_im[h] * state[h][1] for h in range(half)]
                while len(sums) > 1:
                    sums = [sum(sums[m:m + 2]) for m in range(0, len(sums), 2)]
                before = v * skip if k == 0 else y2d[at, :]
                y2d[at, :] = before + sums[0]
            return state

        steps = two // UNROLL // parts_of
        state = lax.fori_loop(part * steps, (part + 1) * steps, body, state)
        if part + 1 < parts_of:
            for h, (re, im) in zip(hs, state):
                st[0, h * sub:(h + 1) * sub, :] = re
                st[1, h * sub:(h + 1) * sub, :] = im

    def all_tokens(g):
        def go(jj):
            for dx, dy in others:
                t_passed(g, dx, dy, jj).wait_recv()
        each(halves, go)

    def multiply(w, g, k, j, mine):
        right = W[w, j]
        away = jnp.dot(A[g, ds((1 - x) * two, two, two), :], right, preferred_element_type=F32)
        cs[k, j] = away.astype(BF16)
        c_send(k, j).start()
        mine[j] = jnp.dot(A[g, ds(x * two, two, two), :], right, preferred_element_type=F32)

    def project(j):
        @pl.when(is_end & (j < kept))
        def _():
            at_end(0, j)

        @pl.when(is_mid | (j < kept))
        def _():
            multiply(0, 0, 0, j, own)

        @pl.when(is_end & (j >= kept))
        def _():
            own[j] = jnp.zeros((two, bw), F32)

    guest_tokens(0)
    smooth_half(0, 0, 1)
    took_y(0, 1)

    def rest_outer(j):
        for side in range(2):
            own_at(1, j, side, is_mid & outer_side(side))

    span(halves, chunks, rest_outer)
    forward_end(0, 0, (0,))
    span(1, halves, guest_tokens)
    smooth_half(1, 0, 2)
    span(1, halves, lambda j: forward_end(0, j, (0,)))
    forward_end(0, 0, (1,))
    smooth_half(1, 1, 2)

    @pl.when(is_host)
    def _():
        took_x(2)
        took_y(2, 0)

    span(1, halves, lambda j: forward_end(0, j, (1,)))
    each(halves, lambda jj: t_local(jj).wait())
    all_tokens(0)

    def guest_back(j):
        @pl.when(is_host)
        def _():
            c_send(2, j).wait_recv()
            bs[j] = (own_g[j] + cr[2, j].astype(F32)).astype(BF16)
            back_send(j).start()

    def hidden(j):
        c_send(0, j).wait_recv()
        jj = j // 2
        target = j % 2

        def band(i, carry):
            at = pl.ds(pl.multiple_of(i * 16, 16), 16)
            for e in range(tiles):
                lane = slice(e * LANES, (e + 1) * LANES)
                smooth = y2d[pl.ds(i * 16 * sub + j * tiles + e, 16, stride=sub), :]
                gate = own[j, at, lane] + cr[0, j, at, lane].astype(F32)
                value = smooth * jax.nn.sigmoid(smooth) * jax.nn.sigmoid(gate)
                hid[j, at, lane] = value.astype(BF16)
            return carry

        for r in range(2):
            lax.fori_loop(r * rows // 16, (r + 1) * rows // 16, band, 0)

            @pl.when(target == x)
            def _():
                for dy in range(1, parts):
                    h_send(0, dy, jj, j, r).start()

            @pl.when(target != x)
            def _():
                h_send(1, 0, jj, j, r).start()

        @pl.when(target == x)
        def _():
            h_own(jj, j).start()
            h_ref(x, y, jj, c)[...] = hid[j]

    def hidden_x(jj):
        for r in range(2):
            h_got(1, 0, jj, r).wait_recv()
            for dy in range(1, parts):
                h_relay(dy, jj, r).start()
        h_pass(1, 0, jj).start()

    def hidden_y(dx, jj):
        for dy in range(1, parts):
            for r in range(2):
                h_got(dx, dy, jj, r).wait_recv()
            h_pass(dx, dy, jj).start()

    def early_project(j):
        forward_far(0, j)
        forward_end(0, halves + j)
        project(j)

    each(halves, early_project)
    own_at(1, 0, 1, inner_right)
    own_inner(1, 1)
    forward(1, 0, 1, (0,))
    span(halves, chunks, lambda j: forward(0, j, 1))

    @pl.when(is_host)
    def _():
        took_y(2, 1)
        all_tokens(2)

    @pl.when(is_end)
    def _():
        each(halves, hidden)

    def guest_sums(j):
        forward_far(0, j)

        @pl.when(is_host & (j >= kept))
        def _():
            multiply(0, 2, 2, j, own_g)

    def guest_step(j):
        guest_sums(j)
        forward_end(1, j - halves)

    span(halves, chunks, guest_step)
    forward(1, 0, 1, (1,))
    span(2, chunks, lambda j: own_inner(1, j))

    @pl.when(is_mid)
    def _():
        each(halves, hidden)

    def late_project(j):
        project(j)

        @pl.when(j >= kept)
        def _():
            guest_back(j)

    span(halves, chunks, late_project)
    span(1, halves, lambda j: forward(1, j, 1))
    forward_far(1, 0)
    span(0, halves // 2, hidden_x)
    hidden(halves)
    span(1, halves, lambda j: forward_far(1, j))
    span(halves + 1, chunks, hidden)
    span(halves, chunks, lambda j: forward_end(1, j))
    span(0, halves // 2, lambda jj: hidden_y(0, jj))
    span(0, halves // 2, lambda jj: hidden_y(1, jj))
    forward(1, halves, 1)
    span(halves // 2, halves, hidden_x)
    span(halves + 1, chunks, lambda j: forward(1, j, 1))
    span(halves // 2, halves, lambda jj: hidden_y(0, jj))
    span(halves // 2, halves, lambda jj: hidden_y(1, jj))

    def all_hidden(jj):
        for dx, dy in others:
            h_passed(dx, dy, jj).wait_recv()

    each(halves, all_hidden)

    def finish(j):
        c_send(1, j).wait_recv()
        mine = ds(c * rows, rows, rows)
        theirs = ds((1 - c) * rows, rows, rows)
        ost[j] = (own[j, theirs, :] + cr[1, j, theirs, :].astype(F32)).astype(BF16)
        o_send(j).start()
        omine[j] = (own[j, mine, :] + cr[1, j, mine, :].astype(F32)).astype(BF16)
        o_keep(j).start()

    def mix(j):
        @pl.when(halves + j < chunks)
        def _():
            forward_far(1, halves + j)

        @pl.when(is_end)
        def _():
            at_end(1, j)
        multiply(1, 1, 1, j, own)

    mix(0)

    def last(j):
        mix(j + 1)
        finish(j)

    each(chunks - 1, last)
    finish(chunks - 1)
    pltpu.make_async_copy(omine, omine, o_l).wait()
    remote(ost, ost, o_s, o_r, partner).wait_recv()

    def sent(ref, sem):
        remote(ref, ref, sem, o_r, partner).wait_send()

    for w in range(2):
        sent(W.at[w, :, ds(z * blk + c * bw, bw, bw)], sw_s.at[w])
        for k in range(lines):
            for side, first, count in ((0, k, lines - k), (1, 0, k + 1)):
                target = k + (1 if side else -1)
                if 0 <= target < lines:
                    n = kept if w == 0 and target in (0, lines - 1) else chunks

                    if k in (0, lines - 1):
                        first, count = k, 1

                    @pl.when(z == k)
                    def _():
                        sent(W.at[w, pl.ds(0, n), pl.ds(first * blk, count * blk)], z_s.at[side, w])
    sent(te_mine, te_s)
    sent(ost, o_s)
    sent(cs.at[1], c_s.at[1])

    @pl.when(is_mid)
    def _():
        sent(cs.at[0], c_s.at[0])

    @pl.when(is_end)
    def _():
        sent(cs.at[0, pl.ds(0, kept)], c_s.at[0])
        sent(G, g_s)

    @pl.when(is_host)
    def _():
        sent(cs.at[2, pl.ds(kept, chunks - kept)], c_s.at[2])
        sent(bs.at[pl.ds(kept, chunks - kept)], b_s)

    def settle_tokens(g):
        def go(jj):
            t_own(g, jj).wait_send()
            t_send(g, 1, 0, jj).wait_send()
            for dy in range(1, parts):
                t_send(g, 0, dy, jj).wait_send()
                t_relay(g, dy, jj).wait_send()
            for dx, dy in peers:
                t_pass(g, dx, dy, jj).wait_send()
        each(halves, go)

    settle_tokens(0)

    @pl.when(is_host)
    def _():
        settle_tokens(2)

    def settle_hidden(jj):
        h_own(jj, 0).wait_send()
        for r in range(2):
            h_send(1, 0, jj, 0, r).wait_send()
            for dy in range(1, parts):
                h_send(0, dy, jj, 0, r).wait_send()
                h_relay(dy, jj, r).wait_send()
        for dx, dy in peers:
            h_pass(dx, dy, jj).wait_send()

    each(halves, settle_hidden)

    e_send().wait_send()

    @pl.when(z < lines - 1)
    def _():
        chain_send().wait_send()


def per_device(shards, parts, tokens, decay_rate, angle, in_coef, out_coef, skip_coef, gate_weight, out_weight):
    rows, width = tokens.shape
    dims = decay_rate.shape[1]
    lines = shards // 4
    bw = gate_weight.shape[0]
    blk = 2 * bw
    chunks = width // blk
    assert shards % 4 == 0 and lines > 3 and dims % 2 == 0
    assert chunks % 2 == 0 and bw % LANES == 0 and chunks * 2 * parts == shards
    sub = chunks * bw // LANES
    two = 2 * rows
    depth = lines * blk
    skip = skip_coef.reshape(2 * sub, LANES)

    hbm = pl.BlockSpec(memory_space=pltpu.HBM)
    vmem = pl.BlockSpec(memory_space=pltpu.VMEM)
    dma = pltpu.SemaphoreType.DMA
    halves = chunks // 2
    n = 2 * parts
    flops = 2 * 2 * 4 * rows * depth * chunks * bw
    return pl.pallas_call(
        functools.partial(mixer_kernel, lines, parts, dims, chunks - max(1, chunks * GUESTS // 4)),
        in_specs=[hbm] * 7 + [vmem],
        out_specs=hbm,
        out_shape=jax.ShapeDtypeStruct((rows, width), BF16),
        scratch_shapes=[
            pltpu.VMEM((5, dims, chunks * bw), F32),
        ] + [pltpu.VMEM((dims * sub, LANES), F32)] * 6 + [
            pltpu.VMEM((sub, LANES), F32),
            pltpu.VMEM((two, chunks * bw), BF16),
            pltpu.VMEM((two * sub, LANES), F32),
            pltpu.VMEM((two * sub, LANES), F32),
            pltpu.VMEM((2, dims * sub, LANES), F32),
            pltpu.VMEM((2, dims * sub, LANES), BF16),
            pltpu.VMEM((2, dims * sub, LANES), BF16),
            pltpu.VMEM((2, dims * sub, LANES), BF16),
            pltpu.VMEM((2, dims * sub, LANES), BF16),
            pltpu.VMEM((3, 4 * rows, depth), BF16),
            pltpu.VMEM((2, chunks, depth, bw), BF16),
            pltpu.VMEM((chunks, two, bw), F32),
            pltpu.VMEM((chunks, two, bw), F32),
            pltpu.VMEM((3, chunks, two, bw), BF16),
            pltpu.VMEM((3, chunks, two, bw), BF16),
            pltpu.VMEM((chunks, two, bw), BF16),
            pltpu.VMEM((chunks, rows, bw), BF16),
            pltpu.VMEM((chunks, rows, bw), BF16),
            pltpu.VMEM((rows, width), BF16),
            pltpu.VMEM((chunks, two, bw), BF16),
            dma((2, chunks)),
            dma,
            dma((halves,)),
            dma,
            dma((2,)),
            dma((2, chunks)),
            dma,
            dma,
            dma((2, 2)),
            dma((2, chunks, lines)),
            dma((4, n, halves)),
            dma((4, n, halves)),
            dma((3, n, halves)),
            dma((3, n, halves)),
            dma,
            dma((chunks,)),
            dma,
            dma,
            dma,
            dma,
            dma,
            dma((3,)),
            dma((3, chunks)),
            dma,
            dma,
            dma,
        ],
        compiler_params=pltpu.CompilerParams(
            collective_id=0, has_side_effects=True, vmem_limit_bytes=56 * 1024 * 1024
        ),
        cost_estimate=pl.CostEstimate(flops=flops, bytes_accessed=4 * tokens.size, transcendentals=0),
        name="mixer",
    )(
        tokens, gate_weight, out_weight, decay_rate.T, angle.T, in_coef.T, out_coef.swapaxes(1, 2), skip,
    )


def solution(mesh):
    in_specs = (
        P("seq", "tp"),
        P("tp", None),
        P("tp", None),
        P("tp", None),
        P(None, "tp", None),
        P("tp"),
        P("seq", "tp"),
        P("seq", "tp"),
    )
    body = functools.partial(per_device, mesh.shape["seq"], mesh.shape["tp"])
    return jax.shard_map(body, mesh=mesh, in_specs=in_specs, out_specs=P("seq", "tp"), check_vma=False)
```

```python
import functools

import jax
import jax.numpy as jnp
from jax import lax
from jax.experimental import pallas as pl
from jax.experimental.pallas import tpu as pltpu
from jax.sharding import PartitionSpec as P

LANES = 128
UNROLL = 8
GUESTS = 2
MESH = pl.DeviceIdType.MESH
F32, BF16 = jnp.float32, jnp.bfloat16


def mixer_kernel(
    lines, parts, dims, kept,
    tok, gate_w, out_w, decay, angle, in_coef, out_coef, skip_in,
    out_ref,
    raw, q_re_ref, q_im_ref, c_re_ref, c_im_ref, s_re_ref, s_im_ref, skip_ref, te, x2d, y2d, st, ein, eout, cin, cout, A, W, own, own_g, cs, cr, hid, ost, G, bs,
    l_w, l_te, l_a, l_raw, sw_s, sw_r, te_s, te_r, z_s, z_r, x_s, x_r, p_s, p_r, g_s, g_r, b_s, e_s, e_r, ch_s, ch_r, c_s, c_r, o_s, o_r,
):
    rows, width = tok.shape
    bw = gate_w.shape[0]
    blk = 2 * bw
    chunks = width // blk
    halves = chunks // 2
    sub = chunks * bw // LANES
    tiles = bw // LANES
    two = 2 * rows

    s = lax.axis_index("seq")
    y = lax.axis_index("tp")
    z, x, c = s // 4, (s // 2) % 2, s % 2

    def dev(zz, xx, cc, yy):
        return ((zz * 2 + xx) * 2 + cc, yy)

    partner = dev(z, x, 1 - c, y)
    is_mid = (z > 0) & (z < lines - 1)
    is_end = jnp.logical_not(is_mid)
    is_host = (z == 1) | (z == lines - 2)
    end_z = jnp.where(z == 1, 0, lines - 1)
    host_z = jnp.where(z == 0, 1, lines - 2)

    def hint(v, m):
        return v if isinstance(v, int) else pl.multiple_of(v, m)

    def ds(start, size, m):
        return pl.ds(hint(start, m), size)

    def remote(src, dst, ssem, rsem, where):
        return pltpu.make_async_remote_copy(src, dst, ssem, rsem, device_id=where, device_id_type=MESH)

    weights = (gate_w, out_w)
    others = [(xx, yy) for yy in range(parts) for xx in range(2)]
    peers = others[1:]

    def w_local(w, j):
        return pltpu.make_async_copy(
            weights[w].at[:, ds(j * blk + c * bw, bw, bw)],
            W.at[w, j, ds(z * blk + c * bw, bw, bw)], l_w.at[w, j])

    def w_swap(w, j):
        return remote(
            weights[w].at[:, ds(j * blk + (1 - c) * bw, bw, bw)],
            W.at[w, j, ds(z * blk + c * bw, bw, bw)], sw_s.at[w], sw_r.at[w, j], partner)

    def te_local(j):
        return pltpu.make_async_copy(
            tok.at[:, ds(j * blk + c * bw, bw, bw)], te.at[ds(c * rows, rows, rows), ds(j * bw, bw, bw)], l_te)

    def raw_local(t, j):
        source = (decay, angle, in_coef, out_coef.at[0], out_coef.at[1])[t]
        return pltpu.make_async_copy(
            source.at[:, ds(j * blk + c * bw, bw, bw)], raw.at[t, :, ds(j * bw, bw, bw)], l_raw)

    def te_swap(j):
        return remote(
            tok.at[:, ds(j * blk + (1 - c) * bw, bw, bw)],
            te.at[ds(c * rows, rows, rows), ds(j * bw, bw, bw)], te_s, te_r, partner)

    def piece(w, j, o):
        return W.at[w, j, ds(o * blk, blk, blk)]

    def z_send(w, j, o, side):
        where = dev(z + (1 if side else -1), x, c, y)
        return remote(piece(w, j, o), piece(w, j, o), z_s.at[side, w], z_r.at[w, j, o], where)

    def at_peer(dx, dy):
        return (x + dx) % 2, (y + dy) % parts

    def a_cols(yy, jj):
        return ds((yy * halves + jj) * blk, blk, blk)

    def slot(dx, yy):
        return dx * parts + yy

    def t_from(g, block):
        return (G if g else tok).at[:, ds(block * blk, blk, blk)]

    def t_ref(g, xx, cc, yy, jj):
        return A.at[g, ds((xx * 2 + cc) * rows, rows, rows), a_cols(yy, jj)]

    def t_send(g, dx, dy, jj):
        xx, yy = at_peer(dx, dy)
        return remote(
            t_from(g, 2 * jj + xx), t_ref(g, x, c, y, jj),
            x_s.at[g, dx * parts + dy, jj], x_r.at[g, slot(dx, y), jj], dev(z, xx, c, yy))

    def t_relay(g, dy, jj):
        xx, yy = at_peer(1, dy)
        ref = t_ref(g, xx, c, y, jj)
        return remote(ref, ref, x_s.at[g, parts + dy, jj], x_r.at[g, slot(1, y), jj], dev(z, x, c, yy))

    def t_got(g, dx, dy, jj):
        xx, yy = at_peer(dx, dy)
        ref = t_ref(g, xx, c, yy, jj)
        return remote(ref, ref, x_s.at[g, dx * parts + dy, jj], x_r.at[g, slot(dx, yy), jj], partner)

    def t_local(jj):
        return pltpu.make_async_copy(t_from(0, 2 * jj + x), t_ref(0, x, c, y, jj), l_a.at[jj])

    def t_own(g, jj):
        return remote(
            t_from(g, 2 * jj + x), t_ref(g, x, c, y, jj), p_s.at[g, 0, jj], p_r.at[g, slot(0, y), jj], partner)

    def t_pass(g, dx, dy, jj):
        xx, yy = at_peer(dx, dy)
        ref = t_ref(g, xx, c, yy, jj)
        return remote(ref, ref, p_s.at[g, dx * parts + dy, jj], p_r.at[g, slot(dx, yy), jj], partner)

    def t_passed(g, dx, dy, jj):
        xx, yy = at_peer(dx, dy)
        ref = t_ref(g, xx, 1 - c, yy, jj)
        return remote(ref, ref, p_s.at[g, dx * parts + dy, jj], p_r.at[g, slot(dx, yy), jj], partner)

    def g_send(k):
        ref = G.at[:, ds(k * blk, blk, blk)]
        return remote(t_from(0, k), ref, g_s, g_r.at[k], dev(host_z, x, c, y))

    def back_send(j):
        return remote(bs.at[j], cr.at[0, j], b_s, c_r.at[0, j], dev(end_z, x, c, y))

    def h_ref(xx, yy, jj, cc):
        cols = ds((yy * halves + jj) * blk + cc * bw, bw, bw)
        return A.at[1, ds(xx * two, two, two), cols]

    def h_band(xx, yy, jj, r):
        cols = ds((yy * halves + jj) * blk + c * bw, bw, bw)
        return A.at[1, ds(xx * two + r * rows, rows, rows), cols]

    def h_send(dx, dy, jj, j, r):
        xx, yy = at_peer(dx, dy)
        return remote(
            hid.at[j, ds(r * rows, rows, rows)], h_band(x, y, jj, r),
            x_s.at[1 + 2 * r, dx * parts + dy, jj], x_r.at[1 + 2 * r, slot(dx, y), jj], dev(z, xx, c, yy))

    def h_got(dx, dy, jj, r):
        xx, yy = at_peer(dx, dy)
        ref = h_band(xx, yy, jj, r)
        return remote(
            ref, ref, x_s.at[1 + 2 * r, dx * parts + dy, jj], x_r.at[1 + 2 * r, slot(dx, yy), jj], dev(z, xx, c, yy))

    def h_relay(dy, jj, r):
        xx, yy = at_peer(1, dy)
        ref = h_band(xx, y, jj, r)
        return remote(
            ref, ref, x_s.at[1 + 2 * r, parts + dy, jj], x_r.at[1 + 2 * r, slot(1, y), jj], dev(z, x, c, yy))

    def h_own(jj, j):
        return remote(hid.at[j], h_ref(x, y, jj, c), p_s.at[1, 0, jj], p_r.at[1, slot(0, y), jj], partner)

    def h_pass(dx, dy, jj):
        xx, yy = at_peer(dx, dy)
        ref = h_ref(xx, yy, jj, c)
        return remote(ref, ref, p_s.at[1, dx * parts + dy, jj], p_r.at[1, slot(dx, yy), jj], partner)

    def h_passed(dx, dy, jj):
        xx, yy = at_peer(dx, dy)
        ref = h_ref(xx, yy, jj, 1 - c)
        return remote(ref, ref, p_s.at[1, dx * parts + dy, jj], p_r.at[1, slot(dx, yy), jj], partner)

    def c_send(w, j):
        return remote(cs.at[w, j], cr.at[w, j], c_s.at[w], c_r.at[w, j], dev(z, 1 - x, c, y))

    def e_send():
        return remote(eout, ein, e_s, e_r, dev(z, 1 - x, c, y))

    def chain_send():
        return remote(cout, cin, ch_s, ch_r, dev(z + 1, x, c, y))

    def o_send(j):
        return remote(ost.at[j], out_ref.at[:, ds(j * blk + c * bw, bw, bw)], o_s, o_r, partner)

    def each(n, f):
        def body(i, carry):
            f(i)
            return carry
        lax.fori_loop(0, n, body, 0)

    each(chunks, lambda j: w_local(0, j).start())
    each(chunks, lambda j: te_local(j).start())
    for t in range(5):
        each(chunks, lambda j: raw_local(t, j).start())
    each(halves, lambda jj: t_local(jj).start())
    each(chunks, lambda j: w_local(1, j).start())

    barrier = pltpu.get_barrier_semaphore()

    def greet(where):
        pl.semaphore_signal(barrier, inc=1, device_id=where, device_id_type=MESH)

    greet(partner)
    for dx, dy in peers:
        xx, yy = at_peer(dx, dy)
        greet(dev(z, xx, c, yy))
    line_peers = [
        (z > 0, dev(z - 1, x, c, y)),
        (z < lines - 1, dev(z + 1, x, c, y)),
    ]
    for there, where in line_peers:
        @pl.when(there)
        def _():
            greet(where)
    pl.semaphore_wait(barrier, 1 + len(peers) + sum(there.astype(jnp.int32) for there, _ in line_peers))

    each(chunks, lambda j: w_swap(0, j).start())

    @pl.when(z == 0)
    def _():
        each(chunks - 1, lambda k: g_send(k).start())

    @pl.when(z == lines - 1)
    def _():
        each(chunks, lambda k: g_send(k).start())

    def t_start(g, jj):
        t_send(g, 1, 0, jj).start()
        for dy in range(1, parts):
            t_send(g, 0, dy, jj).start()
        t_own(g, jj).start()

    each(halves, lambda jj: t_start(0, jj))
    each(chunks, lambda j: te_swap(j).start())
    each(chunks, lambda j: w_swap(1, j).start())

    def own_ready(w, j):
        w_local(w, j).wait()
        w_swap(w, j).wait_recv()

    def wanted(w, j, side):
        target = z + (1 if side else -1)
        inside = (target >= 0) & (target < lines)
        if w == 0:
            inside = inside & (((target > 0) & (target < lines - 1)) | (j < kept))
        return inside

    def outer_side(side):
        target = z + (1 if side else -1)
        return is_end | (target == 0) | (target == lines - 1)

    def own_at(w, j, side, there):
        @pl.when(wanted(w, j, side) & there)
        def _():
            z_send(w, j, z, side).start()

    def own_inner(w, j):
        for side in range(2):
            @pl.when(wanted(w, j, side) & jnp.logical_not(outer_side(side)))
            def _():
                z_send(w, j, z, side).start()

    def hop(w, j, o, side, there):
        @pl.when(there)
        def _():
            z_send(w, j, o, side).wait_recv()

            @pl.when(wanted(w, j, side))
            def _():
                z_send(w, j, o, side).start()

    def relay_cases(d, from_end):
        low, high = z - d, z + d
        if d == 1:
            at_low = (low == 0) if from_end else (low > 0)
            at_high = (high == lines - 1) if from_end else (high < lines - 1)
        else:
            at_low, at_high = low >= 0, high < lines
        return (low, 1, is_mid & at_low), (high, 0, is_mid & at_high)

    def forward_end(w, j, sides=(0, 1)):
        for o, side, there in relay_cases(1, True):
            if side in sides:
                hop(w, j, o, side, there)

    def forward(w, j, d, sides=(0, 1)):
        for o, side, there in relay_cases(d, False):
            if side in sides:
                hop(w, j, o, side, there)

    def forward_far(w, j):
        for d in range(2, lines - 1):
            forward(w, j, d)

    def at_end(w, j):
        for d in range(1, lines):
            @pl.when(z == 0)
            def _():
                z_send(w, j, d, 0).wait_recv()

            @pl.when(z == lines - 1)
            def _():
                z_send(w, j, lines - 1 - d, 0).wait_recv()

    def span(start, stop, f):
        def body(j, carry):
            f(j)
            return carry
        lax.fori_loop(start, stop, body, 0)

    def first_sends(j):
        own_ready(0, j)
        own_at(0, j, 0, z >= 0)
        own_at(0, j, 1, is_mid & (outer_side(1) | (j < halves)))

    each(chunks, first_sends)

    pltpu.make_async_copy(raw, raw, l_raw).wait()
    for e in range(sub):
        band = slice(e * LANES, (e + 1) * LANES)
        rate, theta, scale, o_re, o_im = (raw[t, :, band] for t in range(5))
        magnitude = 1.0 - rate
        scale = scale * jnp.sqrt(1.0 - magnitude * magnitude)
        at = pl.ds(e, dims, stride=sub)
        c_re_ref[at, :] = scale * o_re
        c_im_ref[at, :] = scale * o_im
        q_re_ref[at, :] = magnitude * jnp.cos(theta)
        q_im_ref[at, :] = magnitude * jnp.sin(theta)
        k, lane = e // tiles, e % tiles
        row = 2 * k * tiles + lane
        skip_ref[e:e + 1, :] = jnp.where(c == 0, skip_in[row:row + 1, :], skip_in[row + tiles:row + tiles + 1, :])

    def span_of():
        base = q_re_ref[...], q_im_ref[...]
        total = None
        count = two
        while count:
            if count % 2:
                total = base if total is None else (
                    total[0] * base[0] - total[1] * base[1], total[0] * base[1] + total[1] * base[0])
            base = base[0] * base[0] - base[1] * base[1], 2.0 * base[0] * base[1]
            count //= 2
        s_re_ref[...] = total[0]
        s_im_ref[...] = total[1]

    span_of()

    te_mine = te.at[ds(c * rows, rows, rows), :]
    te_theirs = te.at[ds((1 - c) * rows, rows, rows), :]
    pltpu.make_async_copy(te_mine, te_mine, l_te).wait()
    remote(te_theirs, te_theirs, te_s, te_r, partner).wait_recv()

    def lay(i, carry):
        for e in range(sub):
            v = te[pl.ds(i * 16, 16), e * LANES:(e + 1) * LANES].astype(F32)
            x2d[pl.ds(i * 16 * sub + e, 16, stride=sub), :] = v
        return carry

    lax.fori_loop(0, two // 16, lay, 0)

    def second_own(j):
        own_ready(1, j)
        for side in range(2):
            own_at(1, j, side, is_mid & outer_side(side) & (j < halves))
        own_at(1, j, 0, z == lines - 1)

    each(chunks, second_own)

    half = dims // 2

    def tile(ref, h):
        return ref[h * sub:(h + 1) * sub, :]

    def step(state, v, q_re, q_im):
        return [(a * re - b * im + v, a * im + b * re) for (re, im), a, b in zip(state, q_re, q_im)]

    def end_half(k):
        hs = range(k * half, (k + 1) * half)
        q_re = [tile(q_re_ref, h) for h in hs]
        q_im = [tile(q_im_ref, h) for h in hs]
        zero = jnp.zeros((sub, LANES), F32)

        def body(i, state):
            for u in range(UNROLL):
                state = step(state, x2d[ds((i * UNROLL + u) * sub, sub, sub), :], q_re, q_im)
            return state

        state = lax.fori_loop(0, two // UNROLL, body, [(zero, zero)] * half)
        for h, (re, im) in zip(hs, state):
            st[0, h * sub:(h + 1) * sub, :] = re
            st[1, h * sub:(h + 1) * sub, :] = im

    def took_x(g):
        def go(jj):
            t_got(g, 1, 0, jj).wait_recv()
            for dy in range(1, parts):
                t_relay(g, dy, jj).start()
            t_pass(g, 1, 0, jj).start()
        each(halves, go)

    def took_y(g, dx):
        def go(jj):
            for dy in range(1, parts):
                t_got(g, dx, dy, jj).wait_recv()
                t_pass(g, dx, dy, jj).start()
        each(halves, go)

    end_half(0)
    end_half(1)
    eout[...] = st[...].astype(BF16)
    e_send().start()
    took_x(0)
    inner_left = jnp.logical_not(outer_side(0))
    own_at(1, 0, 0, inner_left)

    def cmul(a, b):
        return a[0] * b[0] - a[1] * b[1], a[0] * b[1] + a[1] * b[0]

    span_q = s_re_ref[...], s_im_ref[...]
    e_send().wait_recv()
    mine = st[0], st[1]
    other = ein[0].astype(F32), ein[1].astype(F32)
    first = [jnp.where(x == 0, m, o) for m, o in zip(mine, other)]
    second = [jnp.where(x == 0, o, m) for m, o in zip(mine, other)]
    plane = [a + b for a, b in zip(cmul(span_q, first), second)]

    @pl.when(z == 0)
    def _():
        cin[...] = jnp.zeros_like(cin)

    @pl.when(z > 0)
    def _():
        chain_send().wait_recv()

    carry = cin[0].astype(F32), cin[1].astype(F32)
    moved = cmul(span_q, carry)
    onward = [a + b for a, b in zip(cmul(span_q, moved), plane)]
    cout[0] = onward[0].astype(BF16)
    cout[1] = onward[1].astype(BF16)

    @pl.when(z < lines - 1)
    def _():
        chain_send().start()

    for k in range(2):
        st[k] = jnp.where(x == 0, carry[k], moved[k] + first[k])

    inner_right = is_mid & jnp.logical_not(outer_side(1))

    @pl.when(z == 0)
    def _():
        g_send(chunks - 1).start()

    each(chunks, lambda j: own_at(0, j, 1, (z == 0) | (inner_right & (j >= halves))))
    each(chunks, lambda j: own_at(1, j, 1, z == 0))
    each(halves, lambda j: forward(0, j, 1))
    took_y(0, 0)

    def guest_tokens(jj):
        @pl.when(is_host)
        def _():
            g_send(2 * jj).wait_recv()
            g_send(2 * jj + 1).wait_recv()
            t_start(2, jj)
            t_ref(2, x, c, y, jj)[...] = t_from(2, 2 * jj + x)[...]

    def smooth_half(k, part, parts_of):
        hs = range(k * half, (k + 1) * half)
        q_re = [tile(q_re_ref, h) for h in hs]
        q_im = [tile(q_im_ref, h) for h in hs]
        c_re = [tile(c_re_ref, h) for h in hs]
        c_im = [tile(c_im_ref, h) for h in hs]
        skip = skip_ref[...]
        state = [(tile(st.at[0], h), tile(st.at[1], h)) for h in hs]

        def body(i, state):
            for u in range(UNROLL):
                at = ds((i * UNROLL + u) * sub, sub, sub)
                v = x2d[at, :]
                state = step(state, v, q_re, q_im)
                sums = [c_re[h] * state[h][0] - c_im[h] * state[h][1] for h in range(half)]
                while len(sums) > 1:
                    sums = [sum(sums[m:m + 2]) for m in range(0, len(sums), 2)]
                before = v * skip if k == 0 else y2d[at, :]
                y2d[at, :] = before + sums[0]
            return state

        steps = two // UNROLL // parts_of
        state = lax.fori_loop(part * steps, (part + 1) * steps, body, state)
        if part + 1 < parts_of:
            for h, (re, im) in zip(hs, state):
                st[0, h * sub:(h + 1) * sub, :] = re
                st[1, h * sub:(h + 1) * sub, :] = im

    def all_tokens(g):
        def go(jj):
            for dx, dy in others:
                t_passed(g, dx, dy, jj).wait_recv()
        each(halves, go)

    def multiply(w, g, k, j, mine):
        right = W[w, j]
        away = jnp.dot(A[g, ds((1 - x) * two, two, two), :], right, preferred_element_type=F32)
        cs[k, j] = away.astype(BF16)
        c_send(k, j).start()
        mine[j] = jnp.dot(A[g, ds(x * two, two, two), :], right, preferred_element_type=F32)

    def project(j):
        @pl.when(is_end & (j < kept))
        def _():
            at_end(0, j)

        @pl.when(is_mid | (j < kept))
        def _():
            multiply(0, 0, 0, j, own)

        @pl.when(is_end & (j >= kept))
        def _():
            own[j] = jnp.zeros((two, bw), F32)

    guest_tokens(0)
    smooth_half(0, 0, 1)
    took_y(0, 1)

    def rest_outer(j):
        for side in range(2):
            own_at(1, j, side, is_mid & outer_side(side))

    span(halves, chunks, rest_outer)
    forward_end(0, 0, (0,))
    span(1, halves, guest_tokens)
    smooth_half(1, 0, 2)
    span(1, halves, lambda j: forward_end(0, j, (0,)))
    forward_end(0, 0, (1,))
    smooth_half(1, 1, 2)

    @pl.when(is_host)
    def _():
        took_x(2)
        took_y(2, 0)

    span(1, halves, lambda j: forward_end(0, j, (1,)))
    each(halves, lambda jj: t_local(jj).wait())
    all_tokens(0)

    def guest_back(j):
        @pl.when(is_host)
        def _():
            c_send(2, j).wait_recv()
            bs[j] = (own_g[j] + cr[2, j].astype(F32)).astype(BF16)
            back_send(j).start()

    def hidden(j):
        c_send(0, j).wait_recv()
        jj = j // 2
        target = j % 2

        def band(i, carry):
            at = pl.ds(pl.multiple_of(i * 16, 16), 16)
            for e in range(tiles):
                lane = slice(e * LANES, (e + 1) * LANES)
                smooth = y2d[pl.ds(i * 16 * sub + j * tiles + e, 16, stride=sub), :]
                gate = own[j, at, lane] + cr[0, j, at, lane].astype(F32)
                value = smooth * jax.nn.sigmoid(smooth) * jax.nn.sigmoid(gate)
                hid[j, at, lane] = value.astype(BF16)
            return carry

        for r in range(2):
            lax.fori_loop(r * rows // 16, (r + 1) * rows // 16, band, 0)

            @pl.when(target == x)
            def _():
                for dy in range(1, parts):
                    h_send(0, dy, jj, j, r).start()

            @pl.when(target != x)
            def _():
                h_send(1, 0, jj, j, r).start()

        @pl.when(target == x)
        def _():
            h_own(jj, j).start()
            h_ref(x, y, jj, c)[...] = hid[j]

    def hidden_x(jj):
        for r in range(2):
            h_got(1, 0, jj, r).wait_recv()
            for dy in range(1, parts):
                h_relay(dy, jj, r).start()
        h_pass(1, 0, jj).start()

    def hidden_y(dx, jj):
        for dy in range(1, parts):
            for r in range(2):
                h_got(dx, dy, jj, r).wait_recv()
            h_pass(dx, dy, jj).start()

    def early_project(j):
        forward_far(0, j)
        forward_end(0, halves + j)
        project(j)

    each(halves, early_project)
    own_at(1, 0, 1, inner_right)
    own_inner(1, 1)
    forward(1, 0, 1, (0,))
    span(halves, chunks, lambda j: forward(0, j, 1))

    @pl.when(is_host)
    def _():
        took_y(2, 1)
        all_tokens(2)

    @pl.when(is_end)
    def _():
        each(halves, hidden)

    def guest_sums(j):
        forward_far(0, j)

        @pl.when(is_host & (j >= kept))
        def _():
            multiply(0, 2, 2, j, own_g)

    def guest_step(j):
        guest_sums(j)
        forward_end(1, j - halves)

    span(halves, chunks, guest_step)
    forward(1, 0, 1, (1,))
    span(2, chunks, lambda j: own_inner(1, j))

    @pl.when(is_mid)
    def _():
        each(halves, hidden)

    def late_project(j):
        project(j)

        @pl.when(j >= kept)
        def _():
            guest_back(j)

    span(halves, chunks, late_project)
    span(1, halves, lambda j: forward(1, j, 1))
    forward_far(1, 0)
    span(0, halves // 2, hidden_x)
    hidden(halves)
    span(1, halves, lambda j: forward_far(1, j))
    span(halves + 1, chunks, hidden)
    span(halves, chunks, lambda j: forward_end(1, j))
    span(0, halves // 2, lambda jj: hidden_y(0, jj))
    span(0, halves // 2, lambda jj: hidden_y(1, jj))
    forward(1, halves, 1)
    span(halves // 2, halves, hidden_x)
    span(halves + 1, chunks, lambda j: forward(1, j, 1))
    span(halves // 2, halves, lambda jj: hidden_y(0, jj))
    span(halves // 2, halves, lambda jj: hidden_y(1, jj))

    def all_hidden(jj):
        for dx, dy in others:
            h_passed(dx, dy, jj).wait_recv()

    each(halves, all_hidden)

    def finish(j):
        c_send(1, j).wait_recv()
        mine = ds(c * rows, rows, rows)
        theirs = ds((1 - c) * rows, rows, rows)
        ost[j] = (own[j, theirs, :] + cr[1, j, theirs, :].astype(F32)).astype(BF16)
        o_send(j).start()
        out_ref[:, ds(j * blk + c * bw, bw, bw)] = (own[j, mine, :] + cr[1, j, mine, :].astype(F32)).astype(BF16)

    def mix(j):
        @pl.when(halves + j < chunks)
        def _():
            forward_far(1, halves + j)

        @pl.when(is_end)
        def _():
            at_end(1, j)
        multiply(1, 1, 1, j, own)

    mix(0)

    def last(j):
        mix(j + 1)
        finish(j)

    each(chunks - 1, last)
    finish(chunks - 1)
    remote(ost, ost, o_s, o_r, partner).wait_recv()

    def sent(ref, sem):
        remote(ref, ref, sem, o_r, partner).wait_send()

    for w in range(2):
        sent(W.at[w, :, ds(z * blk + c * bw, bw, bw)], sw_s.at[w])
        for k in range(lines):
            for side, first, count in ((0, k, lines - k), (1, 0, k + 1)):
                target = k + (1 if side else -1)
                if 0 <= target < lines:
                    n = kept if w == 0 and target in (0, lines - 1) else chunks

                    if k in (0, lines - 1):
                        first, count = k, 1

                    @pl.when(z == k)
                    def _():
                        sent(W.at[w, pl.ds(0, n), pl.ds(first * blk, count * blk)], z_s.at[side, w])
    sent(te_mine, te_s)
    sent(ost, o_s)
    sent(cs.at[1], c_s.at[1])

    @pl.when(is_mid)
    def _():
        sent(cs.at[0], c_s.at[0])

    @pl.when(is_end)
    def _():
        sent(cs.at[0, pl.ds(0, kept)], c_s.at[0])
        sent(G, g_s)

    @pl.when(is_host)
    def _():
        sent(cs.at[2, pl.ds(kept, chunks - kept)], c_s.at[2])
        sent(bs.at[pl.ds(kept, chunks - kept)], b_s)

    def settle_tokens(g):
        def go(jj):
            t_own(g, jj).wait_send()
            t_send(g, 1, 0, jj).wait_send()
            for dy in range(1, parts):
                t_send(g, 0, dy, jj).wait_send()
                t_relay(g, dy, jj).wait_send()
            for dx, dy in peers:
                t_pass(g, dx, dy, jj).wait_send()
        each(halves, go)

    settle_tokens(0)

    @pl.when(is_host)
    def _():
        settle_tokens(2)

    def settle_hidden(jj):
        h_own(jj, 0).wait_send()
        for r in range(2):
            h_send(1, 0, jj, 0, r).wait_send()
            for dy in range(1, parts):
                h_send(0, dy, jj, 0, r).wait_send()
                h_relay(dy, jj, r).wait_send()
        for dx, dy in peers:
            h_pass(dx, dy, jj).wait_send()

    each(halves, settle_hidden)

    e_send().wait_send()

    @pl.when(z < lines - 1)
    def _():
        chain_send().wait_send()


def per_device(shards, parts, tokens, decay_rate, angle, in_coef, out_coef, skip_coef, gate_weight, out_weight):
    rows, width = tokens.shape
    dims = decay_rate.shape[1]
    lines = shards // 4
    bw = gate_weight.shape[0]
    blk = 2 * bw
    chunks = width // blk
    assert shards % 4 == 0 and lines > 3 and dims % 2 == 0
    assert chunks % 2 == 0 and bw % LANES == 0 and chunks * 2 * parts == shards
    sub = chunks * bw // LANES
    two = 2 * rows
    depth = lines * blk
    skip = skip_coef.reshape(2 * sub, LANES)

    hbm = pl.BlockSpec(memory_space=pltpu.HBM)
    vmem = pl.BlockSpec(memory_space=pltpu.VMEM)
    dma = pltpu.SemaphoreType.DMA
    halves = chunks // 2
    n = 2 * parts
    flops = 2 * 2 * 4 * rows * depth * chunks * bw
    return pl.pallas_call(
        functools.partial(mixer_kernel, lines, parts, dims, chunks - max(1, chunks * GUESTS // 4)),
        in_specs=[hbm] * 7 + [vmem],
        out_specs=vmem,
        out_shape=pltpu.VMEM((rows, width), BF16),
        scratch_shapes=[
            pltpu.VMEM((5, dims, chunks * bw), F32),
        ] + [pltpu.VMEM((dims * sub, LANES), F32)] * 6 + [
            pltpu.VMEM((sub, LANES), F32),
            pltpu.VMEM((two, chunks * bw), BF16),
            pltpu.VMEM((two * sub, LANES), F32),
            pltpu.VMEM((two * sub, LANES), F32),
            pltpu.VMEM((2, dims * sub, LANES), F32),
            pltpu.VMEM((2, dims * sub, LANES), BF16),
            pltpu.VMEM((2, dims * sub, LANES), BF16),
            pltpu.VMEM((2, dims * sub, LANES), BF16),
            pltpu.VMEM((2, dims * sub, LANES), BF16),
            pltpu.VMEM((3, 4 * rows, depth), BF16),
            pltpu.VMEM((2, chunks, depth, bw), BF16),
            pltpu.VMEM((chunks, two, bw), F32),
            pltpu.VMEM((chunks, two, bw), F32),
            pltpu.VMEM((3, chunks, two, bw), BF16),
            pltpu.VMEM((3, chunks, two, bw), BF16),
            pltpu.VMEM((chunks, two, bw), BF16),
            pltpu.VMEM((chunks, rows, bw), BF16),
            pltpu.VMEM((rows, width), BF16),
            pltpu.VMEM((chunks, two, bw), BF16),
            dma((2, chunks)),
            dma,
            dma((halves,)),
            dma,
            dma((2,)),
            dma((2, chunks)),
            dma,
            dma,
            dma((2, 2)),
            dma((2, chunks, lines)),
            dma((4, n, halves)),
            dma((4, n, halves)),
            dma((3, n, halves)),
            dma((3, n, halves)),
            dma,
            dma((chunks,)),
            dma,
            dma,
            dma,
            dma,
            dma,
            dma((3,)),
            dma((3, chunks)),
            dma,
            dma,
        ],
        compiler_params=pltpu.CompilerParams(
            collective_id=0, has_side_effects=True, vmem_limit_bytes=56 * 1024 * 1024
        ),
        cost_estimate=pl.CostEstimate(flops=flops, bytes_accessed=4 * tokens.size, transcendentals=0),
        name="mixer",
    )(
        tokens, gate_weight, out_weight, decay_rate.T, angle.T, in_coef.T, out_coef.swapaxes(1, 2), skip,
    )


def solution(mesh):
    in_specs = (
        P("seq", "tp"),
        P("tp", None),
        P("tp", None),
        P("tp", None),
        P(None, "tp", None),
        P("tp"),
        P("seq", "tp"),
        P("seq", "tp"),
    )
    body = functools.partial(per_device, mesh.shape["seq"], mesh.shape["tp"])
    return jax.shard_map(body, mesh=mesh, in_specs=in_specs, out_specs=P("seq", "tp"), check_vma=False)
```

```python
import functools

import jax
import jax.numpy as jnp
from jax import lax
from jax.experimental import pallas as pl
from jax.experimental.pallas import tpu as pltpu
from jax.sharding import PartitionSpec as P

LANES = 128
UNROLL = 8
GUESTS = 2
MESH = pl.DeviceIdType.MESH
F32, BF16 = jnp.float32, jnp.bfloat16


def mixer_kernel(
    lines, parts, dims, kept,
    tok, gate_w, out_w, decay, angle, in_coef, out_coef, skip_in,
    out_ref,
    raw, q_re_ref, q_im_ref, c_re_ref, c_im_ref, s_re_ref, s_im_ref, skip_ref, te, x2d, y2d, st, ein, eout, cin, cout, A, W, own, own_g, cs, cr, hid, ost, G, bs,
    l_w, l_te, l_a, l_raw, sw_s, sw_r, te_s, te_r, z_s, z_r, x_s, x_r, p_s, p_r, g_s, g_r, b_s, e_s, e_r, ch_s, ch_r, c_s, c_r, o_s, o_r,
):
    rows, width = tok.shape
    bw = gate_w.shape[0]
    blk = 2 * bw
    chunks = width // blk
    halves = chunks // 2
    sub = chunks * bw // LANES
    tiles = bw // LANES
    two = 2 * rows

    s = lax.axis_index("seq")
    y = lax.axis_index("tp")
    z, x, c = s // 4, (s // 2) % 2, s % 2

    def dev(zz, xx, cc, yy):
        return ((zz * 2 + xx) * 2 + cc, yy)

    partner = dev(z, x, 1 - c, y)
    is_mid = (z > 0) & (z < lines - 1)
    is_end = jnp.logical_not(is_mid)
    is_host = (z == 1) | (z == lines - 2)
    end_z = jnp.where(z == 1, 0, lines - 1)
    host_z = jnp.where(z == 0, 1, lines - 2)

    def hint(v, m):
        return v if isinstance(v, int) else pl.multiple_of(v, m)

    def ds(start, size, m):
        return pl.ds(hint(start, m), size)

    def remote(src, dst, ssem, rsem, where):
        return pltpu.make_async_remote_copy(src, dst, ssem, rsem, device_id=where, device_id_type=MESH)

    weights = (gate_w, out_w)
    others = [(xx, yy) for yy in range(parts) for xx in range(2)]
    peers = others[1:]

    def w_local(w, j):
        return pltpu.make_async_copy(
            weights[w].at[:, ds(j * blk + c * bw, bw, bw)],
            W.at[w, j, ds(z * blk + c * bw, bw, bw)], l_w.at[w, j])

    def w_swap(w, j):
        return remote(
            weights[w].at[:, ds(j * blk + (1 - c) * bw, bw, bw)],
            W.at[w, j, ds(z * blk + c * bw, bw, bw)], sw_s.at[w], sw_r.at[w, j], partner)

    def te_local(j):
        return pltpu.make_async_copy(
            tok.at[:, ds(j * blk + c * bw, bw, bw)], te.at[ds(c * rows, rows, rows), ds(j * bw, bw, bw)], l_te)

    def raw_local(t, j):
        source = (decay, angle, in_coef, out_coef.at[0], out_coef.at[1])[t]
        return pltpu.make_async_copy(
            source.at[:, ds(j * blk + c * bw, bw, bw)], raw.at[t, :, ds(j * bw, bw, bw)], l_raw)

    def te_swap(j):
        return remote(
            tok.at[:, ds(j * blk + (1 - c) * bw, bw, bw)],
            te.at[ds(c * rows, rows, rows), ds(j * bw, bw, bw)], te_s, te_r, partner)

    def piece(w, j, o):
        return W.at[w, j, ds(o * blk, blk, blk)]

    def z_send(w, j, o, side):
        where = dev(z + (1 if side else -1), x, c, y)
        return remote(piece(w, j, o), piece(w, j, o), z_s.at[side, w], z_r.at[w, j, o], where)

    def at_peer(dx, dy):
        return (x + dx) % 2, (y + dy) % parts

    def a_cols(yy, jj):
        return ds((yy * halves + jj) * blk, blk, blk)

    def slot(dx, yy):
        return dx * parts + yy

    def t_from(g, block):
        return (G if g else tok).at[:, ds(block * blk, blk, blk)]

    def t_ref(g, xx, cc, yy, jj):
        return A.at[g, ds((xx * 2 + cc) * rows, rows, rows), a_cols(yy, jj)]

    def t_send(g, dx, dy, jj):
        xx, yy = at_peer(dx, dy)
        return remote(
            t_from(g, 2 * jj + xx), t_ref(g, x, c, y, jj),
            x_s.at[g, dx * parts + dy, jj], x_r.at[g, slot(dx, y), jj], dev(z, xx, c, yy))

    def t_relay(g, dy, jj):
        xx, yy = at_peer(1, dy)
        ref = t_ref(g, xx, c, y, jj)
        return remote(ref, ref, x_s.at[g, parts + dy, jj], x_r.at[g, slot(1, y), jj], dev(z, x, c, yy))

    def t_got(g, dx, dy, jj):
        xx, yy = at_peer(dx, dy)
        ref = t_ref(g, xx, c, yy, jj)
        return remote(ref, ref, x_s.at[g, dx * parts + dy, jj], x_r.at[g, slot(dx, yy), jj], partner)

    def t_local(jj):
        return pltpu.make_async_copy(t_from(0, 2 * jj + x), t_ref(0, x, c, y, jj), l_a.at[jj])

    def t_own(g, jj):
        return remote(
            t_from(g, 2 * jj + x), t_ref(g, x, c, y, jj), p_s.at[g, 0, jj], p_r.at[g, slot(0, y), jj], partner)

    def t_pass(g, dx, dy, jj):
        xx, yy = at_peer(dx, dy)
        ref = t_ref(g, xx, c, yy, jj)
        return remote(ref, ref, p_s.at[g, dx * parts + dy, jj], p_r.at[g, slot(dx, yy), jj], partner)

    def t_passed(g, dx, dy, jj):
        xx, yy = at_peer(dx, dy)
        ref = t_ref(g, xx, 1 - c, yy, jj)
        return remote(ref, ref, p_s.at[g, dx * parts + dy, jj], p_r.at[g, slot(dx, yy), jj], partner)

    def g_send(k):
        ref = G.at[:, ds(k * blk, blk, blk)]
        return remote(t_from(0, k), ref, g_s, g_r.at[k], dev(host_z, x, c, y))

    def back_send(j):
        return remote(bs.at[j], cr.at[0, j], b_s, c_r.at[0, j], dev(end_z, x, c, y))

    def h_ref(xx, yy, jj, cc):
        cols = ds((yy * halves + jj) * blk + cc * bw, bw, bw)
        return A.at[1, ds(xx * two, two, two), cols]

    def h_band(xx, yy, jj, r):
        cols = ds((yy * halves + jj) * blk + c * bw, bw, bw)
        return A.at[1, ds(xx * two + r * rows, rows, rows), cols]

    def h_send(dx, dy, jj, j, r):
        xx, yy = at_peer(dx, dy)
        return remote(
            hid.at[j, ds(r * rows, rows, rows)], h_band(x, y, jj, r),
            x_s.at[1 + 2 * r, dx * parts + dy, jj], x_r.at[1 + 2 * r, slot(dx, y), jj], dev(z, xx, c, yy))

    def h_got(dx, dy, jj, r):
        xx, yy = at_peer(dx, dy)
        ref = h_band(xx, yy, jj, r)
        return remote(
            ref, ref, x_s.at[1 + 2 * r, dx * parts + dy, jj], x_r.at[1 + 2 * r, slot(dx, yy), jj], dev(z, xx, c, yy))

    def h_relay(dy, jj, r):
        xx, yy = at_peer(1, dy)
        ref = h_band(xx, y, jj, r)
        return remote(
            ref, ref, x_s.at[1 + 2 * r, parts + dy, jj], x_r.at[1 + 2 * r, slot(1, y), jj], dev(z, x, c, yy))

    def h_own(jj, j):
        return remote(hid.at[j], h_ref(x, y, jj, c), p_s.at[1, 0, jj], p_r.at[1, slot(0, y), jj], partner)

    def h_pass(dx, dy, jj):
        xx, yy = at_peer(dx, dy)
        ref = h_ref(xx, yy, jj, c)
        return remote(ref, ref, p_s.at[1, dx * parts + dy, jj], p_r.at[1, slot(dx, yy), jj], partner)

    def h_passed(dx, dy, jj):
        xx, yy = at_peer(dx, dy)
        ref = h_ref(xx, yy, jj, 1 - c)
        return remote(ref, ref, p_s.at[1, dx * parts + dy, jj], p_r.at[1, slot(dx, yy), jj], partner)

    def c_send(w, j):
        return remote(cs.at[w, j], cr.at[w, j], c_s.at[w], c_r.at[w, j], dev(z, 1 - x, c, y))

    def e_send():
        return remote(eout, ein, e_s, e_r, dev(z, 1 - x, c, y))

    def chain_send():
        return remote(cout, cin, ch_s, ch_r, dev(z + 1, x, c, y))

    def o_send(j):
        return remote(ost.at[j], out_ref.at[:, ds(j * blk + c * bw, bw, bw)], o_s, o_r, partner)

    def each(n, f):
        def body(i, carry):
            f(i)
            return carry
        lax.fori_loop(0, n, body, 0)

    each(chunks, lambda j: w_local(0, j).start())
    each(chunks, lambda j: te_local(j).start())
    for t in range(5):
        each(chunks, lambda j: raw_local(t, j).start())
    each(halves, lambda jj: t_local(jj).start())
    each(chunks, lambda j: w_local(1, j).start())

    barrier = pltpu.get_barrier_semaphore()

    def greet(where):
        pl.semaphore_signal(barrier, inc=1, device_id=where, device_id_type=MESH)

    greet(partner)
    for dx, dy in peers:
        xx, yy = at_peer(dx, dy)
        greet(dev(z, xx, c, yy))
    line_peers = [
        (z > 0, dev(z - 1, x, c, y)),
        (z < lines - 1, dev(z + 1, x, c, y)),
    ]
    for there, where in line_peers:
        @pl.when(there)
        def _():
            greet(where)
    pl.semaphore_wait(barrier, 1 + len(peers) + sum(there.astype(jnp.int32) for there, _ in line_peers))

    each(chunks, lambda j: w_swap(0, j).start())

    @pl.when(z == 0)
    def _():
        each(chunks - 1, lambda k: g_send(k).start())

    @pl.when(z == lines - 1)
    def _():
        each(chunks, lambda k: g_send(k).start())

    def t_start(g, jj):
        t_send(g, 1, 0, jj).start()
        for dy in range(1, parts):
            t_send(g, 0, dy, jj).start()
        t_own(g, jj).start()

    each(halves, lambda jj: t_start(0, jj))
    each(chunks, lambda j: te_swap(j).start())
    each(chunks, lambda j: w_swap(1, j).start())

    def own_ready(w, j):
        w_local(w, j).wait()
        w_swap(w, j).wait_recv()

    def wanted(w, j, side):
        target = z + (1 if side else -1)
        inside = (target >= 0) & (target < lines)
        if w == 0:
            inside = inside & (((target > 0) & (target < lines - 1)) | (j < kept))
        return inside

    def outer_side(side):
        target = z + (1 if side else -1)
        return is_end | (target == 0) | (target == lines - 1)

    def own_at(w, j, side, there):
        @pl.when(wanted(w, j, side) & there)
        def _():
            z_send(w, j, z, side).start()

    def own_inner(w, j):
        for side in range(2):
            @pl.when(wanted(w, j, side) & jnp.logical_not(outer_side(side)))
            def _():
                z_send(w, j, z, side).start()

    def hop(w, j, o, side, there):
        @pl.when(there)
        def _():
            z_send(w, j, o, side).wait_recv()

            @pl.when(wanted(w, j, side))
            def _():
                z_send(w, j, o, side).start()

    def relay_cases(d, from_end):
        low, high = z - d, z + d
        if d == 1:
            at_low = (low == 0) if from_end else (low > 0)
            at_high = (high == lines - 1) if from_end else (high < lines - 1)
        else:
            at_low, at_high = low >= 0, high < lines
        return (low, 1, is_mid & at_low), (high, 0, is_mid & at_high)

    def forward_end(w, j, sides=(0, 1)):
        for o, side, there in relay_cases(1, True):
            if side in sides:
                hop(w, j, o, side, there)

    def forward(w, j, d, sides=(0, 1)):
        for o, side, there in relay_cases(d, False):
            if side in sides:
                hop(w, j, o, side, there)

    def forward_far(w, j):
        for d in range(2, lines - 1):
            forward(w, j, d)

    def at_end(w, j):
        for d in range(1, lines):
            @pl.when(z == 0)
            def _():
                z_send(w, j, d, 0).wait_recv()

            @pl.when(z == lines - 1)
            def _():
                z_send(w, j, lines - 1 - d, 0).wait_recv()

    def span(start, stop, f):
        def body(j, carry):
            f(j)
            return carry
        lax.fori_loop(start, stop, body, 0)

    def first_sends(j):
        own_ready(0, j)
        own_at(0, j, 0, z >= 0)
        own_at(0, j, 1, is_mid & (outer_side(1) | (j < halves)))

    each(chunks, first_sends)

    pltpu.make_async_copy(raw, raw, l_raw).wait()
    for e in range(sub):
        band = slice(e * LANES, (e + 1) * LANES)
        rate, theta, scale, o_re, o_im = (raw[t, :, band] for t in range(5))
        magnitude = 1.0 - rate
        scale = scale * jnp.sqrt(1.0 - magnitude * magnitude)
        at = pl.ds(e, dims, stride=sub)
        c_re_ref[at, :] = scale * o_re
        c_im_ref[at, :] = scale * o_im
        q_re_ref[at, :] = magnitude * jnp.cos(theta)
        q_im_ref[at, :] = magnitude * jnp.sin(theta)
        k, lane = e // tiles, e % tiles
        row = 2 * k * tiles + lane
        skip_ref[e:e + 1, :] = jnp.where(c == 0, skip_in[row:row + 1, :], skip_in[row + tiles:row + tiles + 1, :])

    def span_of():
        base = q_re_ref[...], q_im_ref[...]
        total = None
        count = two
        while count:
            if count % 2:
                total = base if total is None else (
                    total[0] * base[0] - total[1] * base[1], total[0] * base[1] + total[1] * base[0])
            base = base[0] * base[0] - base[1] * base[1], 2.0 * base[0] * base[1]
            count //= 2
        s_re_ref[...] = total[0]
        s_im_ref[...] = total[1]

    span_of()

    te_mine = te.at[ds(c * rows, rows, rows), :]
    te_theirs = te.at[ds((1 - c) * rows, rows, rows), :]
    pltpu.make_async_copy(te_mine, te_mine, l_te).wait()
    remote(te_theirs, te_theirs, te_s, te_r, partner).wait_recv()

    def lay(i, carry):
        for e in range(sub):
            v = te[pl.ds(i * 16, 16), e * LANES:(e + 1) * LANES].astype(F32)
            x2d[pl.ds(i * 16 * sub + e, 16, stride=sub), :] = v
        return carry

    lax.fori_loop(0, two // 16, lay, 0)

    def second_own(j):
        own_ready(1, j)
        for side in range(2):
            own_at(1, j, side, is_mid & outer_side(side) & (j < halves))
        own_at(1, j, 0, z == lines - 1)

    each(chunks, second_own)

    half = dims // 2

    def tile(ref, h):
        return ref[h * sub:(h + 1) * sub, :]

    def step(state, v, q_re, q_im):
        return [(a * re - b * im + v, a * im + b * re) for (re, im), a, b in zip(state, q_re, q_im)]

    def end_half(k):
        hs = range(k * half, (k + 1) * half)
        q_re = [tile(q_re_ref, h) for h in hs]
        q_im = [tile(q_im_ref, h) for h in hs]
        zero = jnp.zeros((sub, LANES), F32)

        def body(i, state):
            for u in range(UNROLL):
                state = step(state, x2d[ds((i * UNROLL + u) * sub, sub, sub), :], q_re, q_im)
            return state

        state = lax.fori_loop(0, two // UNROLL, body, [(zero, zero)] * half)
        for h, (re, im) in zip(hs, state):
            st[0, h * sub:(h + 1) * sub, :] = re
            st[1, h * sub:(h + 1) * sub, :] = im

    def took_x(g):
        def go(jj):
            t_got(g, 1, 0, jj).wait_recv()
            for dy in range(1, parts):
                t_relay(g, dy, jj).start()
            t_pass(g, 1, 0, jj).start()
        each(halves, go)

    def took_y(g, dx):
        def go(jj):
            for dy in range(1, parts):
                t_got(g, dx, dy, jj).wait_recv()
                t_pass(g, dx, dy, jj).start()
        each(halves, go)

    end_half(0)
    end_half(1)
    eout[...] = st[...].astype(BF16)
    e_send().start()
    took_x(0)
    inner_left = jnp.logical_not(outer_side(0))
    own_at(1, 0, 0, inner_left)

    def cmul(a, b):
        return a[0] * b[0] - a[1] * b[1], a[0] * b[1] + a[1] * b[0]

    span_q = s_re_ref[...], s_im_ref[...]
    e_send().wait_recv()
    mine = st[0], st[1]
    other = ein[0].astype(F32), ein[1].astype(F32)
    first = [jnp.where(x == 0, m, o) for m, o in zip(mine, other)]
    second = [jnp.where(x == 0, o, m) for m, o in zip(mine, other)]
    plane = [a + b for a, b in zip(cmul(span_q, first), second)]

    @pl.when(z == 0)
    def _():
        cin[...] = jnp.zeros_like(cin)

    @pl.when(z > 0)
    def _():
        chain_send().wait_recv()

    carry = cin[0].astype(F32), cin[1].astype(F32)
    moved = cmul(span_q, carry)
    onward = [a + b for a, b in zip(cmul(span_q, moved), plane)]
    cout[0] = onward[0].astype(BF16)
    cout[1] = onward[1].astype(BF16)

    @pl.when(z < lines - 1)
    def _():
        chain_send().start()

    for k in range(2):
        st[k] = jnp.where(x == 0, carry[k], moved[k] + first[k])

    inner_right = is_mid & jnp.logical_not(outer_side(1))

    @pl.when(z == 0)
    def _():
        g_send(chunks - 1).start()

    each(chunks, lambda j: own_at(0, j, 1, (z == 0) | (inner_right & (j >= halves))))
    each(chunks, lambda j: own_at(1, j, 1, z == 0))
    each(halves, lambda j: forward(0, j, 1))
    took_y(0, 0)

    def guest_tokens(jj):
        @pl.when(is_host)
        def _():
            g_send(2 * jj).wait_recv()
            g_send(2 * jj + 1).wait_recv()
            t_start(2, jj)
            t_ref(2, x, c, y, jj)[...] = t_from(2, 2 * jj + x)[...]

    def smooth_half(k, part, parts_of):
        hs = range(k * half, (k + 1) * half)
        q_re = [tile(q_re_ref, h) for h in hs]
        q_im = [tile(q_im_ref, h) for h in hs]
        c_re = [tile(c_re_ref, h) for h in hs]
        c_im = [tile(c_im_ref, h) for h in hs]
        skip = skip_ref[...]
        state = [(tile(st.at[0], h), tile(st.at[1], h)) for h in hs]

        def body(i, state):
            for u in range(UNROLL):
                at = ds((i * UNROLL + u) * sub, sub, sub)
                v = x2d[at, :]
                state = step(state, v, q_re, q_im)
                sums = [c_re[h] * state[h][0] - c_im[h] * state[h][1] for h in range(half)]
                while len(sums) > 1:
                    sums = [sum(sums[m:m + 2]) for m in range(0, len(sums), 2)]
                before = v * skip if k == 0 else y2d[at, :]
                y2d[at, :] = before + sums[0]
            return state

        steps = two // UNROLL // parts_of
        state = lax.fori_loop(part * steps, (part + 1) * steps, body, state)
        if part + 1 < parts_of:
            for h, (re, im) in zip(hs, state):
                st[0, h * sub:(h + 1) * sub, :] = re
                st[1, h * sub:(h + 1) * sub, :] = im

    def all_tokens(g):
        def go(jj):
            for dx, dy in others:
                t_passed(g, dx, dy, jj).wait_recv()
        each(halves, go)

    def multiply(w, g, k, j, mine):
        right = W[w, j]
        away = jnp.dot(A[g, ds((1 - x) * two, two, two), :], right, preferred_element_type=F32)
        cs[k, j] = away.astype(BF16)
        c_send(k, j).start()
        mine[j] = jnp.dot(A[g, ds(x * two, two, two), :], right, preferred_element_type=F32)

    def project(j):
        @pl.when(is_end & (j < kept))
        def _():
            at_end(0, j)

        @pl.when(is_mid | (j < kept))
        def _():
            multiply(0, 0, 0, j, own)

        @pl.when(is_end & (j >= kept))
        def _():
            own[j] = jnp.zeros((two, bw), F32)

    guest_tokens(0)
    smooth_half(0, 0, 1)
    took_y(0, 1)

    def rest_outer(j):
        for side in range(2):
            own_at(1, j, side, is_mid & outer_side(side))

    span(halves, chunks, rest_outer)
    forward_end(0, 0, (0,))
    span(1, halves, guest_tokens)
    smooth_half(1, 0, 2)
    span(1, halves, lambda j: forward_end(0, j, (0,)))
    forward_end(0, 0, (1,))
    smooth_half(1, 1, 2)

    @pl.when(is_host)
    def _():
        took_x(2)
        took_y(2, 0)

    span(1, halves, lambda j: forward_end(0, j, (1,)))
    each(halves, lambda jj: t_local(jj).wait())
    all_tokens(0)

    def guest_back(j):
        @pl.when(is_host)
        def _():
            c_send(2, j).wait_recv()
            bs[j] = (own_g[j] + cr[2, j].astype(F32)).astype(BF16)
            back_send(j).start()

    def hidden(j):
        c_send(0, j).wait_recv()
        jj = j // 2
        target = j % 2

        def band(i, carry):
            at = pl.ds(pl.multiple_of(i * 16, 16), 16)
            for e in range(tiles):
                lane = slice(e * LANES, (e + 1) * LANES)
                smooth = y2d[pl.ds(i * 16 * sub + j * tiles + e, 16, stride=sub), :]
                gate = own[j, at, lane] + cr[0, j, at, lane].astype(F32)
                value = smooth * jax.nn.sigmoid(smooth) * jax.nn.sigmoid(gate)
                hid[j, at, lane] = value.astype(BF16)
            return carry

        for r in range(2):
            lax.fori_loop(r * rows // 16, (r + 1) * rows // 16, band, 0)

            @pl.when(target == x)
            def _():
                for dy in range(1, parts):
                    h_send(0, dy, jj, j, r).start()

            @pl.when(target != x)
            def _():
                h_send(1, 0, jj, j, r).start()

        @pl.when(target == x)
        def _():
            h_own(jj, j).start()
            h_ref(x, y, jj, c)[...] = hid[j]

    def hidden_x(jj):
        for r in range(2):
            h_got(1, 0, jj, r).wait_recv()
            for dy in range(1, parts):
                h_relay(dy, jj, r).start()
        h_pass(1, 0, jj).start()

    def hidden_y(dx, jj):
        for dy in range(1, parts):
            for r in range(2):
                h_got(dx, dy, jj, r).wait_recv()
            h_pass(dx, dy, jj).start()

    def early_project(j):
        forward_far(0, j)
        forward_end(0, halves + j)
        project(j)

    each(halves, early_project)
    own_at(1, 0, 1, inner_right)
    own_inner(1, 1)
    forward(1, 0, 1, (0,))
    span(halves, chunks, lambda j: forward(0, j, 1))

    @pl.when(is_host)
    def _():
        took_y(2, 1)
        all_tokens(2)

    @pl.when(is_end)
    def _():
        each(halves, hidden)

    def guest_sums(j):
        forward_far(0, j)

        @pl.when(is_host & (j >= kept))
        def _():
            multiply(0, 2, 2, j, own_g)

    def guest_step(j):
        guest_sums(j)
        forward_end(1, j - halves)

    span(halves, chunks, guest_step)
    forward(1, 0, 1, (1,))
    span(2, chunks, lambda j: own_inner(1, j))

    @pl.when(is_mid)
    def _():
        each(halves, hidden)

    def late_project(j):
        project(j)

        @pl.when(j >= kept)
        def _():
            guest_back(j)

    span(halves, chunks, late_project)
    span(1, halves, lambda j: forward(1, j, 1))
    forward_far(1, 0)
    span(0, halves // 2, hidden_x)
    hidden(halves)
    span(1, halves, lambda j: forward_far(1, j))
    span(halves + 1, chunks, hidden)
    span(halves, chunks, lambda j: forward_end(1, j))
    span(0, halves // 2, lambda jj: hidden_y(0, jj))
    span(0, halves // 2, lambda jj: hidden_y(1, jj))
    forward(1, halves, 1)
    span(halves // 2, halves, hidden_x)
    span(halves + 1, chunks, lambda j: forward(1, j, 1))
    span(halves // 2, halves, lambda jj: hidden_y(0, jj))
    span(halves // 2, halves, lambda jj: hidden_y(1, jj))

    def all_hidden(jj):
        for dx, dy in others:
            h_passed(dx, dy, jj).wait_recv()

    each(halves, all_hidden)

    def finish(j):
        c_send(1, j).wait_recv()
        mine = ds(c * rows, rows, rows)
        theirs = ds((1 - c) * rows, rows, rows)
        ost[j] = (own[j, theirs, :] + cr[1, j, theirs, :].astype(F32)).astype(BF16)
        o_send(j).start()
        out_ref[:, ds(j * blk + c * bw, bw, bw)] = (own[j, mine, :] + cr[1, j, mine, :].astype(F32)).astype(BF16)

    def end_mix(j, near, far):
        for o in range(lines):
            if o != far and o != lines - 1 - far:
                z_send(1, j, o, 0).wait_recv()
        mine = ds(x * two, two, two)
        other = ds((1 - x) * two, two, two)
        last_cols = pl.ds(far * blk, blk)
        own_g[j] = jnp.dot(A[1, other, near], W[1, j, near], preferred_element_type=F32)
        own[j] = jnp.dot(A[1, mine, near], W[1, j, near], preferred_element_type=F32)
        z_send(1, j, far, 0).wait_recv()
        right = W[1, j, last_cols]
        cs[1, j] = (own_g[j] + jnp.dot(A[1, other, last_cols], right, preferred_element_type=F32)).astype(BF16)
        c_send(1, j).start()
        own[j] += jnp.dot(A[1, mine, last_cols], right, preferred_element_type=F32)

    def mix(j):
        @pl.when(halves + j < chunks)
        def _():
            forward_far(1, halves + j)

        @pl.when(is_mid)
        def _():
            multiply(1, 1, 1, j, own)

        @pl.when(z == 0)
        def _():
            end_mix(j, pl.ds(0, (lines - 1) * blk), lines - 1)

        @pl.when(z == lines - 1)
        def _():
            end_mix(j, pl.ds(blk, (lines - 1) * blk), 0)

    mix(0)

    def last(j):
        mix(j + 1)
        finish(j)

    each(chunks - 1, last)
    finish(chunks - 1)
    remote(ost, ost, o_s, o_r, partner).wait_recv()

    def sent(ref, sem):
        remote(ref, ref, sem, o_r, partner).wait_send()

    for w in range(2):
        sent(W.at[w, :, ds(z * blk + c * bw, bw, bw)], sw_s.at[w])
        for k in range(lines):
            for side, first, count in ((0, k, lines - k), (1, 0, k + 1)):
                target = k + (1 if side else -1)
                if 0 <= target < lines:
                    n = kept if w == 0 and target in (0, lines - 1) else chunks

                    if k in (0, lines - 1):
                        first, count = k, 1

                    @pl.when(z == k)
                    def _():
                        sent(W.at[w, pl.ds(0, n), pl.ds(first * blk, count * blk)], z_s.at[side, w])
    sent(te_mine, te_s)
    sent(ost, o_s)
    sent(cs.at[1], c_s.at[1])

    @pl.when(is_mid)
    def _():
        sent(cs.at[0], c_s.at[0])

    @pl.when(is_end)
    def _():
        sent(cs.at[0, pl.ds(0, kept)], c_s.at[0])
        sent(G, g_s)

    @pl.when(is_host)
    def _():
        sent(cs.at[2, pl.ds(kept, chunks - kept)], c_s.at[2])
        sent(bs.at[pl.ds(kept, chunks - kept)], b_s)

    def settle_tokens(g):
        def go(jj):
            t_own(g, jj).wait_send()
            t_send(g, 1, 0, jj).wait_send()
            for dy in range(1, parts):
                t_send(g, 0, dy, jj).wait_send()
                t_relay(g, dy, jj).wait_send()
            for dx, dy in peers:
                t_pass(g, dx, dy, jj).wait_send()
        each(halves, go)

    settle_tokens(0)

    @pl.when(is_host)
    def _():
        settle_tokens(2)

    def settle_hidden(jj):
        h_own(jj, 0).wait_send()
        for r in range(2):
            h_send(1, 0, jj, 0, r).wait_send()
            for dy in range(1, parts):
                h_send(0, dy, jj, 0, r).wait_send()
                h_relay(dy, jj, r).wait_send()
        for dx, dy in peers:
            h_pass(dx, dy, jj).wait_send()

    each(halves, settle_hidden)

    e_send().wait_send()

    @pl.when(z < lines - 1)
    def _():
        chain_send().wait_send()


def per_device(shards, parts, tokens, decay_rate, angle, in_coef, out_coef, skip_coef, gate_weight, out_weight):
    rows, width = tokens.shape
    dims = decay_rate.shape[1]
    lines = shards // 4
    bw = gate_weight.shape[0]
    blk = 2 * bw
    chunks = width // blk
    assert shards % 4 == 0 and lines > 3 and dims % 2 == 0
    assert chunks % 2 == 0 and bw % LANES == 0 and chunks * 2 * parts == shards
    sub = chunks * bw // LANES
    two = 2 * rows
    depth = lines * blk
    skip = skip_coef.reshape(2 * sub, LANES)

    hbm = pl.BlockSpec(memory_space=pltpu.HBM)
    vmem = pl.BlockSpec(memory_space=pltpu.VMEM)
    dma = pltpu.SemaphoreType.DMA
    halves = chunks // 2
    n = 2 * parts
    flops = 2 * 2 * 4 * rows * depth * chunks * bw
    return pl.pallas_call(
        functools.partial(mixer_kernel, lines, parts, dims, chunks - max(1, chunks * GUESTS // 4)),
        in_specs=[hbm] * 7 + [vmem],
        out_specs=vmem,
        out_shape=pltpu.VMEM((rows, width), BF16),
        scratch_shapes=[
            pltpu.VMEM((5, dims, chunks * bw), F32),
        ] + [pltpu.VMEM((dims * sub, LANES), F32)] * 6 + [
            pltpu.VMEM((sub, LANES), F32),
            pltpu.VMEM((two, chunks * bw), BF16),
            pltpu.VMEM((two * sub, LANES), F32),
            pltpu.VMEM((two * sub, LANES), F32),
            pltpu.VMEM((2, dims * sub, LANES), F32),
            pltpu.VMEM((2, dims * sub, LANES), BF16),
            pltpu.VMEM((2, dims * sub, LANES), BF16),
            pltpu.VMEM((2, dims * sub, LANES), BF16),
            pltpu.VMEM((2, dims * sub, LANES), BF16),
            pltpu.VMEM((3, 4 * rows, depth), BF16),
            pltpu.VMEM((2, chunks, depth, bw), BF16),
            pltpu.VMEM((chunks, two, bw), F32),
            pltpu.VMEM((chunks, two, bw), F32),
            pltpu.VMEM((3, chunks, two, bw), BF16),
            pltpu.VMEM((3, chunks, two, bw), BF16),
            pltpu.VMEM((chunks, two, bw), BF16),
            pltpu.VMEM((chunks, rows, bw), BF16),
            pltpu.VMEM((rows, width), BF16),
            pltpu.VMEM((chunks, two, bw), BF16),
            dma((2, chunks)),
            dma,
            dma((halves,)),
            dma,
            dma((2,)),
            dma((2, chunks)),
            dma,
            dma,
            dma((2, 2)),
            dma((2, chunks, lines)),
            dma((4, n, halves)),
            dma((4, n, halves)),
            dma((3, n, halves)),
            dma((3, n, halves)),
            dma,
            dma((chunks,)),
            dma,
            dma,
            dma,
            dma,
            dma,
            dma((3,)),
            dma((3, chunks)),
            dma,
            dma,
        ],
        compiler_params=pltpu.CompilerParams(
            collective_id=0, has_side_effects=True, vmem_limit_bytes=56 * 1024 * 1024
        ),
        cost_estimate=pl.CostEstimate(flops=flops, bytes_accessed=4 * tokens.size, transcendentals=0),
        name="mixer",
    )(
        tokens, gate_weight, out_weight, decay_rate.T, angle.T, in_coef.T, out_coef.swapaxes(1, 2), skip,
    )


def solution(mesh):
    in_specs = (
        P("seq", "tp"),
        P("tp", None),
        P("tp", None),
        P("tp", None),
        P(None, "tp", None),
        P("tp"),
        P("seq", "tp"),
        P("seq", "tp"),
    )
    body = functools.partial(per_device, mesh.shape["seq"], mesh.shape["tp"])
    return jax.shard_map(body, mesh=mesh, in_specs=in_specs, out_specs=P("seq", "tp"), check_vma=False)
```
